16 devices in a mesh: outer: 2 (over z), middle: 2 (over y), inner: 4 (over x, core).
Axes of the slice: x: 2, y: 2, z: 2, core: 2. Of those that a mesh axis runs over, the one named last changes fastest.
Arguments:
- g_embed: float32 [16, 4096, 1024], P(('outer', 'middle', 'inner'))
- g_attn: float32 [16, 1, 1024, 4096], P(('outer', 'middle', 'inner'))
- g_ffn_in: float32 [16, 1, 1024, 2816], P(('outer', 'middle', 'inner'))
- g_ffn_out: float32 [16, 1, 2816, 1024], P(('outer', 'middle', 'inner'))
- g_vec: float32 [16, 1, 12032], P(('outer', 'middle', 'inner'))
- m_flat: float32 [14167808], P(('outer', 'middle', 'inner'))
- v_flat: float32 [14167808], P(('outer', 'middle', 'inner'))
- w_flat: float32 [14167808], P(('outer', 'middle', 'inner'))
Outputs:
- output 1: float32 [14167808], P(('outer', 'middle', 'inner'))
- output 2: float32 [14167808], P(('outer', 'middle', 'inner'))
- output 3: float32 [14167808], P(('outer', 'middle', 'inner'))
- output 4: bfloat16 [4096, 1024], replicated
- output 5: bfloat16 [1, 1024, 4096], replicated
- output 6: bfloat16 [1, 1024, 2816], replicated
- output 7: bfloat16 [1, 2816, 1024], replicated
- output 8: bfloat16 [1, 12032], replicated
- output 9: bfloat16 [16, 1770976], P(('outer', 'middle', 'inner'))
All inputs are finite; a program needn't handle non-finite values.
Results may differ from the reference program's by a relative error of at most 0.001.
Values are sent between devices in bfloat16 or wider.
A program may use at most 1 GiB of HBM per device.

```python
import math
import jax
import jax.numpy as jnp

DEVICES = 16
VOCAB_ROWS = 4096
D = 1024
FF = 2816
LAYERS = 1
ADAM_STEP = 3

ADAM_BETA1 = 0.9
ADAM_BETA2 = 0.98
ADAM_EPS = 1e-9
LEARN_RATE = 0.05
NUM_CHIPS = DEVICES // 2
VEC_WIDTH = 9 * D + FF
TENSOR_SHAPES = ((VOCAB_ROWS, D), (LAYERS, D, 4 * D), (LAYERS, D, FF), (LAYERS, FF, D), (LAYERS, VEC_WIDTH))
PARAM_COUNT = sum(math.prod(shape) for shape in TENSOR_SHAPES)


def draw_gradient(gen_key, shape):
    common_key, chip_key, core_key = jax.random.split(gen_key, 3)
    common = jax.random.normal(common_key, shape, jnp.float32)
    per_chip = jax.random.normal(chip_key, (NUM_CHIPS,) + shape, jnp.float32)
    per_core = jax.random.normal(core_key, (DEVICES,) + shape, jnp.float32)
    return common[None] + jnp.repeat(per_chip, 2, axis=0) + 0.25 * per_core


def setup_inputs(seed: int = 0) -> dict:
    key_list = jax.random.split(jax.random.key(seed), 8)
    return {
        'g_embed': draw_gradient(key_list[0], TENSOR_SHAPES[0]),
        'g_attn': draw_gradient(key_list[1], TENSOR_SHAPES[1]),
        'g_ffn_in': draw_gradient(key_list[2], TENSOR_SHAPES[2]),
        'g_ffn_out': draw_gradient(key_list[3], TENSOR_SHAPES[3]),
        'g_vec': draw_gradient(key_list[4], TENSOR_SHAPES[4]),
        'm_flat': 0.3 * jax.random.normal(key_list[5], (PARAM_COUNT,), jnp.float32),
        'v_flat': 0.1 * (0.5 + jax.random.uniform(key_list[6], (PARAM_COUNT,), jnp.float32)),
        'w_flat': jax.random.normal(key_list[7], (PARAM_COUNT,), jnp.float32),
    }


def adam_update(grad_mean, m_old, v_old, w_old):
    m_new = ADAM_BETA1 * m_old + (1.0 - ADAM_BETA1) * grad_mean
    v_new = ADAM_BETA2 * v_old + (1.0 - ADAM_BETA2) * (grad_mean * grad_mean)
    m_hat = m_new / (1.0 - ADAM_BETA1 ** ADAM_STEP)
    v_hat = v_new / (1.0 - ADAM_BETA2 ** ADAM_STEP)
    w_new = w_old - LEARN_RATE * m_hat / (jnp.sqrt(v_hat) + ADAM_EPS)
    return m_new, v_new, w_new


def split_tensors(flat_values, shape_list):
    pieces = []
    offset = 0
    for shape in shape_list:
        count = math.prod(shape)
        pieces.append(flat_values[offset:offset + count].reshape(shape))
        offset += count
    return pieces


def chip_blocks(w_tensors, num_chips):
    blocks = [w_tensors[0].reshape(num_chips, -1)]
    for tensor in w_tensors[1:]:
        layer_count = tensor.shape[0]
        blocks.append(jnp.swapaxes(tensor.reshape(layer_count, num_chips, -1), 0, 1).reshape(num_chips, -1))
    return jnp.concatenate(blocks, axis=1)


def reference(g_embed, g_attn, g_ffn_in, g_ffn_out, g_vec, m_flat, v_flat, w_flat):
    grad_list = (g_embed, g_attn, g_ffn_in, g_ffn_out, g_vec)
    grad_mean = jnp.concatenate([jnp.sum(gradient, axis=0).reshape(-1) for gradient in grad_list]) / DEVICES
    m_new, v_new, w_new = adam_update(grad_mean, m_flat, v_flat, w_flat)
    w_tensors = split_tensors(w_new.astype(jnp.bfloat16), TENSOR_SHAPES)
    w_chip = jnp.repeat(chip_blocks(w_tensors, NUM_CHIPS), 2, axis=0)
    return (m_new, v_new, w_new, w_tensors[0], w_tensors[1], w_tensors[2], w_tensors[3], w_tensors[4], w_chip)
```

```python
import functools
import math
import jax
import jax.numpy as jnp
from jax import lax
from jax.experimental import pallas as pl
from jax.experimental.pallas import tpu as pltpu
from jax.sharding import PartitionSpec as P

MESH_AXES = ('outer', 'middle', 'inner')
MESH = pl.DeviceIdType.MESH
ADAM_BETA1 = 0.9
ADAM_BETA2 = 0.98
ADAM_EPS = 1e-9
LEARN_RATE = 0.05
ADAM_STEP = 3

LANES = 128
SLICE = 885488
TENSORS = ((0, 32768, 8), (32768, 65536, 32), (65536, 88064, 22), (88064, 110592, 8), (110592, 110720, 1))
ROWS = 110720
UNIT = 128
WINDOW = 7296
THIRD = WINDOW // 3
ITEMS = THIRD // UNIT
EDGE = 32768
OWN = 7200
OWN_THIRD = OWN // 3
OWN_CHUNK = 160
OWN_ITEMS = OWN_THIRD // OWN_CHUNK
SIXTEEN = 16


def floor_block(row):
    result = row
    for base, end, tiles in TENSORS:
        block = 8 * tiles if tiles > 1 else UNIT
        floored = base + (row - base) // block * block
        result = jnp.where((row >= base) & (row < end), floored, result)
    return result


def window_start(index):
    row = floor_block(index * (SLICE // 16) // 8)
    return jnp.minimum(row // UNIT * UNIT, ROWS - WINDOW)


def own_start_static(index):
    row = -(-index * SLICE // LANES)
    for base, end, tiles in TENSORS:
        if base <= row < end:
            block = 8 * tiles if tiles > 1 else UNIT
            return base + -(-(row - base) // block) * block
    return ROWS


OWN_STARTS = [own_start_static(d) for d in range(SIXTEEN)] + [ROWS]


def own_start(index):
    result = jnp.int32(0)
    for d in range(SIXTEEN):
        result = jnp.where(index == d, OWN_STARTS[d], result)
    return result


def adam_update(grad_mean, m_old, v_old, w_old):
    m_new = ADAM_BETA1 * m_old + (1.0 - ADAM_BETA1) * grad_mean
    v_new = ADAM_BETA2 * v_old + (1.0 - ADAM_BETA2) * (grad_mean * grad_mean)
    m_hat = m_new / (1.0 - ADAM_BETA1 ** ADAM_STEP)
    v_hat = v_new / (1.0 - ADAM_BETA2 ** ADAM_STEP)
    w_new = w_old - LEARN_RATE * m_hat / (jnp.sqrt(v_hat) + ADAM_EPS)
    return m_new, v_new, w_new


def to_tiles(tensor):
    rows, width = tensor.shape
    return tensor.reshape(rows // 8, 8, width // LANES, LANES).transpose(0, 2, 1, 3).reshape(-1, LANES)


def from_tiles(tiles, width):
    return tiles.reshape(-1, width // LANES, 8, LANES).transpose(0, 2, 1, 3).reshape(-1, width)


ORDERS = ((0, 1, 2), (1, 2, 0), (2, 0, 1))


def position():
    outer, middle, inner = (lax.axis_index(name) for name in MESH_AXES)
    return outer, middle, inner // 2, inner % 2


def neighbour(axis):
    outer, middle, x, core = position()
    z, y = outer, middle
    if axis == 0:
        z = 1 - z
    elif axis == 1:
        y = 1 - y
    elif axis == 2:
        x = 1 - x
    else:
        core = 1 - core
    return (z, y, 2 * x + core)


def scatter_kernel(e_ref, a_ref, f_ref, h_ref, b_ref, m_ref, v_ref, w_ref, out_ref, edge_ref,
                   part, recv0, recv1, recv2, mine, pair_send, pair_recv, mine_sem,
                   send0, send1, send2, arrive0, arrive1, arrive2, out_sem, edge_send, edge_recv):
    z, y, x, core = position()
    chip = (z * 2 + y) * 2 + x
    device = chip * 2 + core
    sources = (e_ref, a_ref, f_ref, h_ref, b_ref)

    before = (device + SIXTEEN - 1) % SIXTEEN
    for n, ref in enumerate((m_ref, v_ref, w_ref)):
        pltpu.make_async_remote_copy(
            src_ref=ref.at[pl.ds(0, EDGE)], dst_ref=edge_ref.at[pl.ds(n * EDGE, EDGE)],
            send_sem=edge_send.at[n], recv_sem=edge_recv.at[n],
            device_id=(before // 8, before // 4 % 2, before % 4), device_id_type=MESH).start()

    def from_source(row, action):
        for source, (base, end, _) in zip(sources, TENSORS):
            @pl.when((row >= base) & (row < end))
            def _():
                action(source.at[pl.ds(pl.multiple_of(row - base, UNIT), UNIT), :])

    def item_row(third, item):
        return pl.multiple_of(third * THIRD + item * UNIT, UNIT)

    def start_pair(item):
        @pl.loop(0, 8)
        def _(j):
            jz, jy, jx = j // 4, j // 2 % 2, j % 2
            other = ((z + jz) % 2 * 2 + (y + jy) % 2) * 2 + (x + jx) % 2
            start = window_start(other * 2 + 1 - core)
            for third in range(3):
                row = item_row(third, item)
                from_source(start + row, lambda src: pltpu.make_async_remote_copy(
                    src_ref=src, dst_ref=part.at[jz, jy, jx, pl.ds(row, UNIT), :],
                    send_sem=pair_send.at[third, item], recv_sem=pair_recv.at[third, item],
                    device_id=neighbour(3), device_id_type=MESH).start())

    def start_mine(item, slot):
        @pl.loop(0, 8)
        def _(j):
            jz, jy, jx = j // 4, j // 2 % 2, j % 2
            other = ((z + jz) % 2 * 2 + (y + jy) % 2) * 2 + (x + jx) % 2
            start = window_start(other * 2 + core)
            for third in range(3):
                row = item_row(third, item)
                from_source(start + row, lambda src: pltpu.make_async_copy(
                    src, mine.at[slot, third, jz, jy, jx], mine_sem.at[slot]).start())

    def hop_copy(third, item, hop):
        rows = pl.ds(item_row(third, item), UNIT)
        first, second, last = ORDERS[third]
        if hop == 0:
            index = tuple(1 if n == first else slice(None) for n in range(3))
            target = recv0.at[:, :, rows, :]
        elif hop == 1:
            index = tuple(0 if n == first else 1 if n == second else slice(None) for n in range(3))
            target = recv1.at[:, rows, :]
        else:
            index = tuple(1 if n == last else 0 for n in range(3))
            target = recv2.at[rows, :]
        return pltpu.make_async_remote_copy(
            src_ref=part.at[index + (rows, slice(None))], dst_ref=target,
            send_sem=(send0, send1, send2)[hop].at[third, item], recv_sem=(arrive0, arrive1, arrive2)[hop].at[third, item],
            device_id=neighbour(ORDERS[third][hop]), device_id_type=MESH)

    def pair_all(third, item):
        block = part.at[:, :, :, pl.ds(item_row(third, item), UNIT), :]
        return pltpu.make_async_remote_copy(
            src_ref=block, dst_ref=block, send_sem=pair_send.at[third, item], recv_sem=pair_recv.at[third, item],
            device_id=neighbour(3), device_id_type=MESH)

    def out_copy(third, item):
        rows = pl.ds(item_row(third, item), UNIT)
        return pltpu.make_async_copy(part.at[0, 0, 0, rows, :], out_ref.at[rows, :], out_sem.at[third, item])

    start_mine(0, 0)
    start_pair(0)
    start_pair(1)

    @pl.loop(0, ITEMS + 4)
    def _(step):
        @pl.when(step < ITEMS)
        def _():
            slot = step % 2

            @pl.when(step + 1 < ITEMS)
            def _():
                start_mine(step + 1, 1 - slot)

            @pl.when(step + 2 < ITEMS)
            def _():
                start_pair(step + 2)

            pltpu.make_async_copy(mine.at[slot], mine.at[slot], mine_sem.at[slot]).wait()
            for third in range(3):
                rows = pl.ds(item_row(third, step), UNIT)
                pair_all(third, step).wait_recv()
                for j in range(8):
                    index = (j // 4, j // 2 % 2, j % 2)
                    part[index + (rows, slice(None))] += mine[(slot, third) + index]
                hop_copy(third, step, 0).start()

        @pl.when((step >= 1) & (step < ITEMS + 1))
        def _():
            item = step - 1
            for third in range(3):
                rows = pl.ds(item_row(third, item), UNIT)
                hop_copy(third, item, 0).wait_recv()
                first = ORDERS[third][0]
                for j in range(4):
                    pair = [j // 2, j % 2]
                    index = tuple(pair[:first] + [0] + pair[first:])
                    part[index + (rows, slice(None))] += recv0[j // 2, j % 2, rows, :]
                hop_copy(third, item, 1).start()

        @pl.when((step >= 2) & (step < ITEMS + 2))
        def _():
            item = step - 2
            for third in range(3):
                rows = pl.ds(item_row(third, item), UNIT)
                hop_copy(third, item, 1).wait_recv()
                last = ORDERS[third][2]
                for j in range(2):
                    index = tuple(j if n == last else 0 for n in range(3))
                    part[index + (rows, slice(None))] += recv1[j, rows, :]
                hop_copy(third, item, 2).start()

        @pl.when((step >= 3) & (step < ITEMS + 3))
        def _():
            item = step - 3
            for third in range(3):
                rows = pl.ds(item_row(third, item), UNIT)
                hop_copy(third, item, 2).wait_recv()
                part[0, 0, 0, rows, :] = (part[0, 0, 0, rows, :] + recv2[rows, :]) / SIXTEEN

        @pl.when(step >= 4)
        def _():
            for third in range(3):
                out_copy(third, step - 4).start()

    @pl.loop(0, ITEMS)
    def _(item):
        for third in range(3):
            pair_all(third, item).wait_send()
            for hop in range(3):
                hop_copy(third, item, hop).wait_send()
            out_copy(third, item).wait()

    for n, ref in enumerate((m_ref, v_ref, w_ref)):
        pltpu.make_async_remote_copy(
            src_ref=ref.at[pl.ds(0, EDGE)], dst_ref=edge_ref.at[pl.ds(n * EDGE, EDGE)],
            send_sem=edge_send.at[n], recv_sem=edge_recv.at[n],
            device_id=(before // 8, before // 4 % 2, before % 4), device_id_type=MESH).wait()


def scatter(grads, m, v, w):
    any_spec = pl.BlockSpec(memory_space=pl.ANY)
    dma = pltpu.SemaphoreType.DMA
    return pl.pallas_call(
        scatter_kernel,
        out_shape=(jax.ShapeDtypeStruct((WINDOW, LANES), jnp.float32), jax.ShapeDtypeStruct((3 * EDGE,), jnp.float32)),
        in_specs=[any_spec] * 8,
        out_specs=(any_spec, any_spec),
        scratch_shapes=[
            pltpu.VMEM((2, 2, 2, WINDOW, LANES), jnp.float32),
            pltpu.VMEM((2, 2, WINDOW, LANES), jnp.float32),
            pltpu.VMEM((2, WINDOW, LANES), jnp.float32),
            pltpu.VMEM((WINDOW, LANES), jnp.float32),
            pltpu.VMEM((2, 3, 2, 2, 2, UNIT, LANES), jnp.float32),
            dma((3, ITEMS)), dma((3, ITEMS)), dma((2,)),
            dma((3, ITEMS)), dma((3, ITEMS)), dma((3, ITEMS)),
            dma((3, ITEMS)), dma((3, ITEMS)), dma((3, ITEMS)),
            dma((3, ITEMS)), dma((3,)), dma((3,)),
        ],
        compiler_params=pltpu.CompilerParams(has_side_effects=True, vmem_limit_bytes=67043328),
    )(*grads, m, v, w)


def gather_kernel(w_ref, full_ref, pair_send, pair_recv, send, arrive, own_sem):
    z, y, x, core = position()
    here = (z, y, x)

    def rows_of(third, item):
        return pl.ds(pl.multiple_of(third * OWN_THIRD + item * OWN_CHUNK, OWN_CHUNK), OWN_CHUNK)

    own = pltpu.make_async_copy(w_ref, full_ref.at[z, y, x, core], own_sem)
    own.start()

    def copy(third, item, hop):
        rows = rows_of(third, item)
        order = ORDERS[third]
        if hop == 0:
            source = w_ref.at[rows, :]
            target = full_ref.at[z, y, x, core, rows, :]
        else:
            index = tuple(slice(None) if n in order[:hop] else here[n] for n in range(3))
            source = target = full_ref.at[index + (core, rows, slice(None))]
        return pltpu.make_async_remote_copy(
            src_ref=source, dst_ref=target, send_sem=send.at[third, item, hop], recv_sem=arrive.at[third, item, hop],
            device_id=neighbour(order[hop]), device_id_type=MESH)

    def arrival(third, item, hop):
        rows = rows_of(third, item)
        order = ORDERS[third]
        index = tuple(slice(None) if n in order[:hop] else (1 - here[n] if n == order[hop] else here[n]) for n in range(3))
        block = full_ref.at[index + (core, rows, slice(None))]
        return pltpu.make_async_remote_copy(
            src_ref=block, dst_ref=block, send_sem=send.at[third, item, hop], recv_sem=arrive.at[third, item, hop],
            device_id=neighbour(order[hop]), device_id_type=MESH)

    def pair(third, item, side):
        block = full_ref.at[:, :, :, side, rows_of(third, item), :]
        return pltpu.make_async_remote_copy(
            src_ref=block, dst_ref=block, send_sem=pair_send.at[third, item], recv_sem=pair_recv.at[third, item],
            device_id=neighbour(3), device_id_type=MESH)

    for third in range(3):
        copy(third, 0, 0).start()
    own.wait()

    @pl.loop(0, OWN_ITEMS + 3)
    def _(step):
        @pl.when(step + 1 < OWN_ITEMS)
        def _():
            for third in range(3):
                copy(third, step + 1, 0).start()

        for hop in range(1, 4):
            @pl.when((step >= hop - 1) & (step < OWN_ITEMS + hop - 1))
            def _():
                item = step - (hop - 1)
                for third in range(3):
                    arrival(third, item, hop - 1).wait_recv()
                    if hop < 3:
                        copy(third, item, hop).start()
                    else:
                        pair(third, item, core).start()

    @pl.loop(0, OWN_ITEMS)
    def _(item):
        for third in range(3):
            pair(third, item, 1 - core).wait_recv()
            pair(third, item, core).wait_send()
            for hop in range(3):
                copy(third, item, hop).wait_send()


def gather(w_own):
    dma = pltpu.SemaphoreType.DMA
    return pl.pallas_call(
        gather_kernel,
        out_shape=jax.ShapeDtypeStruct((2, 2, 2, 2, OWN, LANES), jnp.bfloat16),
        in_specs=[pl.BlockSpec(memory_space=pltpu.VMEM)],
        out_specs=pl.BlockSpec(memory_space=pl.ANY),
        scratch_shapes=[
            dma((3, OWN_ITEMS)), dma((3, OWN_ITEMS)), dma((3, OWN_ITEMS, 3)), dma((3, OWN_ITEMS, 3)), dma(()),
        ],
        compiler_params=pltpu.CompilerParams(has_side_effects=True),
    )(w_own)


def device_index():
    outer, middle, inner = (lax.axis_index(name) for name in MESH_AXES)
    return (outer * 2 + middle) * 4 + inner


def for_blocks(start, length, action):
    for base, end, tiles in TENSORS:
        block = 8 * tiles
        low = (jnp.maximum(start, base) - base + block - 1) // block
        high = jnp.maximum(jnp.minimum(start + length, end) - base, 0) // block

        @pl.loop(low, jnp.maximum(high, low))
        def _(n):
            action(pl.multiple_of(base + n * block - start, 8), tiles)


def flat_kernel(tile_ref, flat_ref):
    def action(row, tiles):
        for t in range(tiles):
            flat_ref[pl.ds(row + t, 8, stride=tiles), :] = tile_ref[pl.ds(row + 8 * t, 8), :]
    for_blocks(window_start(device_index()), WINDOW, action)


def tile_kernel(flat_ref, tile_ref, work):
    def action(row, tiles):
        for t in range(tiles):
            work[pl.ds(row + 8 * t, 8), :] = flat_ref[pl.ds(row + t, 8, stride=tiles), :]
    for_blocks(own_start(device_index()), OWN, action)
    tile_ref[...] = work[...].astype(jnp.bfloat16)


def chip_kernel(e_ref, a_ref, f_ref, h_ref, b_ref, out_ref, buf, sems):
    chip = device_index() // 2
    offset = 0
    copies = []
    for n, ref in enumerate((e_ref, a_ref, f_ref, h_ref)):
        base, end, tiles = TENSORS[n]
        rows = (end - base) // 8
        copies.append((pltpu.make_async_copy(
            ref.at[pl.ds(pl.multiple_of(chip * rows, rows), rows), :], buf.at[pl.ds(offset, rows), :], sems.at[n]),
            offset, rows, tiles))
        copies[-1][0].start()
        offset += rows
    out_ref[pl.ds(offset, 16), :] = b_ref[...]
    for copy, first, rows, tiles in copies:
        copy.wait()

        @pl.loop(0, rows // (16 * tiles))
        def _(n):
            for half in range(2):
                row = pl.multiple_of(first + n * 16 * tiles + half * 8 * tiles, 16) if tiles % 2 == 0 else None
                for t in range(0, tiles, 2):
                    value = buf[pl.ds(row + 8 * t, 16), :].astype(jnp.float32)
                    out_ref[pl.ds(row + t, 8, stride=tiles), :] = value[:8]
                    out_ref[pl.ds(row + t + 1, 8, stride=tiles), :] = value[8:]


CHIP_ROWS = 13824 + 16


def solution(mesh):
    vmem = pl.BlockSpec(memory_space=pltpu.VMEM)
    any_spec = pl.BlockSpec(memory_space=pl.ANY)

    def local_step(g_embed, g_attn, g_ffn_in, g_ffn_out, g_vec, m_shard, v_shard, w_shard):
        device = device_index()
        vec_count = g_vec.size
        grads = [to_tiles(g[0] if g.ndim == 3 else g[0, 0]) for g in (g_embed, g_attn, g_ffn_in, g_ffn_out)]
        grads.append(jnp.pad(g_vec.reshape(-1), (0, UNIT * LANES - vec_count)).reshape(UNIT, LANES))
        mean_tiles, edges = scatter(grads, m_shard, v_shard, w_shard)

        mean_flat = pl.pallas_call(
            flat_kernel, out_shape=jax.ShapeDtypeStruct((WINDOW + 512, LANES), jnp.float32),
            in_specs=[vmem], out_specs=vmem)(mean_tiles).reshape(-1)
        start = window_start(device) * LANES
        mean_ext = lax.dynamic_slice(mean_flat, (device * SLICE - start,), (SLICE + EDGE,))
        m_new, v_new, w_new = adam_update(mean_ext[:SLICE], m_shard, v_shard, w_shard)
        w_edge = adam_update(mean_ext[SLICE:], edges[:EDGE], edges[EDGE:2 * EDGE], edges[2 * EDGE:])[2]
        w_ext = jnp.concatenate([w_new, w_edge, jnp.zeros(((OWN + 512) * LANES - SLICE - EDGE,), jnp.float32)])
        w_rows = lax.dynamic_slice(w_ext, (own_start(device) * LANES - device * SLICE,), (OWN * LANES,)).reshape(OWN, LANES)
        w_own = pl.pallas_call(
            tile_kernel, out_shape=jax.ShapeDtypeStruct((OWN, LANES), jnp.bfloat16),
            in_specs=[vmem], out_specs=vmem, scratch_shapes=[pltpu.VMEM((OWN, LANES), jnp.float32)])(w_rows)

        full = gather(w_own).reshape(SIXTEEN, OWN, LANES)
        tiles = []
        for base, end, _ in TENSORS:
            pieces = []
            for d in range(SIXTEEN):
                low, high = max(OWN_STARTS[d], base), min(OWN_STARTS[d + 1], end)
                if low < high:
                    pieces.append(full[d, low - OWN_STARTS[d]:high - OWN_STARTS[d]])
            tiles.append(jnp.concatenate(pieces, axis=0))
        vec = tiles[4].reshape(-1)[:vec_count]
        tensors = [from_tiles(t, g.shape[-1]).reshape(g.shape[1:]) for t, g in zip(tiles[:4], (g_embed, g_attn, g_ffn_in, g_ffn_out))]

        block = vec_count // 8
        vec_block = lax.dynamic_slice(vec.astype(jnp.float32), (device // 2 * block,), (block,))
        vec_block = jnp.pad(vec_block, (0, 16 * LANES - block)).reshape(16, LANES)
        chip = pl.pallas_call(
            chip_kernel, out_shape=jax.ShapeDtypeStruct((CHIP_ROWS, LANES), jnp.float32),
            in_specs=[any_spec] * 4 + [vmem], out_specs=vmem,
            scratch_shapes=[pltpu.VMEM((13824, LANES), jnp.bfloat16), pltpu.SemaphoreType.DMA((4,))])(*tiles[:4], vec_block)
        w_chip = chip.reshape(1, -1)[:, :13824 * LANES + block].astype(jnp.bfloat16)
        return (m_new, v_new, w_new) + tuple(tensors) + (vec[None], w_chip)

    return jax.shard_map(local_step, mesh=mesh, in_specs=(P(MESH_AXES),) * 8, out_specs=(P(MESH_AXES),) * 3 + (P(),) * 5 + (P(MESH_AXES),), check_vma=False)
```

```python
import functools
import math
import jax
import jax.numpy as jnp
from jax import lax
from jax.experimental import pallas as pl
from jax.experimental.pallas import tpu as pltpu
from jax.sharding import PartitionSpec as P

MESH_AXES = ('outer', 'middle', 'inner')
MESH = pl.DeviceIdType.MESH
ADAM_BETA1 = 0.9
ADAM_BETA2 = 0.98
ADAM_EPS = 1e-9
LEARN_RATE = 0.05
ADAM_STEP = 3

LANES = 128
SLICE = 885488
TENSORS = ((0, 32768, 8), (32768, 65536, 32), (65536, 88064, 22), (88064, 110592, 8), (110592, 110720, 1))
ROWS = 110720
UNIT = 128
WINDOW = 7296
THIRD = WINDOW // 3
ITEMS = THIRD // UNIT
EDGE = 32768
OWN = 7200
OWN_THIRD = OWN // 3
OWN_CHUNK = 160
OWN_ITEMS = OWN_THIRD // OWN_CHUNK
SIXTEEN = 16
FINAL_LIMIT = 20000000
GATHER_LIMIT = 6000000


def floor_block(row):
    result = row
    for base, end, tiles in TENSORS:
        block = 8 * tiles if tiles > 1 else UNIT
        floored = base + (row - base) // block * block
        result = jnp.where((row >= base) & (row < end), floored, result)
    return result


def window_start(index):
    row = floor_block(index * (SLICE // 16) // 8)
    return jnp.minimum(row // UNIT * UNIT, ROWS - WINDOW)


def own_start_static(index):
    row = -(-index * SLICE // LANES)
    for base, end, tiles in TENSORS:
        if base <= row < end:
            block = 8 * tiles if tiles > 1 else UNIT
            return base + -(-(row - base) // block) * block
    return ROWS


OWN_STARTS = [own_start_static(d) for d in range(SIXTEEN)] + [ROWS]


def own_start(index):
    result = jnp.int32(0)
    for d in range(SIXTEEN):
        result = jnp.where(index == d, OWN_STARTS[d], result)
    return result


def adam_update(grad_mean, m_old, v_old, w_old):
    m_new = ADAM_BETA1 * m_old + (1.0 - ADAM_BETA1) * grad_mean
    v_new = ADAM_BETA2 * v_old + (1.0 - ADAM_BETA2) * (grad_mean * grad_mean)
    m_hat = m_new / (1.0 - ADAM_BETA1 ** ADAM_STEP)
    v_hat = v_new / (1.0 - ADAM_BETA2 ** ADAM_STEP)
    w_new = w_old - LEARN_RATE * m_hat / (jnp.sqrt(v_hat) + ADAM_EPS)
    return m_new, v_new, w_new


def to_tiles(tensor):
    rows, width = tensor.shape
    return tensor.reshape(rows // 8, 8, width // LANES, LANES).transpose(0, 2, 1, 3).reshape(-1, LANES)


def from_tiles(tiles, width):
    return tiles.reshape(-1, width // LANES, 8, LANES).transpose(0, 2, 1, 3).reshape(-1, width)


ORDERS = ((0, 1, 2), (1, 2, 0), (2, 0, 1))


def position():
    outer, middle, inner = (lax.axis_index(name) for name in MESH_AXES)
    return outer, middle, inner // 2, inner % 2


def neighbour(axis):
    outer, middle, x, core = position()
    z, y = outer, middle
    if axis == 0:
        z = 1 - z
    elif axis == 1:
        y = 1 - y
    elif axis == 2:
        x = 1 - x
    else:
        core = 1 - core
    return (z, y, 2 * x + core)


def scatter_kernel(e_ref, a_ref, f_ref, h_ref, b_ref, m_ref, v_ref, w_ref, out_ref, edge_ref,
                   part, recv0, recv1, recv2, mine, pair_send, pair_recv, mine_sem,
                   send0, send1, send2, arrive0, arrive1, arrive2, out_sem, edge_send, edge_recv):
    z, y, x, core = position()
    chip = (z * 2 + y) * 2 + x
    device = chip * 2 + core
    sources = (e_ref, a_ref, f_ref, h_ref, b_ref)

    before = (device + SIXTEEN - 1) % SIXTEEN
    for n, ref in enumerate((m_ref, v_ref, w_ref)):
        pltpu.make_async_remote_copy(
            src_ref=ref.at[pl.ds(0, EDGE)], dst_ref=edge_ref.at[pl.ds(n * EDGE, EDGE)],
            send_sem=edge_send.at[n], recv_sem=edge_recv.at[n],
            device_id=(before // 8, before // 4 % 2, before % 4), device_id_type=MESH).start()

    def from_source(row, action):
        for source, (base, end, _) in zip(sources, TENSORS):
            @pl.when((row >= base) & (row < end))
            def _():
                action(source.at[pl.ds(pl.multiple_of(row - base, UNIT), UNIT), :])

    def item_row(third, item):
        return pl.multiple_of(third * THIRD + item * UNIT, UNIT)

    def start_pair(item):
        @pl.loop(0, 8)
        def _(j):
            jz, jy, jx = j // 4, j // 2 % 2, j % 2
            other = ((z + jz) % 2 * 2 + (y + jy) % 2) * 2 + (x + jx) % 2
            start = window_start(other * 2 + 1 - core)
            for third in range(3):
                row = item_row(third, item)
                from_source(start + row, lambda src: pltpu.make_async_remote_copy(
                    src_ref=src, dst_ref=part.at[jz, jy, jx, pl.ds(row, UNIT), :],
                    send_sem=pair_send.at[third, item], recv_sem=pair_recv.at[third, item],
                    device_id=neighbour(3), device_id_type=MESH).start())

    def start_mine(item, slot):
        @pl.loop(0, 8)
        def _(j):
            jz, jy, jx = j // 4, j // 2 % 2, j % 2
            other = ((z + jz) % 2 * 2 + (y + jy) % 2) * 2 + (x + jx) % 2
            start = window_start(other * 2 + core)
            for third in range(3):
                row = item_row(third, item)
                from_source(start + row, lambda src: pltpu.make_async_copy(
                    src, mine.at[slot, third, jz, jy, jx], mine_sem.at[slot]).start())

    def hop_copy(third, item, hop):
        rows = pl.ds(item_row(third, item), UNIT)
        first, second, last = ORDERS[third]
        if hop == 0:
            index = tuple(1 if n == first else slice(None) for n in range(3))
            target = recv0.at[:, :, rows, :]
        elif hop == 1:
            index = tuple(0 if n == first else 1 if n == second else slice(None) for n in range(3))
            target = recv1.at[:, rows, :]
        else:
            index = tuple(1 if n == last else 0 for n in range(3))
            target = recv2.at[rows, :]
        return pltpu.make_async_remote_copy(
            src_ref=part.at[index + (rows, slice(None))], dst_ref=target,
            send_sem=(send0, send1, send2)[hop].at[third, item], recv_sem=(arrive0, arrive1, arrive2)[hop].at[third, item],
            device_id=neighbour(ORDERS[third][hop]), device_id_type=MESH)

    def pair_all(third, item):
        block = part.at[:, :, :, pl.ds(item_row(third, item), UNIT), :]
        return pltpu.make_async_remote_copy(
            src_ref=block, dst_ref=block, send_sem=pair_send.at[third, item], recv_sem=pair_recv.at[third, item],
            device_id=neighbour(3), device_id_type=MESH)

    def out_copy(third, item):
        rows = pl.ds(item_row(third, item), UNIT)
        return pltpu.make_async_copy(part.at[0, 0, 0, rows, :], out_ref.at[rows, :], out_sem.at[third, item])

    start_mine(0, 0)
    start_pair(0)
    start_pair(1)

    @pl.loop(0, ITEMS + 4)
    def _(step):
        @pl.when(step < ITEMS)
        def _():
            slot = step % 2

            @pl.when(step + 1 < ITEMS)
            def _():
                start_mine(step + 1, 1 - slot)

            @pl.when(step + 2 < ITEMS)
            def _():
                start_pair(step + 2)

            pltpu.make_async_copy(mine.at[slot], mine.at[slot], mine_sem.at[slot]).wait()
            for third in range(3):
                rows = pl.ds(item_row(third, step), UNIT)
                pair_all(third, step).wait_recv()
                for j in range(8):
                    index = (j // 4, j // 2 % 2, j % 2)
                    part[index + (rows, slice(None))] += mine[(slot, third) + index]
                hop_copy(third, step, 0).start()

        @pl.when((step >= 1) & (step < ITEMS + 1))
        def _():
            item = step - 1
            for third in range(3):
                rows = pl.ds(item_row(third, item), UNIT)
                hop_copy(third, item, 0).wait_recv()
                first = ORDERS[third][0]
                for j in range(4):
                    pair = [j // 2, j % 2]
                    index = tuple(pair[:first] + [0] + pair[first:])
                    part[index + (rows, slice(None))] += recv0[j // 2, j % 2, rows, :]
                hop_copy(third, item, 1).start()

        @pl.when((step >= 2) & (step < ITEMS + 2))
        def _():
            item = step - 2
            for third in range(3):
                rows = pl.ds(item_row(third, item), UNIT)
                hop_copy(third, item, 1).wait_recv()
                last = ORDERS[third][2]
                for j in range(2):
                    index = tuple(j if n == last else 0 for n in range(3))
                    part[index + (rows, slice(None))] += recv1[j, rows, :]
                hop_copy(third, item, 2).start()

        @pl.when((step >= 3) & (step < ITEMS + 3))
        def _():
            item = step - 3
            for third in range(3):
                rows = pl.ds(item_row(third, item), UNIT)
                hop_copy(third, item, 2).wait_recv()
                part[0, 0, 0, rows, :] = (part[0, 0, 0, rows, :] + recv2[rows, :]) / SIXTEEN

        @pl.when(step >= 4)
        def _():
            for third in range(3):
                out_copy(third, step - 4).start()

    @pl.loop(0, ITEMS)
    def _(item):
        for third in range(3):
            pair_all(third, item).wait_send()
            for hop in range(3):
                hop_copy(third, item, hop).wait_send()
            out_copy(third, item).wait()

    for n, ref in enumerate((m_ref, v_ref, w_ref)):
        pltpu.make_async_remote_copy(
            src_ref=ref.at[pl.ds(0, EDGE)], dst_ref=edge_ref.at[pl.ds(n * EDGE, EDGE)],
            send_sem=edge_send.at[n], recv_sem=edge_recv.at[n],
            device_id=(before // 8, before // 4 % 2, before % 4), device_id_type=MESH).wait()


def scatter(grads, m, v, w):
    any_spec = pl.BlockSpec(memory_space=pl.ANY)
    dma = pltpu.SemaphoreType.DMA
    return pl.pallas_call(
        scatter_kernel,
        out_shape=(jax.ShapeDtypeStruct((WINDOW, LANES), jnp.float32), jax.ShapeDtypeStruct((3 * EDGE,), jnp.float32)),
        in_specs=[any_spec] * 8,
        out_specs=(any_spec, any_spec),
        scratch_shapes=[
            pltpu.VMEM((2, 2, 2, WINDOW, LANES), jnp.float32),
            pltpu.VMEM((2, 2, WINDOW, LANES), jnp.float32),
            pltpu.VMEM((2, WINDOW, LANES), jnp.float32),
            pltpu.VMEM((WINDOW, LANES), jnp.float32),
            pltpu.VMEM((2, 3, 2, 2, 2, UNIT, LANES), jnp.float32),
            dma((3, ITEMS)), dma((3, ITEMS)), dma((2,)),
            dma((3, ITEMS)), dma((3, ITEMS)), dma((3, ITEMS)),
            dma((3, ITEMS)), dma((3, ITEMS)), dma((3, ITEMS)),
            dma((3, ITEMS)), dma((3,)), dma((3,)),
        ],
        compiler_params=pltpu.CompilerParams(has_side_effects=True, vmem_limit_bytes=67043328),
    )(*grads, m, v, w)


def gather_kernel(w_ref, full_ref, pair_send, pair_recv, send, arrive, own_sem):
    z, y, x, core = position()
    here = (z, y, x)

    def rows_of(third, item):
        return pl.ds(pl.multiple_of(third * OWN_THIRD + item * OWN_CHUNK, OWN_CHUNK), OWN_CHUNK)

    own = pltpu.make_async_copy(w_ref, full_ref.at[z, y, x, core], own_sem)
    own.start()

    def copy(third, item, hop):
        rows = rows_of(third, item)
        order = ORDERS[third]
        if hop == 0:
            source = w_ref.at[rows, :]
            target = full_ref.at[z, y, x, core, rows, :]
        else:
            index = tuple(slice(None) if n in order[:hop] else here[n] for n in range(3))
            source = target = full_ref.at[index + (core, rows, slice(None))]
        return pltpu.make_async_remote_copy(
            src_ref=source, dst_ref=target, send_sem=send.at[third, item, hop], recv_sem=arrive.at[third, item, hop],
            device_id=neighbour(order[hop]), device_id_type=MESH)

    def arrival(third, item, hop):
        rows = rows_of(third, item)
        order = ORDERS[third]
        index = tuple(slice(None) if n in order[:hop] else (1 - here[n] if n == order[hop] else here[n]) for n in range(3))
        block = full_ref.at[index + (core, rows, slice(None))]
        return pltpu.make_async_remote_copy(
            src_ref=block, dst_ref=block, send_sem=send.at[third, item, hop], recv_sem=arrive.at[third, item, hop],
            device_id=neighbour(order[hop]), device_id_type=MESH)

    def pair(third, item, side):
        block = full_ref.at[:, :, :, side, rows_of(third, item), :]
        return pltpu.make_async_remote_copy(
            src_ref=block, dst_ref=block, send_sem=pair_send.at[third, item], recv_sem=pair_recv.at[third, item],
            device_id=neighbour(3), device_id_type=MESH)

    for third in range(3):
        copy(third, 0, 0).start()
    own.wait()

    @pl.loop(0, OWN_ITEMS + 3)
    def _(step):
        @pl.when(step + 1 < OWN_ITEMS)
        def _():
            for third in range(3):
                copy(third, step + 1, 0).start()

        for hop in range(1, 4):
            @pl.when((step >= hop - 1) & (step < OWN_ITEMS + hop - 1))
            def _():
                item = step - (hop - 1)
                for third in range(3):
                    arrival(third, item, hop - 1).wait_recv()
                    if hop < 3:
                        copy(third, item, hop).start()
                    else:
                        pair(third, item, core).start()

    @pl.loop(0, OWN_ITEMS)
    def _(item):
        for third in range(3):
            pair(third, item, 1 - core).wait_recv()
            pair(third, item, core).wait_send()
            for hop in range(3):
                copy(third, item, hop).wait_send()


def gather(w_own):
    dma = pltpu.SemaphoreType.DMA
    return pl.pallas_call(
        gather_kernel,
        out_shape=jax.ShapeDtypeStruct((2, 2, 2, 2, OWN, LANES), jnp.bfloat16),
        in_specs=[pl.BlockSpec(memory_space=pltpu.VMEM)],
        out_specs=pl.BlockSpec(memory_space=pltpu.VMEM),
        scratch_shapes=[
            dma((3, OWN_ITEMS)), dma((3, OWN_ITEMS)), dma((3, OWN_ITEMS, 3)), dma((3, OWN_ITEMS, 3)), dma(()),
        ],
        compiler_params=pltpu.CompilerParams(has_side_effects=True, vmem_limit_bytes=GATHER_LIMIT),
    )(w_own)


def device_index():
    outer, middle, inner = (lax.axis_index(name) for name in MESH_AXES)
    return (outer * 2 + middle) * 4 + inner


def for_blocks(start, length, action):
    for base, end, tiles in TENSORS:
        block = 8 * tiles
        low = (jnp.maximum(start, base) - base + block - 1) // block
        high = jnp.maximum(jnp.minimum(start + length, end) - base, 0) // block

        @pl.loop(low, jnp.maximum(high, low))
        def _(n):
            action(pl.multiple_of(base + n * block - start, 8), tiles)


PAD = 8
FLAT_ROWS = WINDOW + 272
SHARD_VREGS = SLICE // 1024
TAIL_ROWS = SLICE % 1024 // LANES
TAIL_LANES = SLICE % LANES
EDGE_ROWS = EDGE // LANES
OWN_FLAT_ROWS = OWN + 512


def lane_index():
    return lax.broadcasted_iota(jnp.int32, (8, LANES), 1)


def mid_kernel(tile_ref, m_ref, v_ref, w_ref, edge_ref, m_out, v_out, w_out, own_ref, flat, shifted, edged, aligned, tiled):
    device = device_index()
    start = window_start(device)

    def to_flat(row, tiles):
        for t in range(tiles):
            flat[pl.ds(row + t, 8, stride=tiles), :] = tile_ref[pl.ds(row + 8 * t, 8), :]
    for_blocks(start, WINDOW, to_flat)

    first_row = device * (SLICE // 16) // 8
    next_row = (device + 1) * (SLICE // 16) // 8
    shift = device * SLICE - first_row * LANES
    next_shift = (device + 1) * SLICE - next_row * LANES
    lane = lane_index()

    def mean_rows(row, amount):
        here = flat[pl.ds(row, 8), :]
        below = flat[pl.ds(row + 1, 8), :]
        back = (LANES - amount) % LANES
        return jnp.where(lane < LANES - amount, pltpu.roll(here, back, 1), pltpu.roll(below, back, 1))

    def shard_step(n):
        at = pl.ds(pl.multiple_of(n * 1024, 1024), 1024)
        mean = mean_rows(first_row - start + n * 8, shift)
        m_new, v_new, w_new = adam_update(mean, *(ref[at].reshape(8, LANES) for ref in (m_ref, v_ref, w_ref)))
        m_out[at] = m_new.reshape(1024)
        v_out[at] = v_new.reshape(1024)
        w_out[at] = w_new.reshape(1024)
        shifted[pl.ds(pl.multiple_of(PAD + n * 8, 8), 8), :] = pltpu.roll(w_new, shift, 1)

    @pl.loop(0, SHARD_VREGS // 4)
    def _(n):
        for k in range(4):
            shard_step(n * 4 + k)
    for n in range(SHARD_VREGS // 4 * 4, SHARD_VREGS):
        shard_step(n)

    mean = mean_rows(first_row - start + SHARD_VREGS * 8, shift)
    for r in range(TAIL_ROWS + 1):
        size = LANES if r < TAIL_ROWS else TAIL_LANES
        at = pl.ds(SHARD_VREGS * 1024 + r * LANES, size)
        m_new, v_new, w_new = adam_update(
            mean[r:r + 1, :size], *(ref[at].reshape(1, size) for ref in (m_ref, v_ref, w_ref)))
        m_out[at] = m_new.reshape(size)
        v_out[at] = v_new.reshape(size)
        w_out[at] = w_new.reshape(size)
        flat[pl.ds(FLAT_ROWS - 8 + r, 1), pl.ds(0, size)] = w_new
    shifted[pl.ds(PAD + SHARD_VREGS * 8, 8), :] = pltpu.roll(flat[pl.ds(FLAT_ROWS - 8, 8), :], shift, 1)

    @pl.loop(0, EDGE_ROWS // 8)
    def _(n):
        mean = mean_rows(next_row - start + n * 8, next_shift)
        old = (edge_ref[pl.ds(pl.multiple_of(k * EDGE + n * 1024, 1024), 1024)].reshape(8, LANES) for k in range(3))
        edged[pl.ds(pl.multiple_of(PAD + n * 8, 8), 8), :] = pltpu.roll(adam_update(mean, *old)[2], next_shift, 1)

    own = own_start(device)
    skip = own - first_row

    @pl.loop(0, SHARD_VREGS + 1)
    def _(n):
        row = PAD + skip + n * 8
        aligned[pl.ds(pl.multiple_of(n * 8, 8), 8), :] = jnp.where(
            lane >= shift, shifted[pl.ds(row, 8), :], shifted[pl.ds(row - 1, 8), :])
    edged[pl.ds(PAD - 1, 1), :] = aligned[pl.ds(next_row - own, 1), :]

    @pl.loop(0, EDGE_ROWS // 8)
    def _(n):
        row = PAD + n * 8
        aligned[pl.ds(next_row - own + n * 8, 8), :] = jnp.where(
            lane >= next_shift, edged[pl.ds(row, 8), :], edged[pl.ds(row - 1, 8), :])

    def to_tile(row, tiles):
        for t in range(tiles):
            tiled[pl.ds(row + 8 * t, 8), :] = aligned[pl.ds(row + t, 8, stride=tiles), :]
    for_blocks(own, OWN, to_tile)

    @pl.loop(0, OWN // 32)
    def _(n):
        rows = pl.ds(pl.multiple_of(n * 32, 32), 32)
        own_ref[rows, :] = tiled[rows, :].astype(jnp.bfloat16)


def mid(mean_tiles, m, v, w, edges):
    vmem = pl.BlockSpec(memory_space=pltpu.VMEM)
    shard = jax.ShapeDtypeStruct((SLICE,), jnp.float32)
    return pl.pallas_call(
        mid_kernel,
        out_shape=(shard, shard, shard, jax.ShapeDtypeStruct((OWN, LANES), jnp.bfloat16)),
        in_specs=[vmem] * 5, out_specs=(vmem,) * 4,
        scratch_shapes=[
            pltpu.VMEM((FLAT_ROWS, LANES), jnp.float32),
            pltpu.VMEM((PAD + SHARD_VREGS * 8 + 8 + 512, LANES), jnp.float32),
            pltpu.VMEM((PAD + EDGE_ROWS, LANES), jnp.float32),
            pltpu.VMEM((OWN_FLAT_ROWS, LANES), jnp.float32),
            pltpu.VMEM((OWN, LANES), jnp.float32),
        ],
        compiler_params=pltpu.CompilerParams(vmem_limit_bytes=60000000),
    )(mean_tiles, m, v, w, edges)


def pieces_of(tensor):
    base, end, _ = TENSORS[tensor]
    for d in range(SIXTEEN):
        low, high = max(OWN_STARTS[d], base), min(OWN_STARTS[d + 1], end)
        if low < high:
            yield d, low - OWN_STARTS[d], low - base, high - low


PIECES = [(tensor,) + piece for tensor in range(4) for piece in pieces_of(tensor)]
VEC_WIDTH = 12032
VEC_ROWS = VEC_WIDTH // LANES
VEC_BLOCK = VEC_WIDTH // 8
CHIP_COUNTS = tuple((end - base) // 8 for base, end, _ in TENSORS[:4])
CHIP_ROWS = sum(CHIP_COUNTS)
CHIP_SIZE = CHIP_ROWS * LANES + VEC_BLOCK


def final_kernel(full_ref, e_out, a_out, f_out, h_out, vec_out, chip_out, block, flat, vec, out_sem, block_sem):
    outs = (e_out, a_out, f_out, h_out)
    chip = device_index() // 2
    copies = []
    for n, (tensor, d, source, target, rows) in enumerate(PIECES):
        copies.append(pltpu.make_async_copy(
            full_ref.at[d, pl.ds(source, rows), :], outs[tensor].at[pl.ds(target, rows), :], out_sem.at[n]))
        copies[-1].start()

    slot, source, _, _ = next(pieces_of(4))
    vec[pl.ds(0, 96), :] = full_ref[slot, pl.ds(source, 96), :].astype(jnp.float32)
    for n in range(VEC_ROWS // 8):
        vec_out[:, n * 1024:(n + 1) * 1024] = vec[n * 8:n * 8 + 8, :].reshape(1, 1024).astype(jnp.bfloat16)
    rest = VEC_ROWS % 8
    vec_out[:, VEC_ROWS // 8 * 1024:] = vec[pl.ds(VEC_ROWS - rest, rest), :].reshape(1, rest * LANES).astype(jnp.bfloat16)

    offset = 0
    for tensor, rows in enumerate(CHIP_COUNTS):
        base, _, tiles = TENSORS[tensor]
        step = 16 * tiles

        @pl.loop(0, rows // step)
        def _(n):
            row = base + chip * rows + n * step
            slot = jnp.int32(0)
            low = jnp.int32(0)
            for d in range(1, SIXTEEN):
                slot = jnp.where(row >= OWN_STARTS[d], d, slot)
                low = jnp.where(row >= OWN_STARTS[d], OWN_STARTS[d], low)
            second = row + 8 * tiles
            slot2 = jnp.int32(0)
            low2 = jnp.int32(0)
            for d in range(1, SIXTEEN):
                slot2 = jnp.where(second >= OWN_STARTS[d], d, slot2)
                low2 = jnp.where(second >= OWN_STARTS[d], OWN_STARTS[d], low2)
            for half, (at_slot, at_row) in enumerate(((slot, row - low), (slot2, second - low2))):
                for t in range(0, tiles, 2):
                    value = full_ref[at_slot, pl.ds(pl.multiple_of(at_row + 8 * t, 16), 16), :].astype(jnp.float32)
                    for k in range(2):
                        to = offset + n * step + half * 8 * tiles + t + k
                        flat[pl.ds(to, 8, stride=tiles), :] = value[8 * k:8 * k + 8]
        offset += rows

    vec_row = chip * (VEC_BLOCK // 32) // 4
    amount = chip * VEC_BLOCK - vec_row * LANES
    back = (LANES - amount) % LANES
    lane = lane_index()
    for n in range(2):
        here, below = vec[pl.ds(vec_row + n * 8, 8), :], vec[pl.ds(vec_row + n * 8 + 1, 8), :]
        flat[pl.ds(CHIP_ROWS + n * 8, 8), :] = jnp.where(
            lane < LANES - amount, pltpu.roll(here, back, 1), pltpu.roll(below, back, 1))

    @pl.loop(0, CHIP_SIZE // 4096)
    def _(n):
        for k in range(4):
            chip_out[:, pl.ds(pl.multiple_of(n * 4096 + k * 1024, 1024), 1024)] = flat[
                pl.ds(pl.multiple_of(n * 32 + k * 8, 8), 8), :].reshape(1, 1024).astype(jnp.bfloat16)
    for n in range(CHIP_SIZE // 4096 * 4, CHIP_SIZE // 1024):
        chip_out[:, n * 1024:(n + 1) * 1024] = flat[n * 8:n * 8 + 8, :].reshape(1, 1024).astype(jnp.bfloat16)
    done = CHIP_SIZE // 1024 * 1024
    rows = (CHIP_SIZE - done) // LANES
    last = CHIP_SIZE - done - rows * LANES
    first = done // LANES
    chip_out[:, done:done + rows * LANES] = flat[first:first + rows, :].reshape(1, rows * LANES).astype(jnp.bfloat16)
    chip_out[:, CHIP_SIZE - last:] = flat[first + rows:first + rows + 1, :last].astype(jnp.bfloat16)

    for copy in copies:
        copy.wait()


def finish(full):
    vmem = pl.BlockSpec(memory_space=pltpu.VMEM)
    any_spec = pl.BlockSpec(memory_space=pl.ANY)
    shape = lambda rows: jax.ShapeDtypeStruct((rows, LANES), jnp.bfloat16)
    return pl.pallas_call(
        final_kernel,
        out_shape=tuple(shape(end - base) for base, end, _ in TENSORS[:4]) + (
            jax.ShapeDtypeStruct((1, VEC_WIDTH), jnp.bfloat16), jax.ShapeDtypeStruct((1, CHIP_SIZE), jnp.bfloat16)),
        in_specs=[vmem], out_specs=(any_spec,) * 4 + (vmem, vmem),
        scratch_shapes=[
            pltpu.VMEM((16, LANES), jnp.bfloat16),
            pltpu.VMEM((CHIP_ROWS + 16, LANES), jnp.float32),
            pltpu.VMEM((120, LANES), jnp.float32),
            pltpu.SemaphoreType.DMA((len(PIECES),)), pltpu.SemaphoreType.DMA(()),
        ],
        compiler_params=pltpu.CompilerParams(vmem_limit_bytes=FINAL_LIMIT),
    )(full)


def solution(mesh):
    def local_step(g_embed, g_attn, g_ffn_in, g_ffn_out, g_vec, m_shard, v_shard, w_shard):
        matrices = (g_embed, g_attn, g_ffn_in, g_ffn_out)
        grads = [to_tiles(g[0] if g.ndim == 3 else g[0, 0]) for g in matrices]
        grads.append(jnp.pad(g_vec.reshape(-1), (0, UNIT * LANES - VEC_WIDTH)).reshape(UNIT, LANES))
        mean_tiles, edges = scatter(grads, m_shard, v_shard, w_shard)
        m_new, v_new, w_new, w_own = mid(mean_tiles, m_shard, v_shard, w_shard, edges)
        full = gather(w_own).reshape(SIXTEEN, OWN, LANES)
        *tiles, vec, w_chip = finish(full)
        tensors = [from_tiles(t, g.shape[-1]).reshape(g.shape[1:]) for t, g in zip(tiles, matrices)]
        return (m_new, v_new, w_new) + tuple(tensors) + (vec, w_chip)

    return jax.shard_map(local_step, mesh=mesh, in_specs=(P(MESH_AXES),) * 8, out_specs=(P(MESH_AXES),) * 3 + (P(),) * 5 + (P(MESH_AXES),), check_vma=False)
```

```python
import functools
import math
import jax
import jax.numpy as jnp
from jax import lax
from jax.experimental import pallas as pl
from jax.experimental.pallas import tpu as pltpu
from jax.sharding import PartitionSpec as P

MESH_AXES = ('outer', 'middle', 'inner')
MESH = pl.DeviceIdType.MESH
ADAM_BETA1 = 0.9
ADAM_BETA2 = 0.98
ADAM_EPS = 1e-9
LEARN_RATE = 0.05
ADAM_STEP = 3

LANES = 128
SLICE = 885488
TENSORS = ((0, 32768, 8), (32768, 65536, 32), (65536, 88064, 22), (88064, 110592, 8), (110592, 110720, 1))
ROWS = 110720
UNIT = 128
WINDOW = 7296
THIRD = WINDOW // 3
ITEMS = THIRD // UNIT
EDGE = 32768
OWN = 7200
OWN_THIRD = OWN // 3
OWN_CHUNK = 160
OWN_ITEMS = OWN_THIRD // OWN_CHUNK
SIXTEEN = 16
FINAL_LIMIT = 20000000
GATHER_LIMIT = 36000000
MID_LIMIT = 64000000


def floor_block(row):
    result = row
    for base, end, tiles in TENSORS:
        block = 8 * tiles if tiles > 1 else UNIT
        floored = base + (row - base) // block * block
        result = jnp.where((row >= base) & (row < end), floored, result)
    return result


def window_start(index):
    row = floor_block(index * (SLICE // 16) // 8)
    return jnp.minimum(row // UNIT * UNIT, ROWS - WINDOW)


def own_start_static(index):
    row = -(-index * SLICE // LANES)
    for base, end, tiles in TENSORS:
        if base <= row < end:
            block = 8 * tiles if tiles > 1 else UNIT
            return base + -(-(row - base) // block) * block
    return ROWS


OWN_STARTS = [own_start_static(d) for d in range(SIXTEEN)] + [ROWS]


def own_start(index):
    result = jnp.int32(0)
    for d in range(SIXTEEN):
        result = jnp.where(index == d, OWN_STARTS[d], result)
    return result


def adam_update(grad_mean, m_old, v_old, w_old):
    m_new = ADAM_BETA1 * m_old + (1.0 - ADAM_BETA1) * grad_mean
    v_new = ADAM_BETA2 * v_old + (1.0 - ADAM_BETA2) * (grad_mean * grad_mean)
    scale = LEARN_RATE / (1.0 - ADAM_BETA1 ** ADAM_STEP)
    w_new = w_old - scale * m_new / (jnp.sqrt(v_new * (1.0 / (1.0 - ADAM_BETA2 ** ADAM_STEP))) + ADAM_EPS)
    return m_new, v_new, w_new


def to_tiles(tensor):
    rows, width = tensor.shape
    return tensor.reshape(rows // 8, 8, width // LANES, LANES).transpose(0, 2, 1, 3).reshape(-1, LANES)


def from_tiles(tiles, width):
    return tiles.reshape(-1, width // LANES, 8, LANES).transpose(0, 2, 1, 3).reshape(-1, width)


ORDERS = ((0, 1, 2), (1, 2, 0), (2, 0, 1))


def position():
    outer, middle, inner = (lax.axis_index(name) for name in MESH_AXES)
    return outer, middle, inner // 2, inner % 2


def neighbour(axis):
    outer, middle, x, core = position()
    z, y = outer, middle
    if axis == 0:
        z = 1 - z
    elif axis == 1:
        y = 1 - y
    elif axis == 2:
        x = 1 - x
    else:
        core = 1 - core
    return (z, y, 2 * x + core)


def scatter_kernel(e_ref, a_ref, f_ref, h_ref, b_ref, m_ref, v_ref, w_ref, out_ref, edge_ref,
                   part, recv0, recv1, recv2, mine, pair_send, pair_recv, mine_sem,
                   send0, send1, send2, arrive0, arrive1, arrive2, out_sem, edge_send, edge_recv):
    z, y, x, core = position()
    chip = (z * 2 + y) * 2 + x
    device = chip * 2 + core
    sources = (e_ref, a_ref, f_ref, h_ref, b_ref)

    before = (device + SIXTEEN - 1) % SIXTEEN
    for n, ref in enumerate((m_ref, v_ref, w_ref)):
        pltpu.make_async_remote_copy(
            src_ref=ref.at[pl.ds(0, EDGE)], dst_ref=edge_ref.at[pl.ds(n * EDGE, EDGE)],
            send_sem=edge_send.at[n], recv_sem=edge_recv.at[n],
            device_id=(before // 8, before // 4 % 2, before % 4), device_id_type=MESH).start()

    def from_source(row, action):
        for source, (base, end, _) in zip(sources, TENSORS):
            @pl.when((row >= base) & (row < end))
            def _():
                action(source.at[pl.ds(pl.multiple_of(row - base, UNIT), UNIT), :])

    def item_row(third, item):
        return pl.multiple_of(third * THIRD + item * UNIT, UNIT)

    def start_pair(item):
        @pl.loop(0, 8)
        def _(j):
            jz, jy, jx = j // 4, j // 2 % 2, j % 2
            other = ((z + jz) % 2 * 2 + (y + jy) % 2) * 2 + (x + jx) % 2
            start = window_start(other * 2 + 1 - core)
            for third in range(3):
                row = item_row(third, item)
                from_source(start + row, lambda src: pltpu.make_async_remote_copy(
                    src_ref=src, dst_ref=part.at[jz, jy, jx, pl.ds(row, UNIT), :],
                    send_sem=pair_send.at[third, item], recv_sem=pair_recv.at[third, item],
                    device_id=neighbour(3), device_id_type=MESH).start())

    def start_mine(item, slot):
        @pl.loop(0, 8)
        def _(j):
            jz, jy, jx = j // 4, j // 2 % 2, j % 2
            other = ((z + jz) % 2 * 2 + (y + jy) % 2) * 2 + (x + jx) % 2
            start = window_start(other * 2 + core)
            for third in range(3):
                row = item_row(third, item)
                from_source(start + row, lambda src: pltpu.make_async_copy(
                    src, mine.at[slot, third, jz, jy, jx], mine_sem.at[slot]).start())

    def hop_copy(third, item, hop):
        rows = pl.ds(item_row(third, item), UNIT)
        first, second, last = ORDERS[third]
        if hop == 0:
            index = tuple(1 if n == first else slice(None) for n in range(3))
            target = recv0.at[:, :, rows, :]
        elif hop == 1:
            index = tuple(0 if n == first else 1 if n == second else slice(None) for n in range(3))
            target = recv1.at[:, rows, :]
        else:
            index = tuple(1 if n == last else 0 for n in range(3))
            target = recv2.at[rows, :]
        return pltpu.make_async_remote_copy(
            src_ref=part.at[index + (rows, slice(None))], dst_ref=target,
            send_sem=(send0, send1, send2)[hop].at[third, item], recv_sem=(arrive0, arrive1, arrive2)[hop].at[third, item],
            device_id=neighbour(ORDERS[third][hop]), device_id_type=MESH)

    def pair_all(third, item):
        block = part.at[:, :, :, pl.ds(item_row(third, item), UNIT), :]
        return pltpu.make_async_remote_copy(
            src_ref=block, dst_ref=block, send_sem=pair_send.at[third, item], recv_sem=pair_recv.at[third, item],
            device_id=neighbour(3), device_id_type=MESH)

    def out_copy(third, item):
        rows = pl.ds(item_row(third, item), UNIT)
        return pltpu.make_async_copy(part.at[0, 0, 0, rows, :], out_ref.at[rows, :], out_sem.at[third, item])

    start_mine(0, 0)
    start_pair(0)
    start_pair(1)

    @pl.loop(0, ITEMS + 4)
    def _(step):
        @pl.when(step < ITEMS)
        def _():
            slot = step % 2

            @pl.when(step + 1 < ITEMS)
            def _():
                start_mine(step + 1, 1 - slot)

            @pl.when(step + 2 < ITEMS)
            def _():
                start_pair(step + 2)

            pltpu.make_async_copy(mine.at[slot], mine.at[slot], mine_sem.at[slot]).wait()
            for third in range(3):
                rows = pl.ds(item_row(third, step), UNIT)
                pair_all(third, step).wait_recv()
                for j in range(8):
                    index = (j // 4, j // 2 % 2, j % 2)
                    part[index + (rows, slice(None))] += mine[(slot, third) + index]
                hop_copy(third, step, 0).start()

        @pl.when((step >= 1) & (step < ITEMS + 1))
        def _():
            item = step - 1
            for third in range(3):
                rows = pl.ds(item_row(third, item), UNIT)
                hop_copy(third, item, 0).wait_recv()
                first = ORDERS[third][0]
                for j in range(4):
                    pair = [j // 2, j % 2]
                    index = tuple(pair[:first] + [0] + pair[first:])
                    part[index + (rows, slice(None))] += recv0[j // 2, j % 2, rows, :]
                hop_copy(third, item, 1).start()

        @pl.when((step >= 2) & (step < ITEMS + 2))
        def _():
            item = step - 2
            for third in range(3):
                rows = pl.ds(item_row(third, item), UNIT)
                hop_copy(third, item, 1).wait_recv()
                last = ORDERS[third][2]
                for j in range(2):
                    index = tuple(j if n == last else 0 for n in range(3))
                    part[index + (rows, slice(None))] += recv1[j, rows, :]
                hop_copy(third, item, 2).start()

        @pl.when((step >= 3) & (step < ITEMS + 3))
        def _():
            item = step - 3
            for third in range(3):
                rows = pl.ds(item_row(third, item), UNIT)
                hop_copy(third, item, 2).wait_recv()
                part[0, 0, 0, rows, :] = (part[0, 0, 0, rows, :] + recv2[rows, :]) / SIXTEEN

        @pl.when(step >= 4)
        def _():
            for third in range(3):
                out_copy(third, step - 4).start()

    @pl.loop(0, ITEMS)
    def _(item):
        for third in range(3):
            pair_all(third, item).wait_send()
            for hop in range(3):
                hop_copy(third, item, hop).wait_send()
            out_copy(third, item).wait()

    for n, ref in enumerate((m_ref, v_ref, w_ref)):
        pltpu.make_async_remote_copy(
            src_ref=ref.at[pl.ds(0, EDGE)], dst_ref=edge_ref.at[pl.ds(n * EDGE, EDGE)],
            send_sem=edge_send.at[n], recv_sem=edge_recv.at[n],
            device_id=(before // 8, before // 4 % 2, before % 4), device_id_type=MESH).wait()


def scatter(grads, m, v, w):
    any_spec = pl.BlockSpec(memory_space=pl.ANY)
    dma = pltpu.SemaphoreType.DMA
    return pl.pallas_call(
        scatter_kernel,
        out_shape=(jax.ShapeDtypeStruct((WINDOW, LANES), jnp.float32), jax.ShapeDtypeStruct((3 * EDGE,), jnp.float32)),
        in_specs=[any_spec] * 8,
        out_specs=(any_spec, any_spec),
        scratch_shapes=[
            pltpu.VMEM((2, 2, 2, WINDOW, LANES), jnp.float32),
            pltpu.VMEM((2, 2, WINDOW, LANES), jnp.float32),
            pltpu.VMEM((2, WINDOW, LANES), jnp.float32),
            pltpu.VMEM((WINDOW, LANES), jnp.float32),
            pltpu.VMEM((2, 3, 2, 2, 2, UNIT, LANES), jnp.float32),
            dma((3, ITEMS)), dma((3, ITEMS)), dma((2,)),
            dma((3, ITEMS)), dma((3, ITEMS)), dma((3, ITEMS)),
            dma((3, ITEMS)), dma((3, ITEMS)), dma((3, ITEMS)),
            dma((3, ITEMS)), dma((3,)), dma((3,)),
        ],
        compiler_params=pltpu.CompilerParams(has_side_effects=True, vmem_limit_bytes=67043328),
    )(*grads, m, v, w)


def gather_kernel(w_ref, full_ref, pair_send, pair_recv, send, arrive, own_sem):
    z, y, x, core = position()
    here = (z, y, x)

    def rows_of(third, item):
        return pl.ds(pl.multiple_of(third * OWN_THIRD + item * OWN_CHUNK, OWN_CHUNK), OWN_CHUNK)

    own = pltpu.make_async_copy(w_ref, full_ref.at[z, y, x, core], own_sem)
    own.start()

    def copy(third, item, hop):
        rows = rows_of(third, item)
        order = ORDERS[third]
        if hop == 0:
            source = w_ref.at[rows, :]
            target = full_ref.at[z, y, x, core, rows, :]
        else:
            index = tuple(slice(None) if n in order[:hop] else here[n] for n in range(3))
            source = target = full_ref.at[index + (core, rows, slice(None))]
        return pltpu.make_async_remote_copy(
            src_ref=source, dst_ref=target, send_sem=send.at[third, item, hop], recv_sem=arrive.at[third, item, hop],
            device_id=neighbour(order[hop]), device_id_type=MESH)

    def arrival(third, item, hop):
        rows = rows_of(third, item)
        order = ORDERS[third]
        index = tuple(slice(None) if n in order[:hop] else (1 - here[n] if n == order[hop] else here[n]) for n in range(3))
        block = full_ref.at[index + (core, rows, slice(None))]
        return pltpu.make_async_remote_copy(
            src_ref=block, dst_ref=block, send_sem=send.at[third, item, hop], recv_sem=arrive.at[third, item, hop],
            device_id=neighbour(order[hop]), device_id_type=MESH)

    def pair(third, item, side):
        block = full_ref.at[:, :, :, side, rows_of(third, item), :]
        return pltpu.make_async_remote_copy(
            src_ref=block, dst_ref=block, send_sem=pair_send.at[third, item], recv_sem=pair_recv.at[third, item],
            device_id=neighbour(3), device_id_type=MESH)

    for third in range(3):
        copy(third, 0, 0).start()
    own.wait()

    @pl.loop(0, OWN_ITEMS + 3)
    def _(step):
        @pl.when(step + 1 < OWN_ITEMS)
        def _():
            for third in range(3):
                copy(third, step + 1, 0).start()

        for hop in range(1, 4):
            @pl.when((step >= hop - 1) & (step < OWN_ITEMS + hop - 1))
            def _():
                item = step - (hop - 1)
                for third in range(3):
                    arrival(third, item, hop - 1).wait_recv()
                    if hop < 3:
                        copy(third, item, hop).start()
                    else:
                        pair(third, item, core).start()

    @pl.loop(0, OWN_ITEMS)
    def _(item):
        for third in range(3):
            pair(third, item, 1 - core).wait_recv()
            pair(third, item, core).wait_send()
            for hop in range(3):
                copy(third, item, hop).wait_send()


def gather(w_own):
    dma = pltpu.SemaphoreType.DMA
    return pl.pallas_call(
        gather_kernel,
        out_shape=jax.ShapeDtypeStruct((2, 2, 2, 2, OWN, LANES), jnp.bfloat16),
        in_specs=[pl.BlockSpec(memory_space=pl.ANY)],
        out_specs=pl.BlockSpec(memory_space=pltpu.VMEM),
        scratch_shapes=[
            dma((3, OWN_ITEMS)), dma((3, OWN_ITEMS)), dma((3, OWN_ITEMS, 3)), dma((3, OWN_ITEMS, 3)), dma(()),
        ],
        compiler_params=pltpu.CompilerParams(has_side_effects=True, vmem_limit_bytes=GATHER_LIMIT),
    )(w_own)


def device_index():
    outer, middle, inner = (lax.axis_index(name) for name in MESH_AXES)
    return (outer * 2 + middle) * 4 + inner


def for_blocks(start, length, action, tensors=TENSORS):
    for base, end, tiles in tensors:
        block = 8 * tiles
        low = (jnp.maximum(start, base) - base + block - 1) // block
        high = jnp.maximum(jnp.minimum(start + length, end) - base, 0) // block

        @pl.loop(low, jnp.maximum(high, low))
        def _(n):
            action(pl.multiple_of(base + n * block - start, 8), tiles)


PAD = 8
FLAT_ROWS = WINDOW + 272
SHARD_VREGS = SLICE // 1024
TAIL_ROWS = SLICE % 1024 // LANES
TAIL_LANES = SLICE % LANES
EDGE_ROWS = EDGE // LANES
OWN_FLAT_ROWS = OWN + 512


def lane_index(rows=8):
    return lax.broadcasted_iota(jnp.int32, (rows, LANES), 1)


BATCH = 128
BATCHES = SHARD_VREGS * 8 // BATCH
CHUNK_BATCHES = 6
CHUNKS = BATCHES // CHUNK_BATCHES
CHUNK = CHUNK_BATCHES * BATCH * LANES


def mid_kernel(tile_ref, m_ref, v_ref, w_ref, edge_ref, m_out, v_out, w_out, own_ref,
               m_buf, v_buf, w_buf, flat, shifted, edged, aligned, in_sem, out_sem):
    device = device_index()
    start = window_start(device)
    arrays = ((m_ref, m_buf, m_out), (v_ref, v_buf, v_out), (w_ref, w_buf, w_out))

    def span(chunk):
        return pl.ds(chunk * CHUNK, CHUNK if chunk < CHUNKS - 1 else SLICE - chunk * CHUNK)

    def loads(chunk):
        return [pltpu.make_async_copy(ref.at[span(chunk)], buf.at[span(chunk)], in_sem.at[n, chunk])
                for n, (ref, buf, _) in enumerate(arrays)]

    def stores(chunk):
        return [pltpu.make_async_copy(buf.at[span(chunk)], out.at[span(chunk)], out_sem.at[n, chunk])
                for n, (_, buf, out) in enumerate(arrays)]

    for chunk in range(CHUNKS):
        for copy in loads(chunk):
            copy.start()

    def to_flat(row, tiles):
        for t in range(tiles):
            flat[pl.ds(row + t, 8, stride=tiles), :] = tile_ref[pl.ds(row + 8 * t, 8), :]
    for_blocks(start, WINDOW, to_flat)

    first_row = device * (SLICE // 16) // 8
    next_row = (device + 1) * (SLICE // 16) // 8
    shift = device * SLICE - first_row * LANES
    next_shift = (device + 1) * SLICE - next_row * LANES

    def mean_rows(row, amount, rows):
        here = flat[pl.ds(row, rows), :]
        below = flat[pl.ds(row + 1, rows), :]
        back = (LANES - amount) % LANES
        return jnp.where(lane_index(rows) < LANES - amount, pltpu.roll(here, back, 1), pltpu.roll(below, back, 1))

    for chunk in range(CHUNKS):
        for copy in loads(chunk):
            copy.wait()

        @pl.loop(chunk * CHUNK_BATCHES, (chunk + 1) * CHUNK_BATCHES)
        def _(n):
            at = pl.ds(pl.multiple_of(n * BATCH * LANES, BATCH * LANES), BATCH * LANES)
            mean = mean_rows(first_row - start + n * BATCH, shift, BATCH)
            new = adam_update(mean, *(buf[at].reshape(BATCH, LANES) for _, buf, _ in arrays))
            for (_, buf, _), value in zip(arrays, new):
                buf[at] = value.reshape(BATCH * LANES)
            shifted[pl.ds(pl.multiple_of(PAD + n * BATCH, 8), BATCH), :] = pltpu.roll(new[2], shift, 1)

        if chunk > 0:
            for copy in stores(chunk - 1):
                copy.start()

    mean = mean_rows(first_row - start + SHARD_VREGS * 8, shift, 8)
    for r in range(TAIL_ROWS + 1):
        size = LANES if r < TAIL_ROWS else TAIL_LANES
        at = pl.ds(SHARD_VREGS * 1024 + r * LANES, size)
        new = adam_update(mean[r:r + 1, :size], *(buf[at].reshape(1, size) for _, buf, _ in arrays))
        for (_, buf, _), value in zip(arrays, new):
            buf[at] = value.reshape(size)
        flat[pl.ds(FLAT_ROWS - 8 + r, 1), pl.ds(0, size)] = new[2]
    shifted[pl.ds(PAD + SHARD_VREGS * 8, 8), :] = pltpu.roll(flat[pl.ds(FLAT_ROWS - 8, 8), :], shift, 1)

    @pl.loop(0, EDGE_ROWS // 64)
    def _(n):
        mean = mean_rows(next_row - start + n * 64, next_shift, 64)
        old = (edge_ref[pl.ds(pl.multiple_of(k * EDGE + n * 8192, 1024), 8192)].reshape(64, LANES) for k in range(3))
        edged[pl.ds(pl.multiple_of(PAD + n * 64, 8), 64), :] = pltpu.roll(adam_update(mean, *old)[2], next_shift, 1)

    for copy in stores(CHUNKS - 1):
        copy.start()

    own = own_start(device)
    skip = own - first_row

    @pl.loop(0, BATCHES + 1)
    def _(n):
        row = PAD + skip + n * BATCH
        aligned[pl.ds(pl.multiple_of(n * BATCH, 8), BATCH), :] = jnp.where(
            lane_index(BATCH) >= shift, shifted[pl.ds(row, BATCH), :], shifted[pl.ds(row - 1, BATCH), :])
    edged[pl.ds(PAD - 1, 1), :] = aligned[pl.ds(next_row - own, 1), :]

    @pl.loop(0, EDGE_ROWS // 64)
    def _(n):
        row = PAD + n * 64
        aligned[pl.ds(next_row - own + n * 64, 64), :] = jnp.where(
            lane_index(64) >= next_shift, edged[pl.ds(row, 64), :], edged[pl.ds(row - 1, 64), :])

    def to_tile(row, tiles):
        for t in range(0, tiles, 2):
            both = [aligned[pl.ds(row + t + k, 8, stride=tiles), :] for k in range(2)]
            own_ref[pl.ds(pl.multiple_of(row + 8 * t, 16), 16), :] = jnp.concatenate(both, axis=0).astype(jnp.bfloat16)

    def plain(row, _):
        own_ref[pl.ds(pl.multiple_of(row, 16), 16), :] = aligned[pl.ds(row, 16), :].astype(jnp.bfloat16)
    for_blocks(own, OWN, to_tile, TENSORS[:4])
    for_blocks(own, OWN, plain, ((*TENSORS[4][:2], 2),))

    for chunk in range(CHUNKS):
        for copy in stores(chunk):
            copy.wait()


def mid(mean_tiles, m, v, w, edges):
    vmem = pl.BlockSpec(memory_space=pltpu.VMEM)
    any_spec = pl.BlockSpec(memory_space=pl.ANY)
    shard = jax.ShapeDtypeStruct((SLICE,), jnp.float32)
    return pl.pallas_call(
        mid_kernel,
        out_shape=(shard, shard, shard, jax.ShapeDtypeStruct((OWN, LANES), jnp.bfloat16)),
        in_specs=[vmem, any_spec, any_spec, any_spec, vmem], out_specs=(any_spec, any_spec, any_spec, vmem),
        scratch_shapes=[
            pltpu.VMEM((SLICE,), jnp.float32), pltpu.VMEM((SLICE,), jnp.float32), pltpu.VMEM((SLICE,), jnp.float32),
            pltpu.VMEM((FLAT_ROWS, LANES), jnp.float32),
            pltpu.VMEM((PAD + SHARD_VREGS * 8 + 8 + 512, LANES), jnp.float32),
            pltpu.VMEM((PAD + EDGE_ROWS, LANES), jnp.float32),
            pltpu.VMEM((OWN_FLAT_ROWS, LANES), jnp.float32),
            pltpu.SemaphoreType.DMA((3, CHUNKS)), pltpu.SemaphoreType.DMA((3, CHUNKS)),
        ],
        compiler_params=pltpu.CompilerParams(vmem_limit_bytes=MID_LIMIT),
    )(mean_tiles, m, v, w, edges)


def pieces_of(tensor):
    base, end, _ = TENSORS[tensor]
    for d in range(SIXTEEN):
        low, high = max(OWN_STARTS[d], base), min(OWN_STARTS[d + 1], end)
        if low < high:
            yield d, low - OWN_STARTS[d], low - base, high - low


PIECES = [(tensor,) + piece for tensor in range(4) for piece in pieces_of(tensor)]
VEC_WIDTH = 12032
VEC_ROWS = VEC_WIDTH // LANES
VEC_BLOCK = VEC_WIDTH // 8
CHIP_COUNTS = tuple((end - base) // 8 for base, end, _ in TENSORS[:4])
CHIP_ROWS = sum(CHIP_COUNTS)
CHIP_SIZE = CHIP_ROWS * LANES + VEC_BLOCK


def final_kernel(full_ref, e_out, a_out, f_out, h_out, vec_out, chip_out, block, flat, vec, out_sem, block_sem):
    outs = (e_out, a_out, f_out, h_out)
    chip = device_index() // 2
    copies = []
    for n, (tensor, d, source, target, rows) in enumerate(PIECES):
        copies.append(pltpu.make_async_copy(
            full_ref.at[d, pl.ds(source, rows), :], outs[tensor].at[pl.ds(target, rows), :], out_sem.at[n]))
        copies[-1].start()

    slot, source, _, _ = next(pieces_of(4))
    vec[pl.ds(0, 96), :] = full_ref[slot, pl.ds(source, 96), :].astype(jnp.float32)
    for n in range(VEC_ROWS // 8):
        vec_out[:, n * 1024:(n + 1) * 1024] = vec[n * 8:n * 8 + 8, :].reshape(1, 1024).astype(jnp.bfloat16)
    rest = VEC_ROWS % 8
    vec_out[:, VEC_ROWS // 8 * 1024:] = vec[pl.ds(VEC_ROWS - rest, rest), :].reshape(1, rest * LANES).astype(jnp.bfloat16)

    offset = 0
    for tensor, rows in enumerate(CHIP_COUNTS):
        base, _, tiles = TENSORS[tensor]
        step = 16 * tiles

        @pl.loop(0, rows // step)
        def _(n):
            row = base + chip * rows + n * step
            slot = jnp.int32(0)
            low = jnp.int32(0)
            for d in range(1, SIXTEEN):
                slot = jnp.where(row >= OWN_STARTS[d], d, slot)
                low = jnp.where(row >= OWN_STARTS[d], OWN_STARTS[d], low)
            second = row + 8 * tiles
            slot2 = jnp.int32(0)
            low2 = jnp.int32(0)
            for d in range(1, SIXTEEN):
                slot2 = jnp.where(second >= OWN_STARTS[d], d, slot2)
                low2 = jnp.where(second >= OWN_STARTS[d], OWN_STARTS[d], low2)
            for half, (at_slot, at_row) in enumerate(((slot, row - low), (slot2, second - low2))):
                for t in range(0, tiles, 2):
                    value = full_ref[at_slot, pl.ds(pl.multiple_of(at_row + 8 * t, 16), 16), :].astype(jnp.float32)
                    for k in range(2):
                        to = offset + n * step + half * 8 * tiles + t + k
                        flat[pl.ds(to, 8, stride=tiles), :] = value[8 * k:8 * k + 8]
        offset += rows

    vec_row = chip * (VEC_BLOCK // 32) // 4
    amount = chip * VEC_BLOCK - vec_row * LANES
    back = (LANES - amount) % LANES
    lane = lane_index()
    for n in range(2):
        here, below = vec[pl.ds(vec_row + n * 8, 8), :], vec[pl.ds(vec_row + n * 8 + 1, 8), :]
        flat[pl.ds(CHIP_ROWS + n * 8, 8), :] = jnp.where(
            lane < LANES - amount, pltpu.roll(here, back, 1), pltpu.roll(below, back, 1))

    @pl.loop(0, CHIP_SIZE // 4096)
    def _(n):
        for k in range(4):
            chip_out[:, pl.ds(pl.multiple_of(n * 4096 + k * 1024, 1024), 1024)] = flat[
                pl.ds(pl.multiple_of(n * 32 + k * 8, 8), 8), :].reshape(1, 1024).astype(jnp.bfloat16)
    for n in range(CHIP_SIZE // 4096 * 4, CHIP_SIZE // 1024):
        chip_out[:, n * 1024:(n + 1) * 1024] = flat[n * 8:n * 8 + 8, :].reshape(1, 1024).astype(jnp.bfloat16)
    done = CHIP_SIZE // 1024 * 1024
    rows = (CHIP_SIZE - done) // LANES
    last = CHIP_SIZE - done - rows * LANES
    first = done // LANES
    chip_out[:, done:done + rows * LANES] = flat[first:first + rows, :].reshape(1, rows * LANES).astype(jnp.bfloat16)
    chip_out[:, CHIP_SIZE - last:] = flat[first + rows:first + rows + 1, :last].astype(jnp.bfloat16)

    for copy in copies:
        copy.wait()


def finish(full):
    vmem = pl.BlockSpec(memory_space=pltpu.VMEM)
    any_spec = pl.BlockSpec(memory_space=pl.ANY)
    shape = lambda rows: jax.ShapeDtypeStruct((rows, LANES), jnp.bfloat16)
    return pl.pallas_call(
        final_kernel,
        out_shape=tuple(shape(end - base) for base, end, _ in TENSORS[:4]) + (
            jax.ShapeDtypeStruct((1, VEC_WIDTH), jnp.bfloat16), jax.ShapeDtypeStruct((1, CHIP_SIZE), jnp.bfloat16)),
        in_specs=[vmem], out_specs=(any_spec,) * 4 + (vmem, vmem),
        scratch_shapes=[
            pltpu.VMEM((16, LANES), jnp.bfloat16),
            pltpu.VMEM((CHIP_ROWS + 16, LANES), jnp.float32),
            pltpu.VMEM((120, LANES), jnp.float32),
            pltpu.SemaphoreType.DMA((len(PIECES),)), pltpu.SemaphoreType.DMA(()),
        ],
        compiler_params=pltpu.CompilerParams(vmem_limit_bytes=FINAL_LIMIT),
    )(full)


def solution(mesh):
    def local_step(g_embed, g_attn, g_ffn_in, g_ffn_out, g_vec, m_shard, v_shard, w_shard):
        matrices = (g_embed, g_attn, g_ffn_in, g_ffn_out)
        grads = [to_tiles(g[0] if g.ndim == 3 else g[0, 0]) for g in matrices]
        grads.append(jnp.pad(g_vec.reshape(-1), (0, UNIT * LANES - VEC_WIDTH)).reshape(UNIT, LANES))
        mean_tiles, edges = scatter(grads, m_shard, v_shard, w_shard)
        m_new, v_new, w_new, w_own = mid(mean_tiles, m_shard, v_shard, w_shard, edges)
        full = gather(w_own).reshape(SIXTEEN, OWN, LANES)
        *tiles, vec, w_chip = finish(full)
        tensors = [from_tiles(t, g.shape[-1]).reshape(g.shape[1:]) for t, g in zip(tiles, matrices)]
        return (m_new, v_new, w_new) + tuple(tensors) + (vec, w_chip)

    return jax.shard_map(local_step, mesh=mesh, in_specs=(P(MESH_AXES),) * 8, out_specs=(P(MESH_AXES),) * 3 + (P(),) * 5 + (P(MESH_AXES),), check_vma=False)
```

```python
import functools
import math
import jax
import jax.numpy as jnp
from jax import lax
from jax.experimental import pallas as pl
from jax.experimental.pallas import tpu as pltpu
from jax.sharding import PartitionSpec as P

MESH_AXES = ('outer', 'middle', 'inner')
MESH = pl.DeviceIdType.MESH
ADAM_BETA1 = 0.9
ADAM_BETA2 = 0.98
ADAM_EPS = 1e-9
LEARN_RATE = 0.05
ADAM_STEP = 3

LANES = 128
SLICE = 885488
TENSORS = ((0, 32768, 8), (32768, 65536, 32), (65536, 88064, 22), (88064, 110592, 8), (110592, 110720, 1))
ROWS = 110720
VEC_BLOCK_ROWS = 128
UNIT = 64
WINDOW = 7232
COUNTS = (38, 38, 37)
FIRSTS = (0, 38, 76)
ITEMS = max(COUNTS)
LAG = 2
EDGE = 32768
OWN = 7104
OWN_THIRD = OWN // 3
OWN_CHUNK = 64
OWN_ITEMS = OWN_THIRD // OWN_CHUNK
OWN_LAG = 2
SIXTEEN = 16
FINAL_LIMIT = 20000000
GATHER_LIMIT = 6000000
MID_LIMIT = 64000000


def floor_block(row):
    result = row
    for base, end, tiles in TENSORS:
        block = 8 * tiles if tiles > 1 else VEC_BLOCK_ROWS
        floored = base + (row - base) // block * block
        result = jnp.where((row >= base) & (row < end), floored, result)
    return result


def window_start(index):
    row = floor_block(index * (SLICE // 16) // 8)
    return jnp.minimum(row // UNIT * UNIT, ROWS - WINDOW)


def own_start_static(index):
    row = -(-index * SLICE // LANES)
    for base, end, tiles in TENSORS:
        if base <= row < end:
            block = 8 * tiles if tiles > 1 else VEC_BLOCK_ROWS
            return base + -(-(row - base) // block) * block
    return ROWS


OWN_STARTS = [own_start_static(d) for d in range(SIXTEEN)] + [ROWS]


def own_start(index):
    result = jnp.int32(0)
    for d in range(SIXTEEN):
        result = jnp.where(index == d, OWN_STARTS[d], result)
    return result


def adam_update(grad_mean, m_old, v_old, w_old):
    m_new = ADAM_BETA1 * m_old + (1.0 - ADAM_BETA1) * grad_mean
    v_new = ADAM_BETA2 * v_old + (1.0 - ADAM_BETA2) * (grad_mean * grad_mean)
    scale = LEARN_RATE / (1.0 - ADAM_BETA1 ** ADAM_STEP)
    w_new = w_old - scale * m_new / (jnp.sqrt(v_new * (1.0 / (1.0 - ADAM_BETA2 ** ADAM_STEP))) + ADAM_EPS)
    return m_new, v_new, w_new


def to_tiles(tensor):
    rows, width = tensor.shape
    return tensor.reshape(rows // 8, 8, width // LANES, LANES).transpose(0, 2, 1, 3).reshape(-1, LANES)


def from_tiles(tiles, width):
    return tiles.reshape(-1, width // LANES, 8, LANES).transpose(0, 2, 1, 3).reshape(-1, width)


ORDERS = ((0, 1, 2), (1, 2, 0), (2, 0, 1))


def position():
    outer, middle, inner = (lax.axis_index(name) for name in MESH_AXES)
    return outer, middle, inner // 2, inner % 2


def neighbour(axis):
    outer, middle, x, core = position()
    z, y = outer, middle
    if axis == 0:
        z = 1 - z
    elif axis == 1:
        y = 1 - y
    elif axis == 2:
        x = 1 - x
    else:
        core = 1 - core
    return (z, y, 2 * x + core)


def scatter_kernel(e_ref, a_ref, f_ref, h_ref, b_ref, m_ref, v_ref, w_ref, out_ref, edge_ref,
                   part, recv0, recv1, recv2, mine, pair_send, pair_recv, mine_sem,
                   send, arrive, out_sem, edge_send, edge_recv):
    z, y, x, core = position()
    chip = (z * 2 + y) * 2 + x
    device = chip * 2 + core
    sources = (e_ref, a_ref, f_ref, h_ref, b_ref)

    before = (device + SIXTEEN - 1) % SIXTEEN
    for n, ref in enumerate((m_ref, v_ref, w_ref)):
        pltpu.make_async_remote_copy(
            src_ref=ref.at[pl.ds(0, EDGE)], dst_ref=edge_ref.at[pl.ds(n * EDGE, EDGE)],
            send_sem=edge_send.at[n], recv_sem=edge_recv.at[n],
            device_id=(before // 8, before // 4 % 2, before % 4), device_id_type=MESH).start()

    def from_source(row, action):
        for source, (base, end, _) in zip(sources, TENSORS):
            @pl.when((row >= base) & (row < end))
            def _():
                action(source.at[pl.ds(pl.multiple_of(row - base, UNIT), UNIT), :])

    def item_row(third, item):
        return pl.multiple_of((FIRSTS[third] + item) * UNIT, UNIT)

    def each_third(item, action):
        for third in range(3):
            if COUNTS[third] == ITEMS:
                action(third)
            else:
                @pl.when(item < COUNTS[third])
                def _():
                    action(third)

    def start_pair(item):
        @pl.loop(0, 8)
        def _(j):
            jz, jy, jx = j // 4, j // 2 % 2, j % 2
            other = ((z + jz) % 2 * 2 + (y + jy) % 2) * 2 + (x + jx) % 2
            start = window_start(other * 2 + 1 - core)

            def action(third):
                row = item_row(third, item)
                from_source(start + row, lambda src: pltpu.make_async_remote_copy(
                    src_ref=src, dst_ref=part.at[jz, jy, jx, pl.ds(row, UNIT), :],
                    send_sem=pair_send.at[third], recv_sem=pair_recv.at[third, item],
                    device_id=neighbour(3), device_id_type=MESH).start())
            each_third(item, action)

    def start_mine(item, slot):
        @pl.loop(0, 8)
        def _(j):
            jz, jy, jx = j // 4, j // 2 % 2, j % 2
            other = ((z + jz) % 2 * 2 + (y + jy) % 2) * 2 + (x + jx) % 2
            start = window_start(other * 2 + core)

            def action(third):
                from_source(start + item_row(third, item), lambda src: pltpu.make_async_copy(
                    src, mine.at[slot, third, jz, jy, jx], mine_sem.at[slot, third]).start())
            each_third(item, action)

    def hop_copy(third, item, hop, whole=False):
        rows = pl.ds(item_row(third, 0), COUNTS[third] * UNIT) if whole else pl.ds(item_row(third, item), UNIT)
        first, second, last = ORDERS[third]
        if hop == 0:
            index = tuple(1 if n == first else slice(None) for n in range(3))
            target = recv0.at[:, :, rows, :]
        elif hop == 1:
            index = tuple(0 if n == first else 1 if n == second else slice(None) for n in range(3))
            target = recv1.at[:, rows, :]
        else:
            index = tuple(1 if n == last else 0 for n in range(3))
            target = recv2.at[rows, :]
        return pltpu.make_async_remote_copy(
            src_ref=part.at[index + (rows, slice(None))], dst_ref=target,
            send_sem=send.at[third, hop], recv_sem=arrive.at[third, hop, item],
            device_id=neighbour(ORDERS[third][hop]), device_id_type=MESH)

    def pair_all(third, item, whole=False):
        rows = pl.ds(item_row(third, 0), COUNTS[third] * UNIT) if whole else pl.ds(item_row(third, item), UNIT)
        block = part.at[:, :, :, rows, :]
        return pltpu.make_async_remote_copy(
            src_ref=block, dst_ref=block, send_sem=pair_send.at[third], recv_sem=pair_recv.at[third, item],
            device_id=neighbour(3), device_id_type=MESH)

    def out_copy(third, item, whole=False):
        rows = pl.ds(item_row(third, 0), COUNTS[third] * UNIT) if whole else pl.ds(item_row(third, item), UNIT)
        return pltpu.make_async_copy(part.at[0, 0, 0, rows, :], out_ref.at[rows, :], out_sem.at[third])

    start_pair(0)
    start_mine(0, 0)

    def stage0(item, third):
        rows = pl.ds(item_row(third, item), UNIT)
        slot = item % 2
        pltpu.make_async_copy(mine.at[slot, third], mine.at[slot, third], mine_sem.at[slot, third]).wait()
        pair_all(third, item).wait_recv()
        for j in range(8):
            index = (j // 4, j // 2 % 2, j % 2)
            part[index + (rows, slice(None))] += mine[(slot, third) + index]
        hop_copy(third, item, 0).start()

    def stage1(item, third):
        rows = pl.ds(item_row(third, item), UNIT)
        hop_copy(third, item, 0).wait_recv()
        first = ORDERS[third][0]
        for j in range(4):
            pair = [j // 2, j % 2]
            index = tuple(pair[:first] + [0] + pair[first:])
            part[index + (rows, slice(None))] += recv0[j // 2, j % 2, rows, :]
        hop_copy(third, item, 1).start()

    def stage2(item, third):
        rows = pl.ds(item_row(third, item), UNIT)
        hop_copy(third, item, 1).wait_recv()
        last = ORDERS[third][2]
        for j in range(2):
            index = tuple(j if n == last else 0 for n in range(3))
            part[index + (rows, slice(None))] += recv1[j, rows, :]
        hop_copy(third, item, 2).start()

    def stage3(item, third):
        rows = pl.ds(item_row(third, item), UNIT)
        hop_copy(third, item, 2).wait_recv()
        part[0, 0, 0, rows, :] = (part[0, 0, 0, rows, :] + recv2[rows, :]) / SIXTEEN

    stages = ((0, stage0), (LAG, stage1), (2 * LAG, stage2), (3 * LAG, stage3),
              (3 * LAG + 1, lambda item, third: out_copy(third, item).start()))

    @pl.loop(0, ITEMS + stages[-1][0])
    def _(step):
        for delay, stage in stages:
            if delay == 0:
                @pl.when(step + 1 < ITEMS)
                def _():
                    start_pair(step + 1)

            @pl.when((step >= delay) & (step < ITEMS + delay))
            def _():
                each_third(step - delay, functools.partial(stage, step - delay))
            if delay == 0:
                @pl.when(step + 1 < ITEMS)
                def _():
                    start_mine(step + 1, (step + 1) % 2)

    for third in range(3):
        pair_all(third, 0, True).wait_send()
        for hop in range(3):
            hop_copy(third, 0, hop, True).wait_send()
        out_copy(third, 0, True).wait()

    for n, ref in enumerate((m_ref, v_ref, w_ref)):
        pltpu.make_async_remote_copy(
            src_ref=ref.at[pl.ds(0, EDGE)], dst_ref=edge_ref.at[pl.ds(n * EDGE, EDGE)],
            send_sem=edge_send.at[n], recv_sem=edge_recv.at[n],
            device_id=(before // 8, before // 4 % 2, before % 4), device_id_type=MESH).wait()


def scatter(grads, m, v, w):
    any_spec = pl.BlockSpec(memory_space=pl.ANY)
    dma = pltpu.SemaphoreType.DMA
    return pl.pallas_call(
        scatter_kernel,
        out_shape=(jax.ShapeDtypeStruct((WINDOW, LANES), jnp.float32), jax.ShapeDtypeStruct((3 * EDGE,), jnp.float32)),
        in_specs=[any_spec] * 8,
        out_specs=(any_spec, any_spec),
        scratch_shapes=[
            pltpu.VMEM((2, 2, 2, WINDOW, LANES), jnp.float32),
            pltpu.VMEM((2, 2, WINDOW, LANES), jnp.float32),
            pltpu.VMEM((2, WINDOW, LANES), jnp.float32),
            pltpu.VMEM((WINDOW, LANES), jnp.float32),
            pltpu.VMEM((2, 3, 2, 2, 2, UNIT, LANES), jnp.float32),
            dma((3,)), dma((3, ITEMS)), dma((2, 3)),
            dma((3, 3)), dma((3, 3, ITEMS)), dma((3,)), dma((3,)), dma((3,)),
        ],
        compiler_params=pltpu.CompilerParams(has_side_effects=True, vmem_limit_bytes=67043328),
    )(*grads, m, v, w)


def gather_kernel(w_ref, full_ref, pair_send, pair_recv, send, arrive):
    z, y, x, core = position()
    here = (z, y, x)

    def rows_of(third, item, whole=False):
        if whole:
            return pl.ds(third * OWN_THIRD, OWN_THIRD)
        return pl.ds(pl.multiple_of(third * OWN_THIRD + item * OWN_CHUNK, OWN_CHUNK), OWN_CHUNK)

    def copy(third, item, hop, whole=False):
        rows = rows_of(third, item, whole)
        order = ORDERS[third]
        if hop == 0:
            source = w_ref.at[rows, :]
            target = full_ref.at[z, y, x, core, rows, :]
        else:
            index = tuple(slice(None) if n in order[:hop] else here[n] for n in range(3))
            source = target = full_ref.at[index + (core, rows, slice(None))]
        return pltpu.make_async_remote_copy(
            src_ref=source, dst_ref=target, send_sem=send.at[third, hop], recv_sem=arrive.at[third, item, hop],
            device_id=neighbour(order[hop]), device_id_type=MESH)

    def arrival(third, item, hop):
        order = ORDERS[third]
        index = tuple(slice(None) if n in order[:hop] else (1 - here[n] if n == order[hop] else here[n]) for n in range(3))
        block = full_ref.at[index + (core, rows_of(third, item), slice(None))]
        return pltpu.make_async_remote_copy(
            src_ref=block, dst_ref=block, send_sem=send.at[third, hop], recv_sem=arrive.at[third, item, hop],
            device_id=neighbour(order[hop]), device_id_type=MESH)

    def pair(third, item, side, whole=False):
        block = full_ref.at[:, :, :, side, rows_of(third, item, whole), :]
        return pltpu.make_async_remote_copy(
            src_ref=block, dst_ref=block, send_sem=pair_send.at[third], recv_sem=pair_recv.at[third, item],
            device_id=neighbour(3), device_id_type=MESH)

    for item in range(OWN_LAG):
        for third in range(3):
            copy(third, item, 0).start()

    @pl.loop(0, OWN // OWN_CHUNK)
    def _(n):
        rows = pl.ds(pl.multiple_of(n * OWN_CHUNK, OWN_CHUNK), OWN_CHUNK)
        full_ref[z, y, x, core, rows, :] = w_ref[rows, :]

    @pl.loop(0, OWN_ITEMS + 2 * OWN_LAG)
    def _(step):
        @pl.when(step + OWN_LAG < OWN_ITEMS)
        def _():
            for third in range(3):
                copy(third, step + OWN_LAG, 0).start()

        for hop in range(1, 4):
            delay = (hop - 1) * OWN_LAG

            @pl.when((step >= delay) & (step < OWN_ITEMS + delay))
            def _():
                item = step - delay
                for third in range(3):
                    arrival(third, item, hop - 1).wait_recv()
                    if hop < 3:
                        copy(third, item, hop).start()
                    else:
                        pair(third, item, core).start()

    @pl.loop(0, OWN_ITEMS)
    def _(item):
        for third in range(3):
            pair(third, item, 1 - core).wait_recv()
    for third in range(3):
        pair(third, 0, core, True).wait_send()
        for hop in range(3):
            copy(third, 0, hop, True).wait_send()


def gather(w_own):
    dma = pltpu.SemaphoreType.DMA
    return pl.pallas_call(
        gather_kernel,
        out_shape=jax.ShapeDtypeStruct((2, 2, 2, 2, OWN, LANES), jnp.bfloat16),
        in_specs=[pl.BlockSpec(memory_space=pltpu.VMEM)],
        out_specs=pl.BlockSpec(memory_space=pltpu.VMEM),
        scratch_shapes=[
            dma((3,)), dma((3, OWN_ITEMS)), dma((3, 3)), dma((3, OWN_ITEMS, 3)),
        ],
        compiler_params=pltpu.CompilerParams(has_side_effects=True, vmem_limit_bytes=GATHER_LIMIT),
    )(w_own)


def device_index():
    outer, middle, inner = (lax.axis_index(name) for name in MESH_AXES)
    return (outer * 2 + middle) * 4 + inner


def for_blocks(start, length, action, tensors=TENSORS):
    for base, end, tiles in tensors:
        block = 8 * tiles
        low = (jnp.maximum(start, base) - base + block - 1) // block
        high = jnp.maximum(jnp.minimum(start + length, end) - base, 0) // block

        @pl.loop(low, jnp.maximum(high, low))
        def _(n):
            action(pl.multiple_of(base + n * block - start, 8), tiles)


PAD = 8
FLAT_ROWS = WINDOW + 272
SHARD_VREGS = SLICE // 1024
TAIL_ROWS = SLICE % 1024 // LANES
TAIL_LANES = SLICE % LANES
EDGE_ROWS = EDGE // LANES
OWN_FLAT_ROWS = OWN + 512


def lane_index(rows=8):
    return lax.broadcasted_iota(jnp.int32, (rows, LANES), 1)


BATCH = 128
BATCHES = SHARD_VREGS * 8 // BATCH
CHUNK_BATCHES = 6
CHUNKS = BATCHES // CHUNK_BATCHES
CHUNK = CHUNK_BATCHES * BATCH * LANES


def mid_kernel(tile_ref, m_ref, v_ref, w_ref, edge_ref, m_out, v_out, w_out, own_ref,
               m_buf, v_buf, w_buf, flat, shifted, edged, aligned, in_sem, out_sem):
    device = device_index()
    start = window_start(device)
    arrays = ((m_ref, m_buf, m_out), (v_ref, v_buf, v_out), (w_ref, w_buf, w_out))

    def span(chunk):
        return pl.ds(chunk * CHUNK, CHUNK if chunk < CHUNKS - 1 else SLICE - chunk * CHUNK)

    def loads(chunk):
        return [pltpu.make_async_copy(ref.at[span(chunk)], buf.at[span(chunk)], in_sem.at[n, chunk])
                for n, (ref, buf, _) in enumerate(arrays)]

    def stores(chunk):
        return [pltpu.make_async_copy(buf.at[span(chunk)], out.at[span(chunk)], out_sem.at[n, chunk])
                for n, (_, buf, out) in enumerate(arrays)]

    for chunk in range(CHUNKS):
        for copy in loads(chunk):
            copy.start()

    def to_flat(row, tiles):
        for t in range(tiles):
            flat[pl.ds(row + t, 8, stride=tiles), :] = tile_ref[pl.ds(row + 8 * t, 8), :]
    for_blocks(start, WINDOW, to_flat)

    first_row = device * (SLICE // 16) // 8
    next_row = (device + 1) * (SLICE // 16) // 8
    shift = device * SLICE - first_row * LANES
    next_shift = (device + 1) * SLICE - next_row * LANES

    def mean_rows(row, amount, rows):
        here = flat[pl.ds(row, rows), :]
        below = flat[pl.ds(row + 1, rows), :]
        back = (LANES - amount) % LANES
        return jnp.where(lane_index(rows) < LANES - amount, pltpu.roll(here, back, 1), pltpu.roll(below, back, 1))

    for chunk in range(CHUNKS):
        for copy in loads(chunk):
            copy.wait()

        @pl.loop(chunk * CHUNK_BATCHES, (chunk + 1) * CHUNK_BATCHES)
        def _(n):
            at = pl.ds(pl.multiple_of(n * BATCH * LANES, BATCH * LANES), BATCH * LANES)
            mean = mean_rows(first_row - start + n * BATCH, shift, BATCH)
            new = adam_update(mean, *(buf[at].reshape(BATCH, LANES) for _, buf, _ in arrays))
            for (_, buf, _), value in zip(arrays, new):
                buf[at] = value.reshape(BATCH * LANES)
            shifted[pl.ds(pl.multiple_of(PAD + n * BATCH, 8), BATCH), :] = pltpu.roll(new[2], shift, 1)

        if chunk > 0:
            for copy in stores(chunk - 1):
                copy.start()

    mean = mean_rows(first_row - start + SHARD_VREGS * 8, shift, 8)
    for r in range(TAIL_ROWS + 1):
        size = LANES if r < TAIL_ROWS else TAIL_LANES
        at = pl.ds(SHARD_VREGS * 1024 + r * LANES, size)
        new = adam_update(mean[r:r + 1, :size], *(buf[at].reshape(1, size) for _, buf, _ in arrays))
        for (_, buf, _), value in zip(arrays, new):
            buf[at] = value.reshape(size)
        flat[pl.ds(FLAT_ROWS - 8 + r, 1), pl.ds(0, size)] = new[2]
    shifted[pl.ds(PAD + SHARD_VREGS * 8, 8), :] = pltpu.roll(flat[pl.ds(FLAT_ROWS - 8, 8), :], shift, 1)

    @pl.loop(0, EDGE_ROWS // 64)
    def _(n):
        mean = mean_rows(next_row - start + n * 64, next_shift, 64)
        old = (edge_ref[pl.ds(pl.multiple_of(k * EDGE + n * 8192, 1024), 8192)].reshape(64, LANES) for k in range(3))
        edged[pl.ds(pl.multiple_of(PAD + n * 64, 8), 64), :] = pltpu.roll(adam_update(mean, *old)[2], next_shift, 1)

    for copy in stores(CHUNKS - 1):
        copy.start()

    own = own_start(device)
    skip = own - first_row

    @pl.loop(0, BATCHES + 1)
    def _(n):
        row = PAD + skip + n * BATCH
        aligned[pl.ds(pl.multiple_of(n * BATCH, 8), BATCH), :] = jnp.where(
            lane_index(BATCH) >= shift, shifted[pl.ds(row, BATCH), :], shifted[pl.ds(row - 1, BATCH), :])
    edged[pl.ds(PAD - 1, 1), :] = aligned[pl.ds(next_row - own, 1), :]

    @pl.loop(0, EDGE_ROWS // 64)
    def _(n):
        row = PAD + n * 64
        aligned[pl.ds(next_row - own + n * 64, 64), :] = jnp.where(
            lane_index(64) >= next_shift, edged[pl.ds(row, 64), :], edged[pl.ds(row - 1, 64), :])

    def to_tile(row, tiles):
        for t in range(0, tiles, 2):
            both = [aligned[pl.ds(row + t + k, 8, stride=tiles), :] for k in range(2)]
            own_ref[pl.ds(pl.multiple_of(row + 8 * t, 16), 16), :] = jnp.concatenate(both, axis=0).astype(jnp.bfloat16)

    def plain(row, _):
        own_ref[pl.ds(pl.multiple_of(row, 16), 16), :] = aligned[pl.ds(row, 16), :].astype(jnp.bfloat16)
    for_blocks(own, OWN, to_tile, TENSORS[:4])
    for_blocks(own, OWN, plain, ((*TENSORS[4][:2], 2),))

    for chunk in range(CHUNKS):
        for copy in stores(chunk):
            copy.wait()


def mid(mean_tiles, m, v, w, edges):
    vmem = pl.BlockSpec(memory_space=pltpu.VMEM)
    any_spec = pl.BlockSpec(memory_space=pl.ANY)
    shard = jax.ShapeDtypeStruct((SLICE,), jnp.float32)
    return pl.pallas_call(
        mid_kernel,
        out_shape=(shard, shard, shard, jax.ShapeDtypeStruct((OWN, LANES), jnp.bfloat16)),
        in_specs=[vmem, any_spec, any_spec, any_spec, vmem], out_specs=(any_spec, any_spec, any_spec, vmem),
        scratch_shapes=[
            pltpu.VMEM((SLICE,), jnp.float32), pltpu.VMEM((SLICE,), jnp.float32), pltpu.VMEM((SLICE,), jnp.float32),
            pltpu.VMEM((FLAT_ROWS, LANES), jnp.float32),
            pltpu.VMEM((PAD + SHARD_VREGS * 8 + 8 + 512, LANES), jnp.float32),
            pltpu.VMEM((PAD + EDGE_ROWS, LANES), jnp.float32),
            pltpu.VMEM((OWN_FLAT_ROWS, LANES), jnp.float32),
            pltpu.SemaphoreType.DMA((3, CHUNKS)), pltpu.SemaphoreType.DMA((3, CHUNKS)),
        ],
        compiler_params=pltpu.CompilerParams(vmem_limit_bytes=MID_LIMIT),
    )(mean_tiles, m, v, w, edges)


def pieces_of(tensor):
    base, end, _ = TENSORS[tensor]
    for d in range(SIXTEEN):
        low, high = max(OWN_STARTS[d], base), min(OWN_STARTS[d + 1], end)
        if low < high:
            yield d, low - OWN_STARTS[d], low - base, high - low


PIECES = [(tensor,) + piece for tensor in range(4) for piece in pieces_of(tensor)]
VEC_WIDTH = 12032
VEC_ROWS = VEC_WIDTH // LANES
VEC_BLOCK = VEC_WIDTH // 8
CHIP_COUNTS = tuple((end - base) // 8 for base, end, _ in TENSORS[:4])
CHIP_ROWS = sum(CHIP_COUNTS)
CHIP_SIZE = CHIP_ROWS * LANES + VEC_BLOCK
CHIP_PARTS = 6
CHIP_PART = CHIP_SIZE // 16384 // CHIP_PARTS * 16384


def final_kernel(full_ref, e_out, a_out, f_out, h_out, vec_out, chip_ref, chip_out, flat, vec, out_sem, chip_sem):
    outs = (e_out, a_out, f_out, h_out)
    chip = device_index() // 2
    copies = []
    for n, (tensor, d, source, target, rows) in enumerate(PIECES):
        copies.append(pltpu.make_async_copy(
            full_ref.at[d, pl.ds(source, rows), :], outs[tensor].at[pl.ds(target, rows), :], out_sem.at[n]))
        copies[-1].start()

    slot, source, _, _ = next(pieces_of(4))
    vec[pl.ds(0, 96), :] = full_ref[slot, pl.ds(source, 96), :].astype(jnp.float32)
    for n in range(VEC_ROWS // 8):
        vec_out[:, n * 1024:(n + 1) * 1024] = vec[n * 8:n * 8 + 8, :].reshape(1, 1024).astype(jnp.bfloat16)
    rest = VEC_ROWS % 8
    vec_out[:, VEC_ROWS // 8 * 1024:] = vec[pl.ds(VEC_ROWS - rest, rest), :].reshape(1, rest * LANES).astype(jnp.bfloat16)

    offset = 0
    for tensor, rows in enumerate(CHIP_COUNTS):
        base, _, tiles = TENSORS[tensor]
        step = 16 * tiles

        begin = base + chip * rows
        slot, low, bound = jnp.int32(0), jnp.int32(0), jnp.int32(OWN_STARTS[1])
        for d in range(1, SIXTEEN):
            inside = begin >= OWN_STARTS[d]
            slot = jnp.where(inside, d, slot)
            low = jnp.where(inside, OWN_STARTS[d], low)
            bound = jnp.where(inside, OWN_STARTS[d + 1], bound)

        @pl.loop(0, rows // step)
        def _(n):
            for half in range(2):
                row = begin + n * step + half * 8 * tiles
                following = row >= bound
                at_slot = jnp.where(following, slot + 1, slot)
                at_row = row - jnp.where(following, bound, low)
                for t in range(0, tiles, 2):
                    value = full_ref[at_slot, pl.ds(pl.multiple_of(at_row + 8 * t, 16), 16), :].astype(jnp.float32)
                    for k in range(2):
                        to = offset + n * step + half * 8 * tiles + t + k
                        flat[pl.ds(to, 8, stride=tiles), :] = value[8 * k:8 * k + 8]
        offset += rows

    vec_row = chip * (VEC_BLOCK // 32) // 4
    amount = chip * VEC_BLOCK - vec_row * LANES
    back = (LANES - amount) % LANES
    lane = lane_index()
    for n in range(2):
        here, below = vec[pl.ds(vec_row + n * 8, 8), :], vec[pl.ds(vec_row + n * 8 + 1, 8), :]
        flat[pl.ds(CHIP_ROWS + n * 8, 8), :] = jnp.where(
            lane < LANES - amount, pltpu.roll(here, back, 1), pltpu.roll(below, back, 1))

    def part_copy(part):
        span = pl.ds(part * CHIP_PART, CHIP_PART if part < CHIP_PARTS - 1 else CHIP_SIZE - part * CHIP_PART)
        return pltpu.make_async_copy(chip_out.at[:, span], chip_ref.at[:, span], chip_sem.at[part])

    for part in range(CHIP_PARTS):
        @pl.loop(part * CHIP_PART // 16384, (part + 1) * CHIP_PART // 16384)
        def _(n):
            chip_out[:, pl.ds(pl.multiple_of(n * 16384, 16384), 16384)] = flat[
                pl.ds(pl.multiple_of(n * 128, 128), 128), :].reshape(1, 16384).astype(jnp.bfloat16)
        if part > 0:
            part_copy(part - 1).start()
    done = CHIP_SIZE // 1024 * 1024
    rows = (CHIP_SIZE - done) // LANES
    last = CHIP_SIZE - done - rows * LANES
    first = done // LANES
    chip_out[:, CHIP_PARTS * CHIP_PART:done] = flat[CHIP_PARTS * CHIP_PART // LANES:first, :].reshape(
        1, done - CHIP_PARTS * CHIP_PART).astype(jnp.bfloat16)
    chip_out[:, done:done + rows * LANES] = flat[first:first + rows, :].reshape(1, rows * LANES).astype(jnp.bfloat16)
    chip_out[:, CHIP_SIZE - last:] = flat[first + rows:first + rows + 1, :last].astype(jnp.bfloat16)
    part_copy(CHIP_PARTS - 1).start()
    for part in range(CHIP_PARTS):
        part_copy(part).wait()
    for copy in copies:
        copy.wait()


def finish(full):
    vmem = pl.BlockSpec(memory_space=pltpu.VMEM)
    any_spec = pl.BlockSpec(memory_space=pl.ANY)
    shape = lambda rows: jax.ShapeDtypeStruct((rows, LANES), jnp.bfloat16)
    return pl.pallas_call(
        final_kernel,
        out_shape=tuple(shape(end - base) for base, end, _ in TENSORS[:4]) + (
            jax.ShapeDtypeStruct((1, VEC_WIDTH), jnp.bfloat16), jax.ShapeDtypeStruct((1, CHIP_SIZE), jnp.bfloat16)),
        in_specs=[vmem], out_specs=(any_spec,) * 4 + (vmem, any_spec),
        scratch_shapes=[
            pltpu.VMEM((1, CHIP_SIZE), jnp.bfloat16),
            pltpu.VMEM((CHIP_ROWS + 16, LANES), jnp.float32),
            pltpu.VMEM((120, LANES), jnp.float32),
            pltpu.SemaphoreType.DMA((len(PIECES),)), pltpu.SemaphoreType.DMA((CHIP_PARTS,)),
        ],
        compiler_params=pltpu.CompilerParams(vmem_limit_bytes=FINAL_LIMIT),
    )(full)


def solution(mesh):
    def local_step(g_embed, g_attn, g_ffn_in, g_ffn_out, g_vec, m_shard, v_shard, w_shard):
        matrices = (g_embed, g_attn, g_ffn_in, g_ffn_out)
        grads = [to_tiles(g[0] if g.ndim == 3 else g[0, 0]) for g in matrices]
        grads.append(jnp.pad(g_vec.reshape(-1), (0, VEC_BLOCK_ROWS * LANES - VEC_WIDTH)).reshape(VEC_BLOCK_ROWS, LANES))
        mean_tiles, edges = scatter(grads, m_shard, v_shard, w_shard)
        m_new, v_new, w_new, w_own = mid(mean_tiles, m_shard, v_shard, w_shard, edges)
        full = gather(w_own).reshape(SIXTEEN, OWN, LANES)
        *tiles, vec, w_chip = finish(full)
        tensors = [from_tiles(t, g.shape[-1]).reshape(g.shape[1:]) for t, g in zip(tiles, matrices)]
        return (m_new, v_new, w_new) + tuple(tensors) + (vec, w_chip)

    return jax.shard_map(local_step, mesh=mesh, in_specs=(P(MESH_AXES),) * 8, out_specs=(P(MESH_AXES),) * 3 + (P(),) * 5 + (P(MESH_AXES),), check_vma=False)
```

```python
import functools
import math
import jax
import jax.numpy as jnp
from jax import lax
from jax.experimental import pallas as pl
from jax.experimental.pallas import tpu as pltpu
from jax.sharding import PartitionSpec as P

MESH_AXES = ('outer', 'middle', 'inner')
MESH = pl.DeviceIdType.MESH
ADAM_BETA1 = 0.9
ADAM_BETA2 = 0.98
ADAM_EPS = 1e-9
LEARN_RATE = 0.05
ADAM_STEP = 3

LANES = 128
SLICE = 885488
TENSORS = ((0, 32768, 8), (32768, 65536, 32), (65536, 88064, 22), (88064, 110592, 8), (110592, 110720, 1))
ROWS = 110720
VEC_BLOCK_ROWS = 128
UNIT = 64
GROUP = 128
WINDOW = 7296
COUNTS = (38, 38, 38)
FIRSTS = (0, 38, 76)
ITEMS = max(COUNTS)
LAG = 2
EDGE = 32768
OWN = 7104
OWN_THIRD = OWN // 3
OWN_CHUNK = 64
OWN_ITEMS = OWN_THIRD // OWN_CHUNK
OWN_LAG = 2
SIXTEEN = 16
FINAL_LIMIT = 20000000
GATHER_LIMIT = 6000000
MID_LIMIT = 64000000


def floor_block(row):
    result = row
    for base, end, tiles in TENSORS:
        block = 8 * tiles if tiles > 1 else VEC_BLOCK_ROWS
        floored = base + (row - base) // block * block
        result = jnp.where((row >= base) & (row < end), floored, result)
    return result


def window_start(index):
    row = floor_block(index * (SLICE // 16) // 8)
    return jnp.minimum(row // GROUP * GROUP, ROWS - WINDOW)


def own_start_static(index):
    row = -(-index * SLICE // LANES)
    for base, end, tiles in TENSORS:
        if base <= row < end:
            block = 8 * tiles if tiles > 1 else VEC_BLOCK_ROWS
            return base + -(-(row - base) // block) * block
    return ROWS


OWN_STARTS = [own_start_static(d) for d in range(SIXTEEN)] + [ROWS]


def own_start(index):
    result = jnp.int32(0)
    for d in range(SIXTEEN):
        result = jnp.where(index == d, OWN_STARTS[d], result)
    return result


def adam_update(grad_mean, m_old, v_old, w_old):
    m_new = ADAM_BETA1 * m_old + (1.0 - ADAM_BETA1) * grad_mean
    v_new = ADAM_BETA2 * v_old + (1.0 - ADAM_BETA2) * (grad_mean * grad_mean)
    scale = LEARN_RATE / (1.0 - ADAM_BETA1 ** ADAM_STEP)
    w_new = w_old - scale * m_new / (jnp.sqrt(v_new * (1.0 / (1.0 - ADAM_BETA2 ** ADAM_STEP))) + ADAM_EPS)
    return m_new, v_new, w_new


def to_tiles(tensor):
    rows, width = tensor.shape
    return tensor.reshape(rows // 8, 8, width // LANES, LANES).transpose(0, 2, 1, 3).reshape(-1, LANES)


def from_tiles(tiles, width):
    return tiles.reshape(-1, width // LANES, 8, LANES).transpose(0, 2, 1, 3).reshape(-1, width)


ORDERS = ((0, 1, 2), (1, 2, 0), (2, 0, 1))


def position():
    outer, middle, inner = (lax.axis_index(name) for name in MESH_AXES)
    return outer, middle, inner // 2, inner % 2


def neighbour(axis):
    outer, middle, x, core = position()
    z, y = outer, middle
    if axis == 0:
        z = 1 - z
    elif axis == 1:
        y = 1 - y
    elif axis == 2:
        x = 1 - x
    else:
        core = 1 - core
    return (z, y, 2 * x + core)


def scatter_kernel(e_ref, a_ref, f_ref, h_ref, b_ref, m_ref, v_ref, w_ref, out_ref, edge_ref,
                   part, recv0, recv1, recv2, mine, pair_send, pair_recv, mine_sem,
                   send, arrive, out_sem, edge_send, edge_recv):
    z, y, x, core = position()
    chip = (z * 2 + y) * 2 + x
    device = chip * 2 + core
    sources = (e_ref, a_ref, f_ref, h_ref, b_ref)

    before = (device + SIXTEEN - 1) % SIXTEEN
    for n, ref in enumerate((m_ref, v_ref, w_ref)):
        pltpu.make_async_remote_copy(
            src_ref=ref.at[pl.ds(0, EDGE)], dst_ref=edge_ref.at[pl.ds(n * EDGE, EDGE)],
            send_sem=edge_send.at[n], recv_sem=edge_recv.at[n],
            device_id=(before // 8, before // 4 % 2, before % 4), device_id_type=MESH).start()

    def from_source(row, action):
        def choose(low, high):
            if high - low == 1:
                action(sources[low].at[pl.ds(pl.multiple_of(row - TENSORS[low][0], GROUP), GROUP), :])
                return
            middle = (low + high) // 2
            lax.cond(row < TENSORS[middle][0], lambda: choose(low, middle), lambda: choose(middle, high))
        choose(0, len(sources))

    def item_row(third, item):
        return pl.multiple_of((FIRSTS[third] + item) * UNIT, UNIT)

    def group_row(third, group):
        return pl.multiple_of(FIRSTS[third] * UNIT + group * GROUP, GROUP)

    def start_group(group, slot):
        @pl.loop(0, 8)
        def _(j):
            jz, jy, jx = j // 4, j // 2 % 2, j % 2
            other = ((z + jz) % 2 * 2 + (y + jy) % 2) * 2 + (x + jx) % 2
            theirs = window_start(other * 2 + 1 - core)
            ours = window_start(other * 2 + core)
            for third in range(3):
                row = group_row(third, group)
                from_source(theirs + row, lambda src: pltpu.make_async_remote_copy(
                    src_ref=src, dst_ref=part.at[jz, jy, jx, pl.ds(row, GROUP), :],
                    send_sem=pair_send.at[third], recv_sem=pair_recv.at[third, group],
                    device_id=neighbour(3), device_id_type=MESH).start())
                from_source(ours + row, lambda src: pltpu.make_async_copy(
                    src, mine.at[slot, third, jz, jy, jx], mine_sem.at[slot, third]).start())

    def hop_copy(third, item, hop, whole=False):
        rows = pl.ds(item_row(third, 0), COUNTS[third] * UNIT) if whole else pl.ds(item_row(third, item), UNIT)
        first, second, last = ORDERS[third]
        if hop == 0:
            index = tuple(1 if n == first else slice(None) for n in range(3))
            target = recv0.at[:, :, rows, :]
        elif hop == 1:
            index = tuple(0 if n == first else 1 if n == second else slice(None) for n in range(3))
            target = recv1.at[:, rows, :]
        else:
            index = tuple(1 if n == last else 0 for n in range(3))
            target = recv2.at[rows, :]
        return pltpu.make_async_remote_copy(
            src_ref=part.at[index + (rows, slice(None))], dst_ref=target,
            send_sem=send.at[third, hop], recv_sem=arrive.at[third, hop, item],
            device_id=neighbour(ORDERS[third][hop]), device_id_type=MESH)

    def pair_all(third, group, whole=False):
        rows = pl.ds(FIRSTS[third] * UNIT, COUNTS[third] * UNIT) if whole else pl.ds(group_row(third, group), GROUP)
        block = part.at[:, :, :, rows, :]
        return pltpu.make_async_remote_copy(
            src_ref=block, dst_ref=block, send_sem=pair_send.at[third], recv_sem=pair_recv.at[third, group],
            device_id=neighbour(3), device_id_type=MESH)

    def out_copy(third, item, whole=False):
        rows = pl.ds(item_row(third, 0), COUNTS[third] * UNIT) if whole else pl.ds(item_row(third, item), UNIT)
        return pltpu.make_async_copy(part.at[0, 0, 0, rows, :], out_ref.at[rows, :], out_sem.at[third])

    start_group(0, 0)

    def stage0(item, third):
        rows = pl.ds(item_row(third, item), UNIT)
        group = item // 2
        slot = group % 2

        @pl.when(item % 2 == 0)
        def _():
            pltpu.make_async_copy(mine.at[slot, third], mine.at[slot, third], mine_sem.at[slot, third]).wait()
            pair_all(third, group).wait_recv()
        within = pl.ds(pl.multiple_of(item % 2 * UNIT, UNIT), UNIT)
        for j in range(8):
            index = (j // 4, j // 2 % 2, j % 2)
            part[index + (rows, slice(None))] += mine[(slot, third) + index + (within, slice(None))]
        hop_copy(third, item, 0).start()

    def stage1(item, third):
        rows = pl.ds(item_row(third, item), UNIT)
        hop_copy(third, item, 0).wait_recv()
        first = ORDERS[third][0]
        for j in range(4):
            pair = [j // 2, j % 2]
            index = tuple(pair[:first] + [0] + pair[first:])
            part[index + (rows, slice(None))] += recv0[j // 2, j % 2, rows, :]
        hop_copy(third, item, 1).start()

    def stage2(item, third):
        rows = pl.ds(item_row(third, item), UNIT)
        hop_copy(third, item, 1).wait_recv()
        last = ORDERS[third][2]
        for j in range(2):
            index = tuple(j if n == last else 0 for n in range(3))
            part[index + (rows, slice(None))] += recv1[j, rows, :]
        hop_copy(third, item, 2).start()

    def stage3(item, third):
        rows = pl.ds(item_row(third, item), UNIT)
        hop_copy(third, item, 2).wait_recv()
        part[0, 0, 0, rows, :] = (part[0, 0, 0, rows, :] + recv2[rows, :]) / SIXTEEN

    stages = ((0, stage0), (LAG, stage1), (2 * LAG, stage2), (3 * LAG, stage3),
              (3 * LAG + 1, lambda item, third: out_copy(third, item).start()))

    @pl.loop(0, ITEMS + stages[-1][0])
    def _(step):
        for delay, stage in stages:
            @pl.when((step >= delay) & (step < ITEMS + delay))
            def _():
                for third in range(3):
                    stage(step - delay, third)

        @pl.when((step % 2 == 0) & (step + 2 < ITEMS))
        def _():
            start_group(step // 2 + 1, (step // 2 + 1) % 2)

    for third in range(3):
        pair_all(third, 0, True).wait_send()
        for hop in range(3):
            hop_copy(third, 0, hop, True).wait_send()
        out_copy(third, 0, True).wait()

    for n, ref in enumerate((m_ref, v_ref, w_ref)):
        pltpu.make_async_remote_copy(
            src_ref=ref.at[pl.ds(0, EDGE)], dst_ref=edge_ref.at[pl.ds(n * EDGE, EDGE)],
            send_sem=edge_send.at[n], recv_sem=edge_recv.at[n],
            device_id=(before // 8, before // 4 % 2, before % 4), device_id_type=MESH).wait()


def scatter(grads, m, v, w):
    any_spec = pl.BlockSpec(memory_space=pl.ANY)
    dma = pltpu.SemaphoreType.DMA
    return pl.pallas_call(
        scatter_kernel,
        out_shape=(jax.ShapeDtypeStruct((WINDOW, LANES), jnp.float32), jax.ShapeDtypeStruct((3 * EDGE,), jnp.float32)),
        in_specs=[any_spec] * 8,
        out_specs=(any_spec, any_spec),
        scratch_shapes=[
            pltpu.VMEM((2, 2, 2, WINDOW, LANES), jnp.float32),
            pltpu.VMEM((2, 2, WINDOW, LANES), jnp.float32),
            pltpu.VMEM((2, WINDOW, LANES), jnp.float32),
            pltpu.VMEM((WINDOW, LANES), jnp.float32),
            pltpu.VMEM((2, 3, 2, 2, 2, GROUP, LANES), jnp.float32),
            dma((3,)), dma((3, ITEMS // 2)), dma((2, 3)),
            dma((3, 3)), dma((3, 3, ITEMS)), dma((3,)), dma((3,)), dma((3,)),
        ],
        compiler_params=pltpu.CompilerParams(has_side_effects=True, vmem_limit_bytes=67043328),
    )(*grads, m, v, w)


def gather_kernel(w_ref, full_ref, pair_send, pair_recv, send, arrive):
    z, y, x, core = position()
    here = (z, y, x)

    def rows_of(third, item, whole=False):
        if whole:
            return pl.ds(third * OWN_THIRD, OWN_THIRD)
        return pl.ds(pl.multiple_of(third * OWN_THIRD + item * OWN_CHUNK, OWN_CHUNK), OWN_CHUNK)

    def copy(third, item, hop, whole=False):
        rows = rows_of(third, item, whole)
        order = ORDERS[third]
        if hop == 0:
            source = w_ref.at[rows, :]
            target = full_ref.at[z, y, x, core, rows, :]
        else:
            index = tuple(slice(None) if n in order[:hop] else here[n] for n in range(3))
            source = target = full_ref.at[index + (core, rows, slice(None))]
        return pltpu.make_async_remote_copy(
            src_ref=source, dst_ref=target, send_sem=send.at[third, hop], recv_sem=arrive.at[third, item, hop],
            device_id=neighbour(order[hop]), device_id_type=MESH)

    def arrival(third, item, hop):
        order = ORDERS[third]
        index = tuple(slice(None) if n in order[:hop] else (1 - here[n] if n == order[hop] else here[n]) for n in range(3))
        block = full_ref.at[index + (core, rows_of(third, item), slice(None))]
        return pltpu.make_async_remote_copy(
            src_ref=block, dst_ref=block, send_sem=send.at[third, hop], recv_sem=arrive.at[third, item, hop],
            device_id=neighbour(order[hop]), device_id_type=MESH)

    def pair(third, item, side, whole=False):
        block = full_ref.at[:, :, :, side, rows_of(third, item, whole), :]
        return pltpu.make_async_remote_copy(
            src_ref=block, dst_ref=block, send_sem=pair_send.at[third], recv_sem=pair_recv.at[third, item],
            device_id=neighbour(3), device_id_type=MESH)

    for item in range(OWN_LAG):
        for third in range(3):
            copy(third, item, 0).start()

    @pl.loop(0, OWN // OWN_CHUNK)
    def _(n):
        rows = pl.ds(pl.multiple_of(n * OWN_CHUNK, OWN_CHUNK), OWN_CHUNK)
        full_ref[z, y, x, core, rows, :] = w_ref[rows, :]

    @pl.loop(0, OWN_ITEMS + 2 * OWN_LAG)
    def _(step):
        @pl.when(step + OWN_LAG < OWN_ITEMS)
        def _():
            for third in range(3):
                copy(third, step + OWN_LAG, 0).start()

        for hop in range(1, 4):
            delay = (hop - 1) * OWN_LAG

            @pl.when((step >= delay) & (step < OWN_ITEMS + delay))
            def _():
                item = step - delay
                for third in range(3):
                    arrival(third, item, hop - 1).wait_recv()
                    if hop < 3:
                        copy(third, item, hop).start()
                    else:
                        pair(third, item, core).start()

    @pl.loop(0, OWN_ITEMS)
    def _(item):
        for third in range(3):
            pair(third, item, 1 - core).wait_recv()
    for third in range(3):
        pair(third, 0, core, True).wait_send()
        for hop in range(3):
            copy(third, 0, hop, True).wait_send()


def gather(w_own):
    dma = pltpu.SemaphoreType.DMA
    return pl.pallas_call(
        gather_kernel,
        out_shape=jax.ShapeDtypeStruct((2, 2, 2, 2, OWN, LANES), jnp.bfloat16),
        in_specs=[pl.BlockSpec(memory_space=pltpu.VMEM)],
        out_specs=pl.BlockSpec(memory_space=pltpu.VMEM),
        scratch_shapes=[
            dma((3,)), dma((3, OWN_ITEMS)), dma((3, 3)), dma((3, OWN_ITEMS, 3)),
        ],
        compiler_params=pltpu.CompilerParams(has_side_effects=True, vmem_limit_bytes=GATHER_LIMIT),
    )(w_own)


def device_index():
    outer, middle, inner = (lax.axis_index(name) for name in MESH_AXES)
    return (outer * 2 + middle) * 4 + inner


def for_blocks(start, length, action, tensors=TENSORS):
    for base, end, tiles in tensors:
        block = 8 * tiles
        low = (jnp.maximum(start, base) - base + block - 1) // block
        high = jnp.maximum(jnp.minimum(start + length, end) - base, 0) // block

        @pl.loop(low, jnp.maximum(high, low))
        def _(n):
            action(pl.multiple_of(base + n * block - start, 8), tiles)


PAD = 8
FLAT_ROWS = WINDOW + 272
SHARD_VREGS = SLICE // 1024
TAIL_ROWS = SLICE % 1024 // LANES
TAIL_LANES = SLICE % LANES
EDGE_ROWS = EDGE // LANES
OWN_FLAT_ROWS = OWN + 512


def lane_index(rows=8):
    return lax.broadcasted_iota(jnp.int32, (rows, LANES), 1)


BATCH = 128
BATCHES = SHARD_VREGS * 8 // BATCH
CHUNK_BATCHES = 6
CHUNKS = BATCHES // CHUNK_BATCHES
CHUNK = CHUNK_BATCHES * BATCH * LANES


def mid_kernel(tile_ref, m_ref, v_ref, w_ref, edge_ref, m_out, v_out, w_out, own_ref,
               m_buf, v_buf, w_buf, flat, shifted, edged, aligned, in_sem, out_sem):
    device = device_index()
    start = window_start(device)
    arrays = ((m_ref, m_buf, m_out), (v_ref, v_buf, v_out), (w_ref, w_buf, w_out))

    def span(chunk):
        return pl.ds(chunk * CHUNK, CHUNK if chunk < CHUNKS - 1 else SLICE - chunk * CHUNK)

    def loads(chunk):
        return [pltpu.make_async_copy(ref.at[span(chunk)], buf.at[span(chunk)], in_sem.at[n, chunk])
                for n, (ref, buf, _) in enumerate(arrays)]

    def stores(chunk):
        return [pltpu.make_async_copy(buf.at[span(chunk)], out.at[span(chunk)], out_sem.at[n, chunk])
                for n, (_, buf, out) in enumerate(arrays)]

    for chunk in range(CHUNKS):
        for copy in loads(chunk):
            copy.start()

    def to_flat(row, tiles):
        for t in range(tiles):
            flat[pl.ds(row + t, 8, stride=tiles), :] = tile_ref[pl.ds(row + 8 * t, 8), :]
    for_blocks(start, WINDOW, to_flat)

    first_row = device * (SLICE // 16) // 8
    next_row = (device + 1) * (SLICE // 16) // 8
    shift = device * SLICE - first_row * LANES
    next_shift = (device + 1) * SLICE - next_row * LANES

    def mean_rows(row, amount, rows):
        here = flat[pl.ds(row, rows), :]
        below = flat[pl.ds(row + 1, rows), :]
        back = (LANES - amount) % LANES
        return jnp.where(lane_index(rows) < LANES - amount, pltpu.roll(here, back, 1), pltpu.roll(below, back, 1))

    for chunk in range(CHUNKS):
        for copy in loads(chunk):
            copy.wait()

        @pl.loop(chunk * CHUNK_BATCHES, (chunk + 1) * CHUNK_BATCHES)
        def _(n):
            at = pl.ds(pl.multiple_of(n * BATCH * LANES, BATCH * LANES), BATCH * LANES)
            mean = mean_rows(first_row - start + n * BATCH, shift, BATCH)
            new = adam_update(mean, *(buf[at].reshape(BATCH, LANES) for _, buf, _ in arrays))
            for (_, buf, _), value in zip(arrays, new):
                buf[at] = value.reshape(BATCH * LANES)
            shifted[pl.ds(pl.multiple_of(PAD + n * BATCH, 8), BATCH), :] = pltpu.roll(new[2], shift, 1)

        if chunk > 0:
            for copy in stores(chunk - 1):
                copy.start()

    mean = mean_rows(first_row - start + SHARD_VREGS * 8, shift, 8)
    for r in range(TAIL_ROWS + 1):
        size = LANES if r < TAIL_ROWS else TAIL_LANES
        at = pl.ds(SHARD_VREGS * 1024 + r * LANES, size)
        new = adam_update(mean[r:r + 1, :size], *(buf[at].reshape(1, size) for _, buf, _ in arrays))
        for (_, buf, _), value in zip(arrays, new):
            buf[at] = value.reshape(size)
        flat[pl.ds(FLAT_ROWS - 8 + r, 1), pl.ds(0, size)] = new[2]
    shifted[pl.ds(PAD + SHARD_VREGS * 8, 8), :] = pltpu.roll(flat[pl.ds(FLAT_ROWS - 8, 8), :], shift, 1)

    @pl.loop(0, EDGE_ROWS // 64)
    def _(n):
        mean = mean_rows(next_row - start + n * 64, next_shift, 64)
        old = (edge_ref[pl.ds(pl.multiple_of(k * EDGE + n * 8192, 1024), 8192)].reshape(64, LANES) for k in range(3))
        edged[pl.ds(pl.multiple_of(PAD + n * 64, 8), 64), :] = pltpu.roll(adam_update(mean, *old)[2], next_shift, 1)

    for copy in stores(CHUNKS - 1):
        copy.start()

    own = own_start(device)
    skip = own - first_row

    @pl.loop(0, BATCHES + 1)
    def _(n):
        row = PAD + skip + n * BATCH
        aligned[pl.ds(pl.multiple_of(n * BATCH, 8), BATCH), :] = jnp.where(
            lane_index(BATCH) >= shift, shifted[pl.ds(row, BATCH), :], shifted[pl.ds(row - 1, BATCH), :])
    edged[pl.ds(PAD - 1, 1), :] = aligned[pl.ds(next_row - own, 1), :]

    @pl.loop(0, EDGE_ROWS // 64)
    def _(n):
        row = PAD + n * 64
        aligned[pl.ds(next_row - own + n * 64, 64), :] = jnp.where(
            lane_index(64) >= next_shift, edged[pl.ds(row, 64), :], edged[pl.ds(row - 1, 64), :])

    def to_tile(row, tiles):
        for t in range(0, tiles, 2):
            both = [aligned[pl.ds(row + t + k, 8, stride=tiles), :] for k in range(2)]
            own_ref[pl.ds(pl.multiple_of(row + 8 * t, 16), 16), :] = jnp.concatenate(both, axis=0).astype(jnp.bfloat16)

    def plain(row, _):
        own_ref[pl.ds(pl.multiple_of(row, 16), 16), :] = aligned[pl.ds(row, 16), :].astype(jnp.bfloat16)
    for_blocks(own, OWN, to_tile, TENSORS[:4])
    for_blocks(own, OWN, plain, ((*TENSORS[4][:2], 2),))

    for chunk in range(CHUNKS):
        for copy in stores(chunk):
            copy.wait()


def mid(mean_tiles, m, v, w, edges):
    vmem = pl.BlockSpec(memory_space=pltpu.VMEM)
    any_spec = pl.BlockSpec(memory_space=pl.ANY)
    shard = jax.ShapeDtypeStruct((SLICE,), jnp.float32)
    return pl.pallas_call(
        mid_kernel,
        out_shape=(shard, shard, shard, jax.ShapeDtypeStruct((OWN, LANES), jnp.bfloat16)),
        in_specs=[vmem, any_spec, any_spec, any_spec, vmem], out_specs=(any_spec, any_spec, any_spec, vmem),
        scratch_shapes=[
            pltpu.VMEM((SLICE,), jnp.float32), pltpu.VMEM((SLICE,), jnp.float32), pltpu.VMEM((SLICE,), jnp.float32),
            pltpu.VMEM((FLAT_ROWS, LANES), jnp.float32),
            pltpu.VMEM((PAD + SHARD_VREGS * 8 + 8 + 512, LANES), jnp.float32),
            pltpu.VMEM((PAD + EDGE_ROWS, LANES), jnp.float32),
            pltpu.VMEM((OWN_FLAT_ROWS, LANES), jnp.float32),
            pltpu.SemaphoreType.DMA((3, CHUNKS)), pltpu.SemaphoreType.DMA((3, CHUNKS)),
        ],
        compiler_params=pltpu.CompilerParams(vmem_limit_bytes=MID_LIMIT),
    )(mean_tiles, m, v, w, edges)


def pieces_of(tensor):
    base, end, _ = TENSORS[tensor]
    for d in range(SIXTEEN):
        low, high = max(OWN_STARTS[d], base), min(OWN_STARTS[d + 1], end)
        if low < high:
            yield d, low - OWN_STARTS[d], low - base, high - low


PIECES = [(tensor,) + piece for tensor in range(4) for piece in pieces_of(tensor)]
VEC_WIDTH = 12032
VEC_ROWS = VEC_WIDTH // LANES
VEC_BLOCK = VEC_WIDTH // 8
CHIP_COUNTS = tuple((end - base) // 8 for base, end, _ in TENSORS[:4])
CHIP_ROWS = sum(CHIP_COUNTS)
CHIP_SIZE = CHIP_ROWS * LANES + VEC_BLOCK
CHIP_PARTS = 6
CHIP_PART = CHIP_SIZE // 16384 // CHIP_PARTS * 16384


def final_kernel(full_ref, e_out, a_out, f_out, h_out, vec_out, chip_ref, chip_out, flat, vec, out_sem, chip_sem):
    outs = (e_out, a_out, f_out, h_out)
    chip = device_index() // 2
    copies = []
    for n, (tensor, d, source, target, rows) in enumerate(PIECES):
        copies.append(pltpu.make_async_copy(
            full_ref.at[d, pl.ds(source, rows), :], outs[tensor].at[pl.ds(target, rows), :], out_sem.at[n]))
        copies[-1].start()

    slot, source, _, _ = next(pieces_of(4))
    vec[pl.ds(0, 96), :] = full_ref[slot, pl.ds(source, 96), :].astype(jnp.float32)
    for n in range(VEC_ROWS // 8):
        vec_out[:, n * 1024:(n + 1) * 1024] = vec[n * 8:n * 8 + 8, :].reshape(1, 1024).astype(jnp.bfloat16)
    rest = VEC_ROWS % 8
    vec_out[:, VEC_ROWS // 8 * 1024:] = vec[pl.ds(VEC_ROWS - rest, rest), :].reshape(1, rest * LANES).astype(jnp.bfloat16)

    offset = 0
    for tensor, rows in enumerate(CHIP_COUNTS):
        base, _, tiles = TENSORS[tensor]
        step = 16 * tiles

        begin = base + chip * rows
        slot, low, bound = jnp.int32(0), jnp.int32(0), jnp.int32(OWN_STARTS[1])
        for d in range(1, SIXTEEN):
            inside = begin >= OWN_STARTS[d]
            slot = jnp.where(inside, d, slot)
            low = jnp.where(inside, OWN_STARTS[d], low)
            bound = jnp.where(inside, OWN_STARTS[d + 1], bound)

        @pl.loop(0, rows // step)
        def _(n):
            for half in range(2):
                row = begin + n * step + half * 8 * tiles
                following = row >= bound
                at_slot = jnp.where(following, slot + 1, slot)
                at_row = row - jnp.where(following, bound, low)
                for t in range(0, tiles, 2):
                    value = full_ref[at_slot, pl.ds(pl.multiple_of(at_row + 8 * t, 16), 16), :].astype(jnp.float32)
                    for k in range(2):
                        to = offset + n * step + half * 8 * tiles + t + k
                        flat[pl.ds(to, 8, stride=tiles), :] = value[8 * k:8 * k + 8]
        offset += rows

    vec_row = chip * (VEC_BLOCK // 32) // 4
    amount = chip * VEC_BLOCK - vec_row * LANES
    back = (LANES - amount) % LANES
    lane = lane_index()
    for n in range(2):
        here, below = vec[pl.ds(vec_row + n * 8, 8), :], vec[pl.ds(vec_row + n * 8 + 1, 8), :]
        flat[pl.ds(CHIP_ROWS + n * 8, 8), :] = jnp.where(
            lane < LANES - amount, pltpu.roll(here, back, 1), pltpu.roll(below, back, 1))

    def part_copy(part):
        span = pl.ds(part * CHIP_PART, CHIP_PART if part < CHIP_PARTS - 1 else CHIP_SIZE - part * CHIP_PART)
        return pltpu.make_async_copy(chip_out.at[:, span], chip_ref.at[:, span], chip_sem.at[part])

    for part in range(CHIP_PARTS):
        @pl.loop(part * CHIP_PART // 16384, (part + 1) * CHIP_PART // 16384)
        def _(n):
            chip_out[:, pl.ds(pl.multiple_of(n * 16384, 16384), 16384)] = flat[
                pl.ds(pl.multiple_of(n * 128, 128), 128), :].reshape(1, 16384).astype(jnp.bfloat16)
        if part > 0:
            part_copy(part - 1).start()
    done = CHIP_SIZE // 1024 * 1024
    rows = (CHIP_SIZE - done) // LANES
    last = CHIP_SIZE - done - rows * LANES
    first = done // LANES
    chip_out[:, CHIP_PARTS * CHIP_PART:done] = flat[CHIP_PARTS * CHIP_PART // LANES:first, :].reshape(
        1, done - CHIP_PARTS * CHIP_PART).astype(jnp.bfloat16)
    chip_out[:, done:done + rows * LANES] = flat[first:first + rows, :].reshape(1, rows * LANES).astype(jnp.bfloat16)
    chip_out[:, CHIP_SIZE - last:] = flat[first + rows:first + rows + 1, :last].astype(jnp.bfloat16)
    part_copy(CHIP_PARTS - 1).start()
    for part in range(CHIP_PARTS):
        part_copy(part).wait()
    for copy in copies:
        copy.wait()


def finish(full):
    vmem = pl.BlockSpec(memory_space=pltpu.VMEM)
    any_spec = pl.BlockSpec(memory_space=pl.ANY)
    shape = lambda rows: jax.ShapeDtypeStruct((rows, LANES), jnp.bfloat16)
    return pl.pallas_call(
        final_kernel,
        out_shape=tuple(shape(end - base) for base, end, _ in TENSORS[:4]) + (
            jax.ShapeDtypeStruct((1, VEC_WIDTH), jnp.bfloat16), jax.ShapeDtypeStruct((1, CHIP_SIZE), jnp.bfloat16)),
        in_specs=[vmem], out_specs=(any_spec,) * 4 + (vmem, any_spec),
        scratch_shapes=[
            pltpu.VMEM((1, CHIP_SIZE), jnp.bfloat16),
            pltpu.VMEM((CHIP_ROWS + 16, LANES), jnp.float32),
            pltpu.VMEM((120, LANES), jnp.float32),
            pltpu.SemaphoreType.DMA((len(PIECES),)), pltpu.SemaphoreType.DMA((CHIP_PARTS,)),
        ],
        compiler_params=pltpu.CompilerParams(vmem_limit_bytes=FINAL_LIMIT),
    )(full)


def solution(mesh):
    def local_step(g_embed, g_attn, g_ffn_in, g_ffn_out, g_vec, m_shard, v_shard, w_shard):
        matrices = (g_embed, g_attn, g_ffn_in, g_ffn_out)
        grads = [to_tiles(g[0] if g.ndim == 3 else g[0, 0]) for g in matrices]
        grads.append(jnp.pad(g_vec.reshape(-1), (0, VEC_BLOCK_ROWS * LANES - VEC_WIDTH)).reshape(VEC_BLOCK_ROWS, LANES))
        mean_tiles, edges = scatter(grads, m_shard, v_shard, w_shard)
        m_new, v_new, w_new, w_own = mid(mean_tiles, m_shard, v_shard, w_shard, edges)
        full = gather(w_own).reshape(SIXTEEN, OWN, LANES)
        *tiles, vec, w_chip = finish(full)
        tensors = [from_tiles(t, g.shape[-1]).reshape(g.shape[1:]) for t, g in zip(tiles, matrices)]
        return (m_new, v_new, w_new) + tuple(tensors) + (vec, w_chip)

    return jax.shard_map(local_step, mesh=mesh, in_specs=(P(MESH_AXES),) * 8, out_specs=(P(MESH_AXES),) * 3 + (P(),) * 5 + (P(MESH_AXES),), check_vma=False)
```

```python
import functools
import math
import jax
import jax.numpy as jnp
from jax import lax
from jax.experimental import pallas as pl
from jax.experimental.pallas import tpu as pltpu
from jax.sharding import PartitionSpec as P

MESH_AXES = ('outer', 'middle', 'inner')
MESH = pl.DeviceIdType.MESH
ADAM_BETA1 = 0.9
ADAM_BETA2 = 0.98
ADAM_EPS = 1e-9
LEARN_RATE = 0.05
ADAM_STEP = 3

LANES = 128
SLICE = 885488
TENSORS = ((0, 32768, 8), (32768, 65536, 32), (65536, 88064, 22), (88064, 110592, 8), (110592, 110720, 1))
ROWS = 110720
VEC_BLOCK_ROWS = 128
UNIT = 64
GROUP = 128
COMMON = 7168
WINDOW = COMMON + GROUP
LONG_SLICE = 10
COUNTS = (38, 38, 36)
FIRSTS = (0, 38, 76)
ITEMS = max(COUNTS)
LAG = 2
EDGE = 32768
OWN = 7104
OWN_THIRD = OWN // 3
OWN_CHUNK = 64
OWN_ITEMS = OWN_THIRD // OWN_CHUNK
OWN_LAG = 2
SIXTEEN = 16
FINAL_LIMIT = 20000000
GATHER_LIMIT = 6000000
MID_LIMIT = 64000000


def floor_block(row):
    result = row
    for base, end, tiles in TENSORS:
        block = 8 * tiles if tiles > 1 else VEC_BLOCK_ROWS
        floored = base + (row - base) // block * block
        result = jnp.where((row >= base) & (row < end), floored, result)
    return result


def window_start(index):
    row = floor_block(index * (SLICE // 16) // 8)
    return jnp.minimum(row // GROUP * GROUP, ROWS - COMMON)


def own_start_static(index):
    row = -(-index * SLICE // LANES)
    for base, end, tiles in TENSORS:
        if base <= row < end:
            block = 8 * tiles if tiles > 1 else VEC_BLOCK_ROWS
            return base + -(-(row - base) // block) * block
    return ROWS


OWN_STARTS = [own_start_static(d) for d in range(SIXTEEN)] + [ROWS]


def own_start(index):
    result = jnp.int32(0)
    for d in range(SIXTEEN):
        result = jnp.where(index == d, OWN_STARTS[d], result)
    return result


def adam_update(grad_mean, m_old, v_old, w_old):
    m_new = ADAM_BETA1 * m_old + (1.0 - ADAM_BETA1) * grad_mean
    v_new = ADAM_BETA2 * v_old + (1.0 - ADAM_BETA2) * (grad_mean * grad_mean)
    scale = LEARN_RATE / (1.0 - ADAM_BETA1 ** ADAM_STEP)
    w_new = w_old - scale * m_new / (jnp.sqrt(v_new * (1.0 / (1.0 - ADAM_BETA2 ** ADAM_STEP))) + ADAM_EPS)
    return m_new, v_new, w_new


def to_tiles(tensor):
    rows, width = tensor.shape
    return tensor.reshape(rows // 8, 8, width // LANES, LANES).transpose(0, 2, 1, 3).reshape(-1, LANES)


def from_tiles(tiles, width):
    return tiles.reshape(-1, width // LANES, 8, LANES).transpose(0, 2, 1, 3).reshape(-1, width)


ORDERS = ((0, 1, 2), (1, 2, 0), (2, 0, 1))


def position():
    outer, middle, inner = (lax.axis_index(name) for name in MESH_AXES)
    return outer, middle, inner // 2, inner % 2


def neighbour(axis):
    outer, middle, x, core = position()
    z, y = outer, middle
    if axis == 0:
        z = 1 - z
    elif axis == 1:
        y = 1 - y
    elif axis == 2:
        x = 1 - x
    else:
        core = 1 - core
    return (z, y, 2 * x + core)


def scatter_kernel(e_ref, a_ref, f_ref, h_ref, b_ref, m_ref, v_ref, w_ref, out_ref, edge_ref,
                   part, recv0, recv1, recv2, mine, pair_send, pair_recv, mine_sem,
                   send, arrive, out_sem, edge_send, edge_recv, long_mine, long_part, long_recv, long_sem):
    z, y, x, core = position()
    chip = (z * 2 + y) * 2 + x
    device = chip * 2 + core
    sources = (e_ref, a_ref, f_ref, h_ref, b_ref)

    before = (device + SIXTEEN - 1) % SIXTEEN
    for n, ref in enumerate((m_ref, v_ref, w_ref)):
        pltpu.make_async_remote_copy(
            src_ref=ref.at[pl.ds(0, EDGE)], dst_ref=edge_ref.at[pl.ds(n * EDGE, EDGE)],
            send_sem=edge_send.at[n], recv_sem=edge_recv.at[n],
            device_id=(before // 8, before // 4 % 2, before % 4), device_id_type=MESH).start()

    def from_source(row, action):
        def choose(low, high):
            if high - low == 1:
                action(sources[low].at[pl.ds(pl.multiple_of(row - TENSORS[low][0], GROUP), GROUP), :])
                return
            middle = (low + high) // 2
            lax.cond(row < TENSORS[middle][0], lambda: choose(low, middle), lambda: choose(middle, high))
        choose(0, len(sources))

    def item_row(third, item):
        return pl.multiple_of((FIRSTS[third] + item) * UNIT, UNIT)

    def each_third(index, counts, action):
        for third in range(3):
            if counts[third] == max(counts):
                action(third)
            else:
                @pl.when(index < counts[third])
                def _():
                    action(third)

    def group_row(third, group):
        return pl.multiple_of(FIRSTS[third] * UNIT + group * GROUP, GROUP)

    def start_group(group, slot):
        @pl.loop(0, 8)
        def _(j):
            jz, jy, jx = j // 4, j // 2 % 2, j % 2
            other = ((z + jz) % 2 * 2 + (y + jy) % 2) * 2 + (x + jx) % 2
            theirs = window_start(other * 2 + 1 - core)
            ours = window_start(other * 2 + core)

            def action(third):
                row = group_row(third, group)
                from_source(theirs + row, lambda src: pltpu.make_async_remote_copy(
                    src_ref=src, dst_ref=part.at[jz, jy, jx, pl.ds(row, GROUP), :],
                    send_sem=pair_send.at[third], recv_sem=pair_recv.at[third, group],
                    device_id=neighbour(3), device_id_type=MESH).start())
                from_source(ours + row, lambda src: pltpu.make_async_copy(
                    src, mine.at[slot, third, jz, jy, jx], mine_sem.at[slot, third]).start())
            each_third(group, [count // 2 for count in COUNTS], action)

    def hop_copy(third, item, hop, whole=False):
        rows = pl.ds(item_row(third, 0), COUNTS[third] * UNIT) if whole else pl.ds(item_row(third, item), UNIT)
        first, second, last = ORDERS[third]
        if hop == 0:
            index = tuple(1 if n == first else slice(None) for n in range(3))
            target = recv0.at[:, :, rows, :]
        elif hop == 1:
            index = tuple(0 if n == first else 1 if n == second else slice(None) for n in range(3))
            target = recv1.at[:, rows, :]
        else:
            index = tuple(1 if n == last else 0 for n in range(3))
            target = recv2.at[rows, :]
        return pltpu.make_async_remote_copy(
            src_ref=part.at[index + (rows, slice(None))], dst_ref=target,
            send_sem=send.at[third, hop], recv_sem=arrive.at[third, hop, item],
            device_id=neighbour(ORDERS[third][hop]), device_id_type=MESH)

    def pair_all(third, group, whole=False):
        rows = pl.ds(FIRSTS[third] * UNIT, COUNTS[third] * UNIT) if whole else pl.ds(group_row(third, group), GROUP)
        block = part.at[:, :, :, rows, :]
        return pltpu.make_async_remote_copy(
            src_ref=block, dst_ref=block, send_sem=pair_send.at[third], recv_sem=pair_recv.at[third, group],
            device_id=neighbour(3), device_id_type=MESH)

    def out_copy(third, item, whole=False):
        rows = pl.ds(item_row(third, 0), COUNTS[third] * UNIT) if whole else pl.ds(item_row(third, item), UNIT)
        return pltpu.make_async_copy(part.at[0, 0, 0, rows, :], out_ref.at[rows, :], out_sem.at[third])

    start_group(0, 0)

    def stage0(item, third):
        rows = pl.ds(item_row(third, item), UNIT)
        group = item // 2
        slot = group % 2

        @pl.when(item % 2 == 0)
        def _():
            pltpu.make_async_copy(mine.at[slot, third], mine.at[slot, third], mine_sem.at[slot, third]).wait()
            pair_all(third, group).wait_recv()
        within = pl.ds(pl.multiple_of(item % 2 * UNIT, UNIT), UNIT)
        for j in range(8):
            index = (j // 4, j // 2 % 2, j % 2)
            part[index + (rows, slice(None))] += mine[(slot, third) + index + (within, slice(None))]
        hop_copy(third, item, 0).start()

    def stage1(item, third):
        rows = pl.ds(item_row(third, item), UNIT)
        hop_copy(third, item, 0).wait_recv()
        first = ORDERS[third][0]
        for j in range(4):
            pair = [j // 2, j % 2]
            index = tuple(pair[:first] + [0] + pair[first:])
            part[index + (rows, slice(None))] += recv0[j // 2, j % 2, rows, :]
        hop_copy(third, item, 1).start()

    def stage2(item, third):
        rows = pl.ds(item_row(third, item), UNIT)
        hop_copy(third, item, 1).wait_recv()
        last = ORDERS[third][2]
        for j in range(2):
            index = tuple(j if n == last else 0 for n in range(3))
            part[index + (rows, slice(None))] += recv1[j, rows, :]
        hop_copy(third, item, 2).start()

    def stage3(item, third):
        rows = pl.ds(item_row(third, item), UNIT)
        hop_copy(third, item, 2).wait_recv()
        part[0, 0, 0, rows, :] = (part[0, 0, 0, rows, :] + recv2[rows, :]) / SIXTEEN

    long_chip, long_core = LONG_SLICE // 2, LONG_SLICE % 2
    lz, ly, lx = (z + long_chip // 4) % 2, (y + long_chip // 2 % 2) % 2, (x + long_chip % 2) % 2
    long_row = window_start(LONG_SLICE) + COMMON
    holder = core == long_core

    def long_pair():
        return pltpu.make_async_remote_copy(
            src_ref=long_mine, dst_ref=long_part, send_sem=long_sem.at[0], recv_sem=long_sem.at[1],
            device_id=neighbour(3), device_id_type=MESH)

    def long_load():
        return pltpu.make_async_copy(
            sources[2].at[pl.ds(pl.multiple_of(long_row - TENSORS[2][0], GROUP), GROUP), :], long_mine, long_sem.at[2])

    def long_hop(hop):
        return pltpu.make_async_remote_copy(
            src_ref=long_part, dst_ref=long_recv.at[hop], send_sem=long_sem.at[3 + hop], recv_sem=long_sem.at[6 + hop],
            device_id=neighbour((2, 0, 1)[hop]), device_id_type=MESH)

    def long_out():
        return pltpu.make_async_copy(long_part, out_ref.at[pl.ds(COMMON, GROUP), :], long_sem.at[9])

    reached = (holder, holder & (lx == 0), holder & (lx == 0) & (lz == 0), holder & (lx == 0) & (lz == 0) & (ly == 0))
    far = (lx == 1, lz == 1, ly == 1)

    def long_start():
        long_load().start()

    def long_exchange():
        long_load().wait()

        @pl.when(core != long_core)
        def _():
            long_pair().start()

    def long_sum():
        @pl.when(holder)
        def _():
            long_pair().wait_recv()
            long_part[...] += long_mine[...]

        @pl.when(core != long_core)
        def _():
            long_pair().wait_send()

    def long_send(hop):
        @pl.when(reached[hop] & far[hop])
        def _():
            long_hop(hop).start()

    def long_add(hop):
        @pl.when(reached[hop] & far[hop])
        def _():
            long_hop(hop).wait_send()

        @pl.when(reached[hop + 1])
        def _():
            long_hop(hop).wait_recv()
            if hop < 2:
                long_part[...] += long_recv[hop]
            else:
                long_part[...] = (long_part[...] + long_recv[hop]) / SIXTEEN

    def long_store():
        @pl.when(reached[3])
        def _():
            long_out().start()

    long_stages = ((4, long_start), (6, long_exchange), (8, long_sum)) + tuple(
        (9 + 3 * hop + k, functools.partial((long_send, long_add)[k // 2], hop)) for hop in range(3) for k in (0, 2)
    ) + ((19, long_store),)

    stages = ((0, stage0), (LAG, stage1), (2 * LAG, stage2), (3 * LAG, stage3),
              (3 * LAG + 1, lambda item, third: out_copy(third, item).start()))

    @pl.loop(0, ITEMS + stages[-1][0])
    def _(step):
        for delay, stage in stages:
            @pl.when((step >= delay) & (step < ITEMS + delay))
            def _():
                each_third(step - delay, COUNTS, functools.partial(stage, step - delay))

        for at, stage in long_stages:
            @pl.when(step == at)
            def _():
                stage()

        @pl.when((step % 2 == 0) & (step + 2 < ITEMS))
        def _():
            start_group(step // 2 + 1, (step // 2 + 1) % 2)

    for third in range(3):
        pair_all(third, 0, True).wait_send()
        for hop in range(3):
            hop_copy(third, 0, hop, True).wait_send()
        out_copy(third, 0, True).wait()

    @pl.when(reached[3])
    def _():
        long_out().wait()

    for n, ref in enumerate((m_ref, v_ref, w_ref)):
        pltpu.make_async_remote_copy(
            src_ref=ref.at[pl.ds(0, EDGE)], dst_ref=edge_ref.at[pl.ds(n * EDGE, EDGE)],
            send_sem=edge_send.at[n], recv_sem=edge_recv.at[n],
            device_id=(before // 8, before // 4 % 2, before % 4), device_id_type=MESH).wait()


def scatter(grads, m, v, w):
    any_spec = pl.BlockSpec(memory_space=pl.ANY)
    dma = pltpu.SemaphoreType.DMA
    return pl.pallas_call(
        scatter_kernel,
        out_shape=(jax.ShapeDtypeStruct((WINDOW, LANES), jnp.float32), jax.ShapeDtypeStruct((3 * EDGE,), jnp.float32)),
        in_specs=[any_spec] * 8,
        out_specs=(any_spec, any_spec),
        scratch_shapes=[
            pltpu.VMEM((2, 2, 2, COMMON, LANES), jnp.float32),
            pltpu.VMEM((2, 2, COMMON, LANES), jnp.float32),
            pltpu.VMEM((2, COMMON, LANES), jnp.float32),
            pltpu.VMEM((COMMON, LANES), jnp.float32),
            pltpu.VMEM((2, 3, 2, 2, 2, GROUP, LANES), jnp.float32),
            dma((3,)), dma((3, ITEMS // 2)), dma((2, 3)),
            dma((3, 3)), dma((3, 3, ITEMS)), dma((3,)), dma((3,)), dma((3,)),
            pltpu.VMEM((GROUP, LANES), jnp.float32), pltpu.VMEM((GROUP, LANES), jnp.float32),
            pltpu.VMEM((3, GROUP, LANES), jnp.float32), dma((10,)),
        ],
        compiler_params=pltpu.CompilerParams(has_side_effects=True, vmem_limit_bytes=67043328),
    )(*grads, m, v, w)


def gather_kernel(w_ref, full_ref, pair_send, pair_recv, send, arrive):
    z, y, x, core = position()
    here = (z, y, x)

    def rows_of(third, item, whole=False):
        if whole:
            return pl.ds(third * OWN_THIRD, OWN_THIRD)
        return pl.ds(pl.multiple_of(third * OWN_THIRD + item * OWN_CHUNK, OWN_CHUNK), OWN_CHUNK)

    def copy(third, item, hop, whole=False):
        rows = rows_of(third, item, whole)
        order = ORDERS[third]
        if hop == 0:
            source = w_ref.at[rows, :]
            target = full_ref.at[z, y, x, core, rows, :]
        else:
            index = tuple(slice(None) if n in order[:hop] else here[n] for n in range(3))
            source = target = full_ref.at[index + (core, rows, slice(None))]
        return pltpu.make_async_remote_copy(
            src_ref=source, dst_ref=target, send_sem=send.at[third, hop], recv_sem=arrive.at[third, item, hop],
            device_id=neighbour(order[hop]), device_id_type=MESH)

    def arrival(third, item, hop):
        order = ORDERS[third]
        index = tuple(slice(None) if n in order[:hop] else (1 - here[n] if n == order[hop] else here[n]) for n in range(3))
        block = full_ref.at[index + (core, rows_of(third, item), slice(None))]
        return pltpu.make_async_remote_copy(
            src_ref=block, dst_ref=block, send_sem=send.at[third, hop], recv_sem=arrive.at[third, item, hop],
            device_id=neighbour(order[hop]), device_id_type=MESH)

    def pair(third, item, side, whole=False):
        block = full_ref.at[:, :, :, side, rows_of(third, item, whole), :]
        return pltpu.make_async_remote_copy(
            src_ref=block, dst_ref=block, send_sem=pair_send.at[third], recv_sem=pair_recv.at[third, item],
            device_id=neighbour(3), device_id_type=MESH)

    for item in range(OWN_LAG):
        for third in range(3):
            copy(third, item, 0).start()

    @pl.loop(0, OWN // OWN_CHUNK)
    def _(n):
        rows = pl.ds(pl.multiple_of(n * OWN_CHUNK, OWN_CHUNK), OWN_CHUNK)
        full_ref[z, y, x, core, rows, :] = w_ref[rows, :]

    @pl.loop(0, OWN_ITEMS + 2 * OWN_LAG)
    def _(step):
        @pl.when(step + OWN_LAG < OWN_ITEMS)
        def _():
            for third in range(3):
                copy(third, step + OWN_LAG, 0).start()

        for hop in range(1, 4):
            delay = (hop - 1) * OWN_LAG

            @pl.when((step >= delay) & (step < OWN_ITEMS + delay))
            def _():
                item = step - delay
                for third in range(3):
                    arrival(third, item, hop - 1).wait_recv()
                    if hop < 3:
                        copy(third, item, hop).start()
                    else:
                        pair(third, item, core).start()

    @pl.loop(0, OWN_ITEMS)
    def _(item):
        for third in range(3):
            pair(third, item, 1 - core).wait_recv()
    for third in range(3):
        pair(third, 0, core, True).wait_send()
        for hop in range(3):
            copy(third, 0, hop, True).wait_send()


def gather(w_own):
    dma = pltpu.SemaphoreType.DMA
    return pl.pallas_call(
        gather_kernel,
        out_shape=jax.ShapeDtypeStruct((2, 2, 2, 2, OWN, LANES), jnp.bfloat16),
        in_specs=[pl.BlockSpec(memory_space=pltpu.VMEM)],
        out_specs=pl.BlockSpec(memory_space=pltpu.VMEM),
        scratch_shapes=[
            dma((3,)), dma((3, OWN_ITEMS)), dma((3, 3)), dma((3, OWN_ITEMS, 3)),
        ],
        compiler_params=pltpu.CompilerParams(has_side_effects=True, vmem_limit_bytes=GATHER_LIMIT),
    )(w_own)


def device_index():
    outer, middle, inner = (lax.axis_index(name) for name in MESH_AXES)
    return (outer * 2 + middle) * 4 + inner


def for_blocks(start, length, action, tensors=TENSORS):
    for base, end, tiles in tensors:
        block = 8 * tiles
        low = (jnp.maximum(start, base) - base + block - 1) // block
        high = jnp.maximum(jnp.minimum(start + length, end) - base, 0) // block

        count = jnp.maximum(high - low, 0)
        together = 4 if tiles <= 8 else 1

        @pl.loop(0, count // together)
        def _(n):
            for k in range(together):
                action(pl.multiple_of(base + (low + n * together + k) * block - start, 8), tiles)

        if together > 1:
            @pl.loop(count // together * together, count)
            def _(n):
                action(pl.multiple_of(base + (low + n) * block - start, 8), tiles)


PAD = 8
FLAT_ROWS = WINDOW + 272
SHARD_VREGS = SLICE // 1024
TAIL_ROWS = SLICE % 1024 // LANES
TAIL_LANES = SLICE % LANES
EDGE_ROWS = EDGE // LANES
OWN_FLAT_ROWS = OWN + 512


def lane_index(rows=8):
    return lax.broadcasted_iota(jnp.int32, (rows, LANES), 1)


BATCH = 256
BATCHES = SHARD_VREGS * 8 // BATCH
CHUNK_BATCHES = 3
CHUNKS = BATCHES // CHUNK_BATCHES
CHUNK = CHUNK_BATCHES * BATCH * LANES


def mid_kernel(tile_ref, m_ref, v_ref, w_ref, edge_ref, m_out, v_out, w_out, own_ref,
               m_buf, v_buf, w_buf, flat, shifted, edged, aligned, in_sem, out_sem):
    device = device_index()
    start = window_start(device)
    arrays = ((m_ref, m_buf, m_out), (v_ref, v_buf, v_out), (w_ref, w_buf, w_out))

    def span(chunk):
        return pl.ds(chunk * CHUNK, CHUNK if chunk < CHUNKS - 1 else SLICE - chunk * CHUNK)

    def loads(chunk):
        return [pltpu.make_async_copy(ref.at[span(chunk)], buf.at[span(chunk)], in_sem.at[n, chunk])
                for n, (ref, buf, _) in enumerate(arrays)]

    def stores(chunk):
        return [pltpu.make_async_copy(buf.at[span(chunk)], out.at[span(chunk)], out_sem.at[n, chunk])
                for n, (_, buf, out) in enumerate(arrays)]

    for chunk in range(CHUNKS):
        for copy in loads(chunk):
            copy.start()

    def to_flat(row, tiles):
        for t in range(tiles):
            flat[pl.ds(row + t, 8, stride=tiles), :] = tile_ref[pl.ds(row + 8 * t, 8), :]
    for_blocks(start, WINDOW, to_flat)

    first_row = device * (SLICE // 16) // 8
    next_row = (device + 1) * (SLICE // 16) // 8
    shift = device * SLICE - first_row * LANES
    next_shift = (device + 1) * SLICE - next_row * LANES

    def mean_rows(row, amount, rows):
        here = flat[pl.ds(row, rows), :]
        below = flat[pl.ds(row + 1, rows), :]
        back = (LANES - amount) % LANES
        return jnp.where(lane_index(rows) < LANES - amount, pltpu.roll(here, back, 1), pltpu.roll(below, back, 1))

    for chunk in range(CHUNKS):
        for copy in loads(chunk):
            copy.wait()

        @pl.loop(chunk * CHUNK_BATCHES, (chunk + 1) * CHUNK_BATCHES)
        def _(n):
            at = pl.ds(pl.multiple_of(n * BATCH * LANES, BATCH * LANES), BATCH * LANES)
            mean = mean_rows(first_row - start + n * BATCH, shift, BATCH)
            new = adam_update(mean, *(buf[at].reshape(BATCH, LANES) for _, buf, _ in arrays))
            for (_, buf, _), value in zip(arrays, new):
                buf[at] = value.reshape(BATCH * LANES)
            shifted[pl.ds(pl.multiple_of(PAD + n * BATCH, 8), BATCH), :] = pltpu.roll(new[2], shift, 1)

        if chunk > 0:
            for copy in stores(chunk - 1):
                copy.start()

    mean = mean_rows(first_row - start + SHARD_VREGS * 8, shift, 8)
    for r in range(TAIL_ROWS + 1):
        size = LANES if r < TAIL_ROWS else TAIL_LANES
        at = pl.ds(SHARD_VREGS * 1024 + r * LANES, size)
        new = adam_update(mean[r:r + 1, :size], *(buf[at].reshape(1, size) for _, buf, _ in arrays))
        for (_, buf, _), value in zip(arrays, new):
            buf[at] = value.reshape(size)
        flat[pl.ds(FLAT_ROWS - 8 + r, 1), pl.ds(0, size)] = new[2]
    shifted[pl.ds(PAD + SHARD_VREGS * 8, 8), :] = pltpu.roll(flat[pl.ds(FLAT_ROWS - 8, 8), :], shift, 1)

    @pl.loop(0, EDGE_ROWS // 64)
    def _(n):
        mean = mean_rows(next_row - start + n * 64, next_shift, 64)
        old = (edge_ref[pl.ds(pl.multiple_of(k * EDGE + n * 8192, 1024), 8192)].reshape(64, LANES) for k in range(3))
        edged[pl.ds(pl.multiple_of(PAD + n * 64, 8), 64), :] = pltpu.roll(adam_update(mean, *old)[2], next_shift, 1)

    for copy in stores(CHUNKS - 1):
        copy.start()

    own = own_start(device)
    skip = own - first_row

    @pl.loop(0, BATCHES + 1)
    def _(n):
        row = PAD + skip + n * BATCH
        aligned[pl.ds(pl.multiple_of(n * BATCH, 8), BATCH), :] = jnp.where(
            lane_index(BATCH) >= shift, shifted[pl.ds(row, BATCH), :], shifted[pl.ds(row - 1, BATCH), :])
    edged[pl.ds(PAD - 1, 1), :] = aligned[pl.ds(next_row - own, 1), :]

    @pl.loop(0, EDGE_ROWS // 64)
    def _(n):
        row = PAD + n * 64
        aligned[pl.ds(next_row - own + n * 64, 64), :] = jnp.where(
            lane_index(64) >= next_shift, edged[pl.ds(row, 64), :], edged[pl.ds(row - 1, 64), :])

    def to_tile(row, tiles):
        for t in range(0, tiles, 2):
            both = [aligned[pl.ds(row + t + k, 8, stride=tiles), :] for k in range(2)]
            own_ref[pl.ds(pl.multiple_of(row + 8 * t, 16), 16), :] = jnp.concatenate(both, axis=0).astype(jnp.bfloat16)

    def plain(row, _):
        own_ref[pl.ds(pl.multiple_of(row, 16), 16), :] = aligned[pl.ds(row, 16), :].astype(jnp.bfloat16)
    for_blocks(own, OWN, to_tile, TENSORS[:4])
    for_blocks(own, OWN, plain, ((*TENSORS[4][:2], 2),))

    for chunk in range(CHUNKS):
        for copy in stores(chunk):
            copy.wait()


def mid(mean_tiles, m, v, w, edges):
    vmem = pl.BlockSpec(memory_space=pltpu.VMEM)
    any_spec = pl.BlockSpec(memory_space=pl.ANY)
    shard = jax.ShapeDtypeStruct((SLICE,), jnp.float32)
    return pl.pallas_call(
        mid_kernel,
        out_shape=(shard, shard, shard, jax.ShapeDtypeStruct((OWN, LANES), jnp.bfloat16)),
        in_specs=[vmem, any_spec, any_spec, any_spec, vmem], out_specs=(any_spec, any_spec, any_spec, vmem),
        scratch_shapes=[
            pltpu.VMEM((SLICE,), jnp.float32), pltpu.VMEM((SLICE,), jnp.float32), pltpu.VMEM((SLICE,), jnp.float32),
            pltpu.VMEM((FLAT_ROWS, LANES), jnp.float32),
            pltpu.VMEM((PAD + SHARD_VREGS * 8 + 8 + 512, LANES), jnp.float32),
            pltpu.VMEM((PAD + EDGE_ROWS, LANES), jnp.float32),
            pltpu.VMEM((OWN_FLAT_ROWS, LANES), jnp.float32),
            pltpu.SemaphoreType.DMA((3, CHUNKS)), pltpu.SemaphoreType.DMA((3, CHUNKS)),
        ],
        compiler_params=pltpu.CompilerParams(vmem_limit_bytes=MID_LIMIT),
    )(mean_tiles, m, v, w, edges)


def pieces_of(tensor):
    base, end, _ = TENSORS[tensor]
    for d in range(SIXTEEN):
        low, high = max(OWN_STARTS[d], base), min(OWN_STARTS[d + 1], end)
        if low < high:
            yield d, low - OWN_STARTS[d], low - base, high - low


PIECES = [(tensor,) + piece for tensor in range(4) for piece in pieces_of(tensor)]
VEC_WIDTH = 12032
VEC_ROWS = VEC_WIDTH // LANES
VEC_BLOCK = VEC_WIDTH // 8
CHIP_COUNTS = tuple((end - base) // 8 for base, end, _ in TENSORS[:4])
CHIP_ROWS = sum(CHIP_COUNTS)
CHIP_SIZE = CHIP_ROWS * LANES + VEC_BLOCK
CHIP_PARTS = 6
CHIP_PART = CHIP_SIZE // 16384 // CHIP_PARTS * 16384


def final_kernel(full_ref, e_out, a_out, f_out, h_out, vec_out, chip_ref, chip_out, flat, vec, out_sem, chip_sem):
    outs = (e_out, a_out, f_out, h_out)
    chip = device_index() // 2
    copies = []
    for n, (tensor, d, source, target, rows) in enumerate(PIECES):
        copies.append(pltpu.make_async_copy(
            full_ref.at[d, pl.ds(source, rows), :], outs[tensor].at[pl.ds(target, rows), :], out_sem.at[n]))
        copies[-1].start()

    slot, source, _, _ = next(pieces_of(4))
    vec[pl.ds(0, 96), :] = full_ref[slot, pl.ds(source, 96), :].astype(jnp.float32)
    for n in range(VEC_ROWS // 8):
        vec_out[:, n * 1024:(n + 1) * 1024] = vec[n * 8:n * 8 + 8, :].reshape(1, 1024).astype(jnp.bfloat16)
    rest = VEC_ROWS % 8
    vec_out[:, VEC_ROWS // 8 * 1024:] = vec[pl.ds(VEC_ROWS - rest, rest), :].reshape(1, rest * LANES).astype(jnp.bfloat16)

    offset = 0
    for tensor, rows in enumerate(CHIP_COUNTS):
        base, _, tiles = TENSORS[tensor]
        step = 16 * tiles

        begin = base + chip * rows
        slot, low, bound = jnp.int32(0), jnp.int32(0), jnp.int32(OWN_STARTS[1])
        for d in range(1, SIXTEEN):
            inside = begin >= OWN_STARTS[d]
            slot = jnp.where(inside, d, slot)
            low = jnp.where(inside, OWN_STARTS[d], low)
            bound = jnp.where(inside, OWN_STARTS[d + 1], bound)

        @pl.loop(0, rows // step)
        def _(n):
            for half in range(2):
                row = begin + n * step + half * 8 * tiles
                following = row >= bound
                at_slot = jnp.where(following, slot + 1, slot)
                at_row = row - jnp.where(following, bound, low)
                for t in range(0, tiles, 2):
                    value = full_ref[at_slot, pl.ds(pl.multiple_of(at_row + 8 * t, 16), 16), :].astype(jnp.float32)
                    for k in range(2):
                        to = offset + n * step + half * 8 * tiles + t + k
                        flat[pl.ds(to, 8, stride=tiles), :] = value[8 * k:8 * k + 8]
        offset += rows

    vec_row = chip * (VEC_BLOCK // 32) // 4
    amount = chip * VEC_BLOCK - vec_row * LANES
    back = (LANES - amount) % LANES
    lane = lane_index()
    for n in range(2):
        here, below = vec[pl.ds(vec_row + n * 8, 8), :], vec[pl.ds(vec_row + n * 8 + 1, 8), :]
        flat[pl.ds(CHIP_ROWS + n * 8, 8), :] = jnp.where(
            lane < LANES - amount, pltpu.roll(here, back, 1), pltpu.roll(below, back, 1))

    def part_copy(part):
        span = pl.ds(part * CHIP_PART, CHIP_PART if part < CHIP_PARTS - 1 else CHIP_SIZE - part * CHIP_PART)
        return pltpu.make_async_copy(chip_out.at[:, span], chip_ref.at[:, span], chip_sem.at[part])

    for part in range(CHIP_PARTS):
        @pl.loop(part * CHIP_PART // 16384, (part + 1) * CHIP_PART // 16384)
        def _(n):
            chip_out[:, pl.ds(pl.multiple_of(n * 16384, 16384), 16384)] = flat[
                pl.ds(pl.multiple_of(n * 128, 128), 128), :].reshape(1, 16384).astype(jnp.bfloat16)
        if part > 0:
            part_copy(part - 1).start()
    done = CHIP_SIZE // 1024 * 1024
    rows = (CHIP_SIZE - done) // LANES
    last = CHIP_SIZE - done - rows * LANES
    first = done // LANES
    chip_out[:, CHIP_PARTS * CHIP_PART:done] = flat[CHIP_PARTS * CHIP_PART // LANES:first, :].reshape(
        1, done - CHIP_PARTS * CHIP_PART).astype(jnp.bfloat16)
    chip_out[:, done:done + rows * LANES] = flat[first:first + rows, :].reshape(1, rows * LANES).astype(jnp.bfloat16)
    chip_out[:, CHIP_SIZE - last:] = flat[first + rows:first + rows + 1, :last].astype(jnp.bfloat16)
    part_copy(CHIP_PARTS - 1).start()
    for part in range(CHIP_PARTS):
        part_copy(part).wait()
    for copy in copies:
        copy.wait()


def finish(full):
    vmem = pl.BlockSpec(memory_space=pltpu.VMEM)
    any_spec = pl.BlockSpec(memory_space=pl.ANY)
    shape = lambda rows: jax.ShapeDtypeStruct((rows, LANES), jnp.bfloat16)
    return pl.pallas_call(
        final_kernel,
        out_shape=tuple(shape(end - base) for base, end, _ in TENSORS[:4]) + (
            jax.ShapeDtypeStruct((1, VEC_WIDTH), jnp.bfloat16), jax.ShapeDtypeStruct((1, CHIP_SIZE), jnp.bfloat16)),
        in_specs=[vmem], out_specs=(any_spec,) * 4 + (vmem, any_spec),
        scratch_shapes=[
            pltpu.VMEM((1, CHIP_SIZE), jnp.bfloat16),
            pltpu.VMEM((CHIP_ROWS + 16, LANES), jnp.float32),
            pltpu.VMEM((120, LANES), jnp.float32),
            pltpu.SemaphoreType.DMA((len(PIECES),)), pltpu.SemaphoreType.DMA((CHIP_PARTS,)),
        ],
        compiler_params=pltpu.CompilerParams(vmem_limit_bytes=FINAL_LIMIT),
    )(full)


def solution(mesh):
    def local_step(g_embed, g_attn, g_ffn_in, g_ffn_out, g_vec, m_shard, v_shard, w_shard):
        matrices = (g_embed, g_attn, g_ffn_in, g_ffn_out)
        grads = [to_tiles(g[0] if g.ndim == 3 else g[0, 0]) for g in matrices]
        grads.append(jnp.pad(g_vec, ((0, 0), (0, 0), (0, VEC_BLOCK_ROWS * LANES - VEC_WIDTH))).reshape(VEC_BLOCK_ROWS, LANES))
        mean_tiles, edges = scatter(grads, m_shard, v_shard, w_shard)
        m_new, v_new, w_new, w_own = mid(mean_tiles, m_shard, v_shard, w_shard, edges)
        full = gather(w_own).reshape(SIXTEEN, OWN, LANES)
        *tiles, vec, w_chip = finish(full)
        tensors = [from_tiles(t, g.shape[-1]).reshape(g.shape[1:]) for t, g in zip(tiles, matrices)]
        return (m_new, v_new, w_new) + tuple(tensors) + (vec, w_chip)

    return jax.shard_map(local_step, mesh=mesh, in_specs=(P(MESH_AXES),) * 8, out_specs=(P(MESH_AXES),) * 3 + (P(),) * 5 + (P(MESH_AXES),), check_vma=False)
```

```python
import functools
import math
import jax
import jax.numpy as jnp
from jax import lax
from jax.experimental import pallas as pl
from jax.experimental.pallas import tpu as pltpu
from jax.sharding import PartitionSpec as P

MESH_AXES = ('outer', 'middle', 'inner')
MESH = pl.DeviceIdType.MESH
ADAM_BETA1 = 0.9
ADAM_BETA2 = 0.98
ADAM_EPS = 1e-9
LEARN_RATE = 0.05
ADAM_STEP = 3

LANES = 128
SLICE = 885488
TENSORS = ((0, 32768, 8), (32768, 65536, 32), (65536, 88064, 22), (88064, 110592, 8), (110592, 110720, 1))
ROWS = 110720
VEC_BLOCK_ROWS = 128
UNIT = 64
GROUP = 128
COMMON = 7168
WINDOW = COMMON + GROUP
LONG_SLICE = 10
COUNTS = (38, 38, 36)
FIRSTS = (0, 38, 76)
ITEMS = max(COUNTS)
LAG = 2
EDGE = 32768
OWN = 7104
OWN_THIRD = OWN // 3
OWN_CHUNK = 64
OWN_ITEMS = OWN_THIRD // OWN_CHUNK
OWN_LAG = 2
SIXTEEN = 16
FINAL_LIMIT = 20000000
GATHER_LIMIT = 6000000
MID_LIMIT = 52000000


def floor_block(row):
    result = row
    for base, end, tiles in TENSORS:
        block = 8 * tiles if tiles > 1 else VEC_BLOCK_ROWS
        floored = base + (row - base) // block * block
        result = jnp.where((row >= base) & (row < end), floored, result)
    return result


def window_start(index):
    row = floor_block(index * (SLICE // 16) // 8)
    return jnp.minimum(row // GROUP * GROUP, ROWS - COMMON)


def own_start_static(index):
    row = -(-index * SLICE // LANES)
    for base, end, tiles in TENSORS:
        if base <= row < end:
            block = 8 * tiles if tiles > 1 else VEC_BLOCK_ROWS
            return base + -(-(row - base) // block) * block
    return ROWS


OWN_STARTS = [own_start_static(d) for d in range(SIXTEEN)] + [ROWS]


def own_start(index):
    result = jnp.int32(0)
    for d in range(SIXTEEN):
        result = jnp.where(index == d, OWN_STARTS[d], result)
    return result


def adam_update(grad_mean, m_old, v_old, w_old):
    m_new = ADAM_BETA1 * m_old + (1.0 - ADAM_BETA1) * grad_mean
    v_new = ADAM_BETA2 * v_old + (1.0 - ADAM_BETA2) * (grad_mean * grad_mean)
    scale = LEARN_RATE / (1.0 - ADAM_BETA1 ** ADAM_STEP)
    w_new = w_old - scale * m_new / (jnp.sqrt(v_new * (1.0 / (1.0 - ADAM_BETA2 ** ADAM_STEP))) + ADAM_EPS)
    return m_new, v_new, w_new


def to_tiles(tensor):
    rows, width = tensor.shape
    return tensor.reshape(rows // 8, 8, width // LANES, LANES).transpose(0, 2, 1, 3).reshape(-1, LANES)


def from_tiles(tiles, width):
    return tiles.reshape(-1, width // LANES, 8, LANES).transpose(0, 2, 1, 3).reshape(-1, width)


ORDERS = ((0, 1, 2), (1, 2, 0), (2, 0, 1))


def position():
    outer, middle, inner = (lax.axis_index(name) for name in MESH_AXES)
    return outer, middle, inner // 2, inner % 2


def neighbour(axis):
    outer, middle, x, core = position()
    z, y = outer, middle
    if axis == 0:
        z = 1 - z
    elif axis == 1:
        y = 1 - y
    elif axis == 2:
        x = 1 - x
    else:
        core = 1 - core
    return (z, y, 2 * x + core)


def meet(devices):
    barrier = pltpu.get_barrier_semaphore()
    for device in devices:
        pl.semaphore_signal(barrier, inc=1, device_id=device, device_id_type=MESH)
    pl.semaphore_wait(barrier, len(devices))


def scatter_kernel(e_ref, a_ref, f_ref, h_ref, b_ref, m_ref, v_ref, w_ref, out_ref, edge_ref,
                   part, recv0, recv1, recv2, mine, pair_send, pair_recv, mine_sem,
                   send, arrive, out_sem, edge_send, edge_recv, long_mine, long_part, long_recv, long_sem):
    z, y, x, core = position()
    chip = (z * 2 + y) * 2 + x
    device = chip * 2 + core
    sources = (e_ref, a_ref, f_ref, h_ref, b_ref)

    before = (device + SIXTEEN - 1) % SIXTEEN
    after = (device + 1) % SIXTEEN
    meet([neighbour(axis) for axis in range(4)] + [(d // 8, d // 4 % 2, d % 4) for d in (before, after)])
    for n, ref in enumerate((m_ref, v_ref, w_ref)):
        pltpu.make_async_remote_copy(
            src_ref=ref.at[pl.ds(0, EDGE)], dst_ref=edge_ref.at[pl.ds(n * EDGE, EDGE)],
            send_sem=edge_send.at[n], recv_sem=edge_recv.at[n],
            device_id=(before // 8, before // 4 % 2, before % 4), device_id_type=MESH).start()

    def from_source(row, action):
        def choose(low, high):
            if high - low == 1:
                action(sources[low].at[pl.ds(pl.multiple_of(row - TENSORS[low][0], GROUP), GROUP), :])
                return
            middle = (low + high) // 2
            lax.cond(row < TENSORS[middle][0], lambda: choose(low, middle), lambda: choose(middle, high))
        choose(0, len(sources))

    def item_row(third, item):
        return pl.multiple_of((FIRSTS[third] + item) * UNIT, UNIT)

    def each_third(index, counts, action):
        for third in range(3):
            if counts[third] == max(counts):
                action(third)
            else:
                @pl.when(index < counts[third])
                def _():
                    action(third)

    def group_row(third, group):
        return pl.multiple_of(FIRSTS[third] * UNIT + group * GROUP, GROUP)

    def start_group(group, slot):
        @pl.loop(0, 8)
        def _(j):
            jz, jy, jx = j // 4, j // 2 % 2, j % 2
            other = ((z + jz) % 2 * 2 + (y + jy) % 2) * 2 + (x + jx) % 2
            theirs = window_start(other * 2 + 1 - core)
            ours = window_start(other * 2 + core)

            def action(third):
                row = group_row(third, group)
                from_source(theirs + row, lambda src: pltpu.make_async_remote_copy(
                    src_ref=src, dst_ref=part.at[jz, jy, jx, pl.ds(row, GROUP), :],
                    send_sem=pair_send.at[third], recv_sem=pair_recv.at[third, group],
                    device_id=neighbour(3), device_id_type=MESH).start())
                from_source(ours + row, lambda src: pltpu.make_async_copy(
                    src, mine.at[slot, third, jz, jy, jx], mine_sem.at[slot, third]).start())
            each_third(group, [count // 2 for count in COUNTS], action)

    def hop_copy(third, item, hop, whole=False):
        rows = pl.ds(item_row(third, 0), COUNTS[third] * UNIT) if whole else pl.ds(item_row(third, item), UNIT)
        first, second, last = ORDERS[third]
        if hop == 0:
            index = tuple(1 if n == first else slice(None) for n in range(3))
            target = recv0.at[:, :, rows, :]
        elif hop == 1:
            index = tuple(0 if n == first else 1 if n == second else slice(None) for n in range(3))
            target = recv1.at[:, rows, :]
        else:
            index = tuple(1 if n == last else 0 for n in range(3))
            target = recv2.at[rows, :]
        return pltpu.make_async_remote_copy(
            src_ref=part.at[index + (rows, slice(None))], dst_ref=target,
            send_sem=send.at[third, hop], recv_sem=arrive.at[third, hop, item],
            device_id=neighbour(ORDERS[third][hop]), device_id_type=MESH)

    def pair_all(third, group, whole=False):
        rows = pl.ds(FIRSTS[third] * UNIT, COUNTS[third] * UNIT) if whole else pl.ds(group_row(third, group), GROUP)
        block = part.at[:, :, :, rows, :]
        return pltpu.make_async_remote_copy(
            src_ref=block, dst_ref=block, send_sem=pair_send.at[third], recv_sem=pair_recv.at[third, group],
            device_id=neighbour(3), device_id_type=MESH)

    def out_copy(third, item, whole=False):
        rows = pl.ds(item_row(third, 0), COUNTS[third] * UNIT) if whole else pl.ds(item_row(third, item), UNIT)
        return pltpu.make_async_copy(part.at[0, 0, 0, rows, :], out_ref.at[rows, :], out_sem.at[third])

    start_group(0, 0)

    def stage0(item, third):
        rows = pl.ds(item_row(third, item), UNIT)
        group = item // 2
        slot = group % 2

        @pl.when(item % 2 == 0)
        def _():
            pltpu.make_async_copy(mine.at[slot, third], mine.at[slot, third], mine_sem.at[slot, third]).wait()
            pair_all(third, group).wait_recv()
        within = pl.ds(pl.multiple_of(item % 2 * UNIT, UNIT), UNIT)
        for j in range(8):
            index = (j // 4, j // 2 % 2, j % 2)
            part[index + (rows, slice(None))] += mine[(slot, third) + index + (within, slice(None))]
        hop_copy(third, item, 0).start()

    def stage1(item, third):
        rows = pl.ds(item_row(third, item), UNIT)
        hop_copy(third, item, 0).wait_recv()
        first = ORDERS[third][0]
        for j in range(4):
            pair = [j // 2, j % 2]
            index = tuple(pair[:first] + [0] + pair[first:])
            part[index + (rows, slice(None))] += recv0[j // 2, j % 2, rows, :]
        hop_copy(third, item, 1).start()

    def stage2(item, third):
        rows = pl.ds(item_row(third, item), UNIT)
        hop_copy(third, item, 1).wait_recv()
        last = ORDERS[third][2]
        for j in range(2):
            index = tuple(j if n == last else 0 for n in range(3))
            part[index + (rows, slice(None))] += recv1[j, rows, :]
        hop_copy(third, item, 2).start()

    def stage3(item, third):
        rows = pl.ds(item_row(third, item), UNIT)
        hop_copy(third, item, 2).wait_recv()
        part[0, 0, 0, rows, :] = (part[0, 0, 0, rows, :] + recv2[rows, :]) / SIXTEEN

    long_chip, long_core = LONG_SLICE // 2, LONG_SLICE % 2
    lz, ly, lx = (z + long_chip // 4) % 2, (y + long_chip // 2 % 2) % 2, (x + long_chip % 2) % 2
    long_row = window_start(LONG_SLICE) + COMMON
    holder = core == long_core

    def long_pair():
        return pltpu.make_async_remote_copy(
            src_ref=long_mine, dst_ref=long_part, send_sem=long_sem.at[0], recv_sem=long_sem.at[1],
            device_id=neighbour(3), device_id_type=MESH)

    def long_load():
        return pltpu.make_async_copy(
            sources[2].at[pl.ds(pl.multiple_of(long_row - TENSORS[2][0], GROUP), GROUP), :], long_mine, long_sem.at[2])

    def long_hop(hop):
        return pltpu.make_async_remote_copy(
            src_ref=long_part, dst_ref=long_recv.at[hop], send_sem=long_sem.at[3 + hop], recv_sem=long_sem.at[6 + hop],
            device_id=neighbour((2, 0, 1)[hop]), device_id_type=MESH)

    def long_out():
        return pltpu.make_async_copy(long_part, out_ref.at[pl.ds(COMMON, GROUP), :], long_sem.at[9])

    reached = (holder, holder & (lx == 0), holder & (lx == 0) & (lz == 0), holder & (lx == 0) & (lz == 0) & (ly == 0))
    far = (lx == 1, lz == 1, ly == 1)

    def long_start():
        long_load().start()

    def long_exchange():
        long_load().wait()

        @pl.when(core != long_core)
        def _():
            long_pair().start()

    def long_sum():
        @pl.when(holder)
        def _():
            long_pair().wait_recv()
            long_part[...] += long_mine[...]

        @pl.when(core != long_core)
        def _():
            long_pair().wait_send()

    def long_send(hop):
        @pl.when(reached[hop] & far[hop])
        def _():
            long_hop(hop).start()

    def long_add(hop):
        @pl.when(reached[hop] & far[hop])
        def _():
            long_hop(hop).wait_send()

        @pl.when(reached[hop + 1])
        def _():
            long_hop(hop).wait_recv()
            if hop < 2:
                long_part[...] += long_recv[hop]
            else:
                long_part[...] = (long_part[...] + long_recv[hop]) / SIXTEEN

    def long_store():
        @pl.when(reached[3])
        def _():
            long_out().start()

    long_stages = ((4, long_start), (6, long_exchange), (8, long_sum)) + tuple(
        (9 + 3 * hop + k, functools.partial((long_send, long_add)[k // 2], hop)) for hop in range(3) for k in (0, 2)
    ) + ((19, long_store),)

    stages = ((0, stage0), (LAG, stage1), (2 * LAG, stage2), (3 * LAG, stage3),
              (3 * LAG + 1, lambda item, third: out_copy(third, item).start()))

    @pl.loop(0, ITEMS + stages[-1][0])
    def _(step):
        for delay, stage in stages:
            @pl.when((step >= delay) & (step < ITEMS + delay))
            def _():
                each_third(step - delay, COUNTS, functools.partial(stage, step - delay))

        for at, stage in long_stages:
            @pl.when(step == at)
            def _():
                stage()

        @pl.when((step % 2 == 0) & (step + 2 < ITEMS))
        def _():
            start_group(step // 2 + 1, (step // 2 + 1) % 2)

    for third in range(3):
        pair_all(third, 0, True).wait_send()
        for hop in range(3):
            hop_copy(third, 0, hop, True).wait_send()
        out_copy(third, 0, True).wait()

    @pl.when(reached[3])
    def _():
        long_out().wait()

    for n, ref in enumerate((m_ref, v_ref, w_ref)):
        pltpu.make_async_remote_copy(
            src_ref=ref.at[pl.ds(0, EDGE)], dst_ref=edge_ref.at[pl.ds(n * EDGE, EDGE)],
            send_sem=edge_send.at[n], recv_sem=edge_recv.at[n],
            device_id=(before // 8, before // 4 % 2, before % 4), device_id_type=MESH).wait()


def scatter(grads, m, v, w):
    any_spec = pl.BlockSpec(memory_space=pl.ANY)
    dma = pltpu.SemaphoreType.DMA
    return pl.pallas_call(
        scatter_kernel,
        out_shape=(jax.ShapeDtypeStruct((WINDOW, LANES), jnp.float32), jax.ShapeDtypeStruct((3 * EDGE,), jnp.float32)),
        in_specs=[any_spec] * 8,
        out_specs=(any_spec, any_spec),
        scratch_shapes=[
            pltpu.VMEM((2, 2, 2, COMMON, LANES), jnp.float32),
            pltpu.VMEM((2, 2, COMMON, LANES), jnp.float32),
            pltpu.VMEM((2, COMMON, LANES), jnp.float32),
            pltpu.VMEM((COMMON, LANES), jnp.float32),
            pltpu.VMEM((2, 3, 2, 2, 2, GROUP, LANES), jnp.float32),
            dma((3,)), dma((3, ITEMS // 2)), dma((2, 3)),
            dma((3, 3)), dma((3, 3, ITEMS)), dma((3,)), dma((3,)), dma((3,)),
            pltpu.VMEM((GROUP, LANES), jnp.float32), pltpu.VMEM((GROUP, LANES), jnp.float32),
            pltpu.VMEM((3, GROUP, LANES), jnp.float32), dma((10,)),
        ],
        compiler_params=pltpu.CompilerParams(has_side_effects=True, collective_id=0, vmem_limit_bytes=67043328),
    )(*grads, m, v, w)


def gather_kernel(w_ref, full_ref, pair_send, pair_recv, send, arrive):
    z, y, x, core = position()
    here = (z, y, x)

    def rows_of(third, item, whole=False):
        if whole:
            return pl.ds(third * OWN_THIRD, OWN_THIRD)
        return pl.ds(pl.multiple_of(third * OWN_THIRD + item * OWN_CHUNK, OWN_CHUNK), OWN_CHUNK)

    def copy(third, item, hop, whole=False):
        rows = rows_of(third, item, whole)
        order = ORDERS[third]
        if hop == 0:
            source = w_ref.at[rows, :]
            target = full_ref.at[z, y, x, core, rows, :]
        else:
            index = tuple(slice(None) if n in order[:hop] else here[n] for n in range(3))
            source = target = full_ref.at[index + (core, rows, slice(None))]
        return pltpu.make_async_remote_copy(
            src_ref=source, dst_ref=target, send_sem=send.at[third, hop], recv_sem=arrive.at[third, item, hop],
            device_id=neighbour(order[hop]), device_id_type=MESH)

    def arrival(third, item, hop):
        order = ORDERS[third]
        index = tuple(slice(None) if n in order[:hop] else (1 - here[n] if n == order[hop] else here[n]) for n in range(3))
        block = full_ref.at[index + (core, rows_of(third, item), slice(None))]
        return pltpu.make_async_remote_copy(
            src_ref=block, dst_ref=block, send_sem=send.at[third, hop], recv_sem=arrive.at[third, item, hop],
            device_id=neighbour(order[hop]), device_id_type=MESH)

    def pair(third, item, side, whole=False):
        block = full_ref.at[:, :, :, side, rows_of(third, item, whole), :]
        return pltpu.make_async_remote_copy(
            src_ref=block, dst_ref=block, send_sem=pair_send.at[third], recv_sem=pair_recv.at[third, item],
            device_id=neighbour(3), device_id_type=MESH)

    meet([neighbour(axis) for axis in range(4)])
    for item in range(OWN_LAG):
        for third in range(3):
            copy(third, item, 0).start()

    @pl.loop(0, OWN // OWN_CHUNK)
    def _(n):
        rows = pl.ds(pl.multiple_of(n * OWN_CHUNK, OWN_CHUNK), OWN_CHUNK)
        full_ref[z, y, x, core, rows, :] = w_ref[rows, :]

    @pl.loop(0, OWN_ITEMS + 2 * OWN_LAG)
    def _(step):
        @pl.when(step + OWN_LAG < OWN_ITEMS)
        def _():
            for third in range(3):
                copy(third, step + OWN_LAG, 0).start()

        for hop in range(1, 4):
            delay = (hop - 1) * OWN_LAG

            @pl.when((step >= delay) & (step < OWN_ITEMS + delay))
            def _():
                item = step - delay
                for third in range(3):
                    arrival(third, item, hop - 1).wait_recv()
                    if hop < 3:
                        copy(third, item, hop).start()
                    else:
                        pair(third, item, core).start()

    @pl.loop(0, OWN_ITEMS)
    def _(item):
        for third in range(3):
            pair(third, item, 1 - core).wait_recv()
    for third in range(3):
        pair(third, 0, core, True).wait_send()
        for hop in range(3):
            copy(third, 0, hop, True).wait_send()


def gather(w_own):
    dma = pltpu.SemaphoreType.DMA
    return pl.pallas_call(
        gather_kernel,
        out_shape=jax.ShapeDtypeStruct((2, 2, 2, 2, OWN, LANES), jnp.bfloat16),
        in_specs=[pl.BlockSpec(memory_space=pltpu.VMEM)],
        out_specs=pl.BlockSpec(memory_space=pltpu.VMEM),
        scratch_shapes=[
            dma((3,)), dma((3, OWN_ITEMS)), dma((3, 3)), dma((3, OWN_ITEMS, 3)),
        ],
        compiler_params=pltpu.CompilerParams(has_side_effects=True, collective_id=1, vmem_limit_bytes=GATHER_LIMIT),
    )(w_own)


def device_index():
    outer, middle, inner = (lax.axis_index(name) for name in MESH_AXES)
    return (outer * 2 + middle) * 4 + inner


def for_blocks(start, length, action, tensors=TENSORS):
    for base, end, tiles in tensors:
        block = 8 * tiles
        low = (jnp.maximum(start, base) - base + block - 1) // block
        high = jnp.maximum(jnp.minimum(start + length, end) - base, 0) // block

        count = jnp.maximum(high - low, 0)
        together = 4 if tiles <= 8 else 1

        @pl.loop(0, count // together)
        def _(n):
            for k in range(together):
                action(pl.multiple_of(base + (low + n * together + k) * block - start, 8), tiles)

        if together > 1:
            @pl.loop(count // together * together, count)
            def _(n):
                action(pl.multiple_of(base + (low + n) * block - start, 8), tiles)


PAD = 8
FLAT_ROWS = WINDOW + 272
SHARD_VREGS = SLICE // 1024
TAIL_ROWS = SLICE % 1024 // LANES
TAIL_LANES = SLICE % LANES
EDGE_ROWS = EDGE // LANES
OWN_FLAT_ROWS = OWN + 512


def lane_index(rows=8):
    return lax.broadcasted_iota(jnp.int32, (rows, LANES), 1)


BATCH = 256
BATCHES = SHARD_VREGS * 8 // BATCH
CHUNK_BATCHES = 3
CHUNKS = BATCHES // CHUNK_BATCHES
CHUNK = CHUNK_BATCHES * BATCH * LANES


def mid_kernel(tile_ref, m_ref, v_ref, w_ref, edge_ref, m_out, v_out, w_out, own_ref,
               m_buf, v_buf, w_buf, flat, shifted, edged, aligned, in_sem, out_sem):
    device = device_index()
    start = window_start(device)
    arrays = ((m_ref, m_buf, m_out), (v_ref, v_buf, v_out), (w_ref, w_buf, w_out))

    def span(chunk):
        return pl.ds(chunk * CHUNK, CHUNK if chunk < CHUNKS - 1 else SLICE - chunk * CHUNK)

    def loads(chunk):
        return [pltpu.make_async_copy(ref.at[span(chunk)], buf.at[span(chunk)], in_sem.at[n, chunk])
                for n, (ref, buf, _) in enumerate(arrays)]

    def stores(chunk):
        return [pltpu.make_async_copy(buf.at[span(chunk)], out.at[span(chunk)], out_sem.at[n, chunk])
                for n, (_, buf, out) in enumerate(arrays)]

    for chunk in range(CHUNKS):
        for copy in loads(chunk):
            copy.start()

    def to_flat(row, tiles):
        for t in range(tiles):
            flat[pl.ds(row + t, 8, stride=tiles), :] = tile_ref[pl.ds(row + 8 * t, 8), :]
    for_blocks(start, WINDOW, to_flat)

    first_row = device * (SLICE // 16) // 8
    next_row = (device + 1) * (SLICE // 16) // 8
    shift = device * SLICE - first_row * LANES
    next_shift = (device + 1) * SLICE - next_row * LANES

    def mean_rows(row, amount, rows):
        here = flat[pl.ds(row, rows), :]
        below = flat[pl.ds(row + 1, rows), :]
        back = (LANES - amount) % LANES
        return jnp.where(lane_index(rows) < LANES - amount, pltpu.roll(here, back, 1), pltpu.roll(below, back, 1))

    for chunk in range(CHUNKS):
        for copy in loads(chunk):
            copy.wait()

        @pl.loop(chunk * CHUNK_BATCHES, (chunk + 1) * CHUNK_BATCHES)
        def _(n):
            at = pl.ds(pl.multiple_of(n * BATCH * LANES, BATCH * LANES), BATCH * LANES)
            mean = mean_rows(first_row - start + n * BATCH, shift, BATCH)
            new = adam_update(mean, *(buf[at].reshape(BATCH, LANES) for _, buf, _ in arrays))
            for (_, buf, _), value in zip(arrays, new):
                buf[at] = value.reshape(BATCH * LANES)
            shifted[pl.ds(pl.multiple_of(PAD + n * BATCH, 8), BATCH), :] = pltpu.roll(new[2], shift, 1)

        if chunk > 0:
            for copy in stores(chunk - 1):
                copy.start()

    mean = mean_rows(first_row - start + SHARD_VREGS * 8, shift, 8)
    for r in range(TAIL_ROWS + 1):
        size = LANES if r < TAIL_ROWS else TAIL_LANES
        at = pl.ds(SHARD_VREGS * 1024 + r * LANES, size)
        new = adam_update(mean[r:r + 1, :size], *(buf[at].reshape(1, size) for _, buf, _ in arrays))
        for (_, buf, _), value in zip(arrays, new):
            buf[at] = value.reshape(size)
        flat[pl.ds(FLAT_ROWS - 8 + r, 1), pl.ds(0, size)] = new[2]
    shifted[pl.ds(PAD + SHARD_VREGS * 8, 8), :] = pltpu.roll(flat[pl.ds(FLAT_ROWS - 8, 8), :], shift, 1)

    @pl.loop(0, EDGE_ROWS // 64)
    def _(n):
        mean = mean_rows(next_row - start + n * 64, next_shift, 64)
        old = (edge_ref[pl.ds(pl.multiple_of(k * EDGE + n * 8192, 1024), 8192)].reshape(64, LANES) for k in range(3))
        edged[pl.ds(pl.multiple_of(PAD + n * 64, 8), 64), :] = pltpu.roll(adam_update(mean, *old)[2], next_shift, 1)

    for copy in stores(CHUNKS - 1):
        copy.start()

    own = own_start(device)
    skip = own - first_row

    @pl.loop(0, BATCHES + 1)
    def _(n):
        row = PAD + skip + n * BATCH
        aligned[pl.ds(pl.multiple_of(n * BATCH, 8), BATCH), :] = jnp.where(
            lane_index(BATCH) >= shift, shifted[pl.ds(row, BATCH), :], shifted[pl.ds(row - 1, BATCH), :])
    edged[pl.ds(PAD - 1, 1), :] = aligned[pl.ds(next_row - own, 1), :]

    @pl.loop(0, EDGE_ROWS // 64)
    def _(n):
        row = PAD + n * 64
        aligned[pl.ds(next_row - own + n * 64, 64), :] = jnp.where(
            lane_index(64) >= next_shift, edged[pl.ds(row, 64), :], edged[pl.ds(row - 1, 64), :])

    def to_tile(row, tiles):
        for t in range(0, tiles, 2):
            both = [aligned[pl.ds(row + t + k, 8, stride=tiles), :] for k in range(2)]
            own_ref[pl.ds(pl.multiple_of(row + 8 * t, 16), 16), :] = jnp.concatenate(both, axis=0).astype(jnp.bfloat16)

    def plain(row, _):
        own_ref[pl.ds(pl.multiple_of(row, 16), 16), :] = aligned[pl.ds(row, 16), :].astype(jnp.bfloat16)
    for_blocks(own, OWN, to_tile, TENSORS[:4])
    for_blocks(own, OWN, plain, ((*TENSORS[4][:2], 2),))

    for chunk in range(CHUNKS):
        for copy in stores(chunk):
            copy.wait()


def mid(mean_tiles, m, v, w, edges):
    vmem = pl.BlockSpec(memory_space=pltpu.VMEM)
    any_spec = pl.BlockSpec(memory_space=pl.ANY)
    shard = jax.ShapeDtypeStruct((SLICE,), jnp.float32)
    return pl.pallas_call(
        mid_kernel,
        out_shape=(shard, shard, shard, jax.ShapeDtypeStruct((OWN, LANES), jnp.bfloat16)),
        in_specs=[vmem, any_spec, any_spec, any_spec, vmem], out_specs=(any_spec, any_spec, any_spec, vmem),
        scratch_shapes=[
            pltpu.VMEM((SLICE,), jnp.float32), pltpu.VMEM((SLICE,), jnp.float32), pltpu.VMEM((SLICE,), jnp.float32),
            pltpu.VMEM((FLAT_ROWS, LANES), jnp.float32),
            pltpu.VMEM((PAD + SHARD_VREGS * 8 + 8 + 512, LANES), jnp.float32),
            pltpu.VMEM((PAD + EDGE_ROWS, LANES), jnp.float32),
            pltpu.VMEM((OWN_FLAT_ROWS, LANES), jnp.float32),
            pltpu.SemaphoreType.DMA((3, CHUNKS)), pltpu.SemaphoreType.DMA((3, CHUNKS)),
        ],
        compiler_params=pltpu.CompilerParams(vmem_limit_bytes=MID_LIMIT),
    )(mean_tiles, m, v, w, edges)


def pieces_of(tensor):
    base, end, _ = TENSORS[tensor]
    for d in range(SIXTEEN):
        low, high = max(OWN_STARTS[d], base), min(OWN_STARTS[d + 1], end)
        if low < high:
            yield d, low - OWN_STARTS[d], low - base, high - low


PIECES = [(tensor,) + piece for tensor in range(4) for piece in pieces_of(tensor)]
VEC_WIDTH = 12032
VEC_ROWS = VEC_WIDTH // LANES
VEC_BLOCK = VEC_WIDTH // 8
CHIP_COUNTS = tuple((end - base) // 8 for base, end, _ in TENSORS[:4])
CHIP_ROWS = sum(CHIP_COUNTS)
CHIP_SIZE = CHIP_ROWS * LANES + VEC_BLOCK
CHIP_PARTS = 6
CHIP_PART = CHIP_SIZE // 16384 // CHIP_PARTS * 16384


def final_kernel(full_ref, e_out, a_out, f_out, h_out, vec_out, chip_ref, chip_out, flat, vec, out_sem, chip_sem):
    outs = (e_out, a_out, f_out, h_out)
    chip = device_index() // 2
    copies = []
    for n, (tensor, d, source, target, rows) in enumerate(PIECES):
        copies.append(pltpu.make_async_copy(
            full_ref.at[d, pl.ds(source, rows), :], outs[tensor].at[pl.ds(target, rows), :], out_sem.at[n]))
        copies[-1].start()

    slot, source, _, _ = next(pieces_of(4))
    vec[pl.ds(0, 96), :] = full_ref[slot, pl.ds(source, 96), :].astype(jnp.float32)
    for n in range(VEC_ROWS // 8):
        vec_out[:, n * 1024:(n + 1) * 1024] = vec[n * 8:n * 8 + 8, :].reshape(1, 1024).astype(jnp.bfloat16)
    rest = VEC_ROWS % 8
    vec_out[:, VEC_ROWS // 8 * 1024:] = vec[pl.ds(VEC_ROWS - rest, rest), :].reshape(1, rest * LANES).astype(jnp.bfloat16)

    offset = 0
    for tensor, rows in enumerate(CHIP_COUNTS):
        base, _, tiles = TENSORS[tensor]
        step = 16 * tiles

        begin = base + chip * rows
        slot, low, bound = jnp.int32(0), jnp.int32(0), jnp.int32(OWN_STARTS[1])
        for d in range(1, SIXTEEN):
            inside = begin >= OWN_STARTS[d]
            slot = jnp.where(inside, d, slot)
            low = jnp.where(inside, OWN_STARTS[d], low)
            bound = jnp.where(inside, OWN_STARTS[d + 1], bound)

        @pl.loop(0, rows // step)
        def _(n):
            for half in range(2):
                row = begin + n * step + half * 8 * tiles
                following = row >= bound
                at_slot = jnp.where(following, slot + 1, slot)
                at_row = row - jnp.where(following, bound, low)
                for t in range(0, tiles, 2):
                    value = full_ref[at_slot, pl.ds(pl.multiple_of(at_row + 8 * t, 16), 16), :].astype(jnp.float32)
                    for k in range(2):
                        to = offset + n * step + half * 8 * tiles + t + k
                        flat[pl.ds(to, 8, stride=tiles), :] = value[8 * k:8 * k + 8]
        offset += rows

    vec_row = chip * (VEC_BLOCK // 32) // 4
    amount = chip * VEC_BLOCK - vec_row * LANES
    back = (LANES - amount) % LANES
    lane = lane_index()
    for n in range(2):
        here, below = vec[pl.ds(vec_row + n * 8, 8), :], vec[pl.ds(vec_row + n * 8 + 1, 8), :]
        flat[pl.ds(CHIP_ROWS + n * 8, 8), :] = jnp.where(
            lane < LANES - amount, pltpu.roll(here, back, 1), pltpu.roll(below, back, 1))

    def part_copy(part):
        span = pl.ds(part * CHIP_PART, CHIP_PART if part < CHIP_PARTS - 1 else CHIP_SIZE - part * CHIP_PART)
        return pltpu.make_async_copy(chip_out.at[:, span], chip_ref.at[:, span], chip_sem.at[part])

    for part in range(CHIP_PARTS):
        @pl.loop(part * CHIP_PART // 16384, (part + 1) * CHIP_PART // 16384)
        def _(n):
            chip_out[:, pl.ds(pl.multiple_of(n * 16384, 16384), 16384)] = flat[
                pl.ds(pl.multiple_of(n * 128, 128), 128), :].reshape(1, 16384).astype(jnp.bfloat16)
        if part > 0:
            part_copy(part - 1).start()
    done = CHIP_SIZE // 1024 * 1024
    rows = (CHIP_SIZE - done) // LANES
    last = CHIP_SIZE - done - rows * LANES
    first = done // LANES
    chip_out[:, CHIP_PARTS * CHIP_PART:done] = flat[CHIP_PARTS * CHIP_PART // LANES:first, :].reshape(
        1, done - CHIP_PARTS * CHIP_PART).astype(jnp.bfloat16)
    chip_out[:, done:done + rows * LANES] = flat[first:first + rows, :].reshape(1, rows * LANES).astype(jnp.bfloat16)
    chip_out[:, CHIP_SIZE - last:] = flat[first + rows:first + rows + 1, :last].astype(jnp.bfloat16)
    part_copy(CHIP_PARTS - 1).start()
    for part in range(CHIP_PARTS):
        part_copy(part).wait()
    for copy in copies:
        copy.wait()


def finish(full):
    vmem = pl.BlockSpec(memory_space=pltpu.VMEM)
    any_spec = pl.BlockSpec(memory_space=pl.ANY)
    shape = lambda rows: jax.ShapeDtypeStruct((rows, LANES), jnp.bfloat16)
    return pl.pallas_call(
        final_kernel,
        out_shape=tuple(shape(end - base) for base, end, _ in TENSORS[:4]) + (
            jax.ShapeDtypeStruct((1, VEC_WIDTH), jnp.bfloat16), jax.ShapeDtypeStruct((1, CHIP_SIZE), jnp.bfloat16)),
        in_specs=[vmem], out_specs=(any_spec,) * 4 + (vmem, any_spec),
        scratch_shapes=[
            pltpu.VMEM((1, CHIP_SIZE), jnp.bfloat16),
            pltpu.VMEM((CHIP_ROWS + 16, LANES), jnp.float32),
            pltpu.VMEM((120, LANES), jnp.float32),
            pltpu.SemaphoreType.DMA((len(PIECES),)), pltpu.SemaphoreType.DMA((CHIP_PARTS,)),
        ],
        compiler_params=pltpu.CompilerParams(vmem_limit_bytes=FINAL_LIMIT),
    )(full)


def solution(mesh):
    def local_step(g_embed, g_attn, g_ffn_in, g_ffn_out, g_vec, m_shard, v_shard, w_shard):
        matrices = (g_embed, g_attn, g_ffn_in, g_ffn_out)
        grads = [to_tiles(g[0] if g.ndim == 3 else g[0, 0]) for g in matrices]
        grads.append(jnp.pad(g_vec, ((0, 0), (0, 0), (0, VEC_BLOCK_ROWS * LANES - VEC_WIDTH))).reshape(VEC_BLOCK_ROWS, LANES))
        mean_tiles, edges = scatter(grads, m_shard, v_shard, w_shard)
        m_new, v_new, w_new, w_own = mid(mean_tiles, m_shard, v_shard, w_shard, edges)
        full = gather(w_own).reshape(SIXTEEN, OWN, LANES)
        *tiles, vec, w_chip = finish(full)
        tensors = [from_tiles(t, g.shape[-1]).reshape(g.shape[1:]) for t, g in zip(tiles, matrices)]
        return (m_new, v_new, w_new) + tuple(tensors) + (vec, w_chip)

    return jax.shard_map(local_step, mesh=mesh, in_specs=(P(MESH_AXES),) * 8, out_specs=(P(MESH_AXES),) * 3 + (P(),) * 5 + (P(MESH_AXES),), check_vma=False)
```

```python
import functools
import math
import jax
import jax.numpy as jnp
from jax import lax
from jax.experimental import pallas as pl
from jax.experimental.pallas import tpu as pltpu
from jax.sharding import PartitionSpec as P

MESH_AXES = ('outer', 'middle', 'inner')
MESH = pl.DeviceIdType.MESH
ADAM_BETA1 = 0.9
ADAM_BETA2 = 0.98
ADAM_EPS = 1e-9
LEARN_RATE = 0.05
ADAM_STEP = 3

LANES = 128
SLICE = 885488
TENSORS = ((0, 32768, 8), (32768, 65536, 32), (65536, 88064, 22), (88064, 110592, 8), (110592, 110720, 1))
ROWS = 110720
VEC_BLOCK_ROWS = 128
UNIT = 64
GROUP = 128
COMMON = 7168
WINDOW = COMMON + GROUP
LONG_SLICE = 10
COUNTS = (38, 38, 36)
FIRSTS = (0, 38, 76)
ITEMS = max(COUNTS)
LAG = 2
EDGE = 32768
OWN = 7104
OWN_THIRD = OWN // 3
OWN_CHUNK = 64
OWN_ITEMS = OWN_THIRD // OWN_CHUNK
OWN_LAG = 2
SIXTEEN = 16
FINAL_LIMIT = 20000000
GATHER_LIMIT = 6000000
MID_LIMIT = 52000000


def floor_block(row):
    result = row
    for base, end, tiles in TENSORS:
        block = 8 * tiles if tiles > 1 else VEC_BLOCK_ROWS
        floored = base + (row - base) // block * block
        result = jnp.where((row >= base) & (row < end), floored, result)
    return result


def window_start(index):
    row = floor_block(index * (SLICE // 16) // 8)
    return jnp.minimum(row // GROUP * GROUP, ROWS - COMMON)


def own_start_static(index):
    row = -(-index * SLICE // LANES)
    for base, end, tiles in TENSORS:
        if base <= row < end:
            block = 8 * tiles if tiles > 1 else VEC_BLOCK_ROWS
            return base + -(-(row - base) // block) * block
    return ROWS


OWN_STARTS = [own_start_static(d) for d in range(SIXTEEN)] + [ROWS]


def own_start(index):
    result = jnp.int32(0)
    for d in range(SIXTEEN):
        result = jnp.where(index == d, OWN_STARTS[d], result)
    return result


def adam_update(grad_mean, m_old, v_old, w_old):
    m_new = ADAM_BETA1 * m_old + (1.0 - ADAM_BETA1) * grad_mean
    v_new = ADAM_BETA2 * v_old + (1.0 - ADAM_BETA2) * (grad_mean * grad_mean)
    scale = LEARN_RATE / (1.0 - ADAM_BETA1 ** ADAM_STEP)
    w_new = w_old - scale * m_new / (jnp.sqrt(v_new * (1.0 / (1.0 - ADAM_BETA2 ** ADAM_STEP))) + ADAM_EPS)
    return m_new, v_new, w_new


def to_tiles(tensor):
    rows, width = tensor.shape
    return tensor.reshape(rows // 8, 8, width // LANES, LANES).transpose(0, 2, 1, 3).reshape(-1, LANES)


def from_tiles(tiles, width):
    return tiles.reshape(-1, width // LANES, 8, LANES).transpose(0, 2, 1, 3).reshape(-1, width)


ORDERS = ((0, 1, 2), (1, 2, 0), (2, 0, 1))


def position():
    outer, middle, inner = (lax.axis_index(name) for name in MESH_AXES)
    return outer, middle, inner // 2, inner % 2


def neighbour(axis):
    outer, middle, x, core = position()
    z, y = outer, middle
    if axis == 0:
        z = 1 - z
    elif axis == 1:
        y = 1 - y
    elif axis == 2:
        x = 1 - x
    else:
        core = 1 - core
    return (z, y, 2 * x + core)


def meet(devices):
    barrier = pltpu.get_barrier_semaphore()
    for device in devices:
        pl.semaphore_signal(barrier, inc=1, device_id=device, device_id_type=MESH)
    pl.semaphore_wait(barrier, len(devices))


def scatter_kernel(e_ref, a_ref, f_ref, h_ref, b_ref, m_ref, v_ref, w_ref, out_ref, edge_ref,
                   part, recv0, recv1, recv2, mine, pair_send, pair_recv, mine_sem,
                   send, arrive, out_sem, edge_send, edge_recv, long_mine, long_part, long_recv, long_sem, vec_raw, vec_rows, vec_sem):
    z, y, x, core = position()
    chip = (z * 2 + y) * 2 + x
    device = chip * 2 + core
    sources = (e_ref, a_ref, f_ref, h_ref, vec_rows)
    vec_load = pltpu.make_async_copy(b_ref, vec_raw, vec_sem)
    vec_load.start()

    before = (device + SIXTEEN - 1) % SIXTEEN
    after = (device + 1) % SIXTEEN
    meet([neighbour(axis) for axis in range(4)] + [(d // 8, d // 4 % 2, d % 4) for d in (before, after)])
    for n, ref in enumerate((m_ref, v_ref, w_ref)):
        pltpu.make_async_remote_copy(
            src_ref=ref.at[pl.ds(0, EDGE)], dst_ref=edge_ref.at[pl.ds(n * EDGE, EDGE)],
            send_sem=edge_send.at[n], recv_sem=edge_recv.at[n],
            device_id=(before // 8, before // 4 % 2, before % 4), device_id_type=MESH).start()

    def from_source(row, action):
        def choose(low, high):
            if high - low == 1:
                action(sources[low].at[pl.ds(pl.multiple_of(row - TENSORS[low][0], GROUP), GROUP), :])
                return
            middle = (low + high) // 2
            lax.cond(row < TENSORS[middle][0], lambda: choose(low, middle), lambda: choose(middle, high))
        choose(0, len(sources))

    def item_row(third, item):
        return pl.multiple_of((FIRSTS[third] + item) * UNIT, UNIT)

    def each_third(index, counts, action):
        for third in range(3):
            if counts[third] == max(counts):
                action(third)
            else:
                @pl.when(index < counts[third])
                def _():
                    action(third)

    def group_row(third, group):
        return pl.multiple_of(FIRSTS[third] * UNIT + group * GROUP, GROUP)

    def start_group(group, slot, side):
        @pl.loop(0, 4)
        def _(n):
            def action(third):
                index = [n // 2, n % 2]
                index = index[:ORDERS[third][0]] + [side] + index[ORDERS[third][0]:]
                jz, jy, jx = index
                other = ((z + jz) % 2 * 2 + (y + jy) % 2) * 2 + (x + jx) % 2
                theirs = window_start(other * 2 + 1 - core)
                ours = window_start(other * 2 + core)
                row = group_row(third, group)
                from_source(theirs + row, lambda src: pltpu.make_async_remote_copy(
                    src_ref=src, dst_ref=part.at[jz, jy, jx, pl.ds(row, GROUP), :],
                    send_sem=pair_send.at[third], recv_sem=pair_recv.at[side, third, group],
                    device_id=neighbour(3), device_id_type=MESH).start())
                from_source(ours + row, lambda src: pltpu.make_async_copy(
                    src, mine.at[slot, third, side, n], mine_sem.at[slot, third, side]).start())
            each_third(group, [count // 2 for count in COUNTS], action)

    def hop_copy(third, item, hop, whole=False):
        rows = pl.ds(item_row(third, 0), COUNTS[third] * UNIT) if whole else pl.ds(item_row(third, item), UNIT)
        first, second, last = ORDERS[third]
        if hop == 0:
            index = tuple(1 if n == first else slice(None) for n in range(3))
            target = recv0.at[:, :, rows, :]
        elif hop == 1:
            index = tuple(0 if n == first else 1 if n == second else slice(None) for n in range(3))
            target = recv1.at[:, rows, :]
        else:
            index = tuple(1 if n == last else 0 for n in range(3))
            target = recv2.at[rows, :]
        return pltpu.make_async_remote_copy(
            src_ref=part.at[index + (rows, slice(None))], dst_ref=target,
            send_sem=send.at[third, hop], recv_sem=arrive.at[third, hop, item],
            device_id=neighbour(ORDERS[third][hop]), device_id_type=MESH)

    def pair_side(third, group, side):
        index = tuple(side if n == ORDERS[third][0] else slice(None) for n in range(3))
        block = part.at[index + (pl.ds(group_row(third, group), GROUP), slice(None))]
        return pltpu.make_async_remote_copy(
            src_ref=block, dst_ref=block, send_sem=pair_send.at[third], recv_sem=pair_recv.at[side, third, group],
            device_id=neighbour(3), device_id_type=MESH)

    def pair_whole(third):
        block = part.at[:, :, :, pl.ds(FIRSTS[third] * UNIT, COUNTS[third] * UNIT), :]
        return pltpu.make_async_remote_copy(
            src_ref=block, dst_ref=block, send_sem=pair_send.at[third], recv_sem=pair_recv.at[0, third, 0],
            device_id=neighbour(3), device_id_type=MESH)

    def out_copy(third, item, whole=False):
        rows = pl.ds(item_row(third, 0), COUNTS[third] * UNIT) if whole else pl.ds(item_row(third, item), UNIT)
        return pltpu.make_async_copy(part.at[0, 0, 0, rows, :], out_ref.at[rows, :], out_sem.at[third])

    start_group(0, 0, 1)
    start_group(0, 0, 0)

    def add_mine(side, item, third):
        rows = pl.ds(item_row(third, item), UNIT)
        group = item // 2
        slot = group % 2

        @pl.when(item % 2 == 0)
        def _():
            block = mine.at[slot, third, side]
            pltpu.make_async_copy(block, block, mine_sem.at[slot, third, side]).wait()
            pair_side(third, group, side).wait_recv()
        within = pl.ds(pl.multiple_of(item % 2 * UNIT, UNIT), UNIT)
        first = ORDERS[third][0]
        for n in range(4):
            index = [n // 2, n % 2]
            index = tuple(index[:first] + [side] + index[first:])
            part[index + (rows, slice(None))] += mine[slot, third, side, n, within, :]
        if side:
            hop_copy(third, item, 0).start()

    def stage1(item, third):
        rows = pl.ds(item_row(third, item), UNIT)
        hop_copy(third, item, 0).wait_recv()
        first = ORDERS[third][0]
        for j in range(4):
            pair = [j // 2, j % 2]
            index = tuple(pair[:first] + [0] + pair[first:])
            part[index + (rows, slice(None))] += recv0[j // 2, j % 2, rows, :]
        hop_copy(third, item, 1).start()

    def stage2(item, third):
        rows = pl.ds(item_row(third, item), UNIT)
        hop_copy(third, item, 1).wait_recv()
        last = ORDERS[third][2]
        for j in range(2):
            index = tuple(j if n == last else 0 for n in range(3))
            part[index + (rows, slice(None))] += recv1[j, rows, :]
        hop_copy(third, item, 2).start()

    def stage3(item, third):
        rows = pl.ds(item_row(third, item), UNIT)
        hop_copy(third, item, 2).wait_recv()
        part[0, 0, 0, rows, :] = (part[0, 0, 0, rows, :] + recv2[rows, :]) / SIXTEEN

    long_chip, long_core = LONG_SLICE // 2, LONG_SLICE % 2
    lz, ly, lx = (z + long_chip // 4) % 2, (y + long_chip // 2 % 2) % 2, (x + long_chip % 2) % 2
    long_row = window_start(LONG_SLICE) + COMMON
    holder = core == long_core

    def long_pair():
        return pltpu.make_async_remote_copy(
            src_ref=long_mine, dst_ref=long_part, send_sem=long_sem.at[0], recv_sem=long_sem.at[1],
            device_id=neighbour(3), device_id_type=MESH)

    def long_load():
        return pltpu.make_async_copy(
            sources[2].at[pl.ds(pl.multiple_of(long_row - TENSORS[2][0], GROUP), GROUP), :], long_mine, long_sem.at[2])

    def long_hop(hop):
        return pltpu.make_async_remote_copy(
            src_ref=long_part, dst_ref=long_recv.at[hop], send_sem=long_sem.at[3 + hop], recv_sem=long_sem.at[6 + hop],
            device_id=neighbour((2, 0, 1)[hop]), device_id_type=MESH)

    def long_out():
        return pltpu.make_async_copy(long_part, out_ref.at[pl.ds(COMMON, GROUP), :], long_sem.at[9])

    reached = (holder, holder & (lx == 0), holder & (lx == 0) & (lz == 0), holder & (lx == 0) & (lz == 0) & (ly == 0))
    far = (lx == 1, lz == 1, ly == 1)

    def long_start():
        long_load().start()

    def long_exchange():
        long_load().wait()

        @pl.when(core != long_core)
        def _():
            long_pair().start()

    def long_sum():
        @pl.when(holder)
        def _():
            long_pair().wait_recv()
            long_part[...] += long_mine[...]

        @pl.when(core != long_core)
        def _():
            long_pair().wait_send()

    def long_send(hop):
        @pl.when(reached[hop] & far[hop])
        def _():
            long_hop(hop).start()

    def long_add(hop):
        @pl.when(reached[hop] & far[hop])
        def _():
            long_hop(hop).wait_send()

        @pl.when(reached[hop + 1])
        def _():
            long_hop(hop).wait_recv()
            if hop < 2:
                long_part[...] += long_recv[hop]
            else:
                long_part[...] = (long_part[...] + long_recv[hop]) / SIXTEEN

    def long_store():
        @pl.when(reached[3])
        def _():
            long_out().start()

    long_stages = ((4, long_start), (6, long_exchange), (8, long_sum)) + tuple(
        (9 + 3 * hop + k, functools.partial((long_send, long_add)[k // 2], hop)) for hop in range(3) for k in (0, 2)
    ) + ((19, long_store),)

    stages = ((0, functools.partial(add_mine, 1)), (0, functools.partial(add_mine, 0)), (LAG, stage1), (2 * LAG, stage2), (3 * LAG, stage3),
              (3 * LAG + 1, lambda item, third: out_copy(third, item).start()))

    vec_load.wait()
    vec_rows[pl.ds(VEC_ROWS // 8 * 8, VEC_BLOCK_ROWS - VEC_ROWS // 8 * 8), :] = jnp.zeros(
        (VEC_BLOCK_ROWS - VEC_ROWS // 8 * 8, LANES), jnp.float32)
    for n in range(-(-VEC_ROWS // 8)):
        rows = min(8, VEC_ROWS - n * 8)
        vec_rows[n * 8:n * 8 + rows, :] = vec_raw[:, n * 1024:n * 1024 + rows * LANES].reshape(rows, LANES)

    @pl.loop(0, ITEMS + stages[-1][0])
    def _(step):
        for delay, stage in stages:
            @pl.when((step >= delay) & (step < ITEMS + delay))
            def _():
                each_third(step - delay, COUNTS, functools.partial(stage, step - delay))

        for at, stage in long_stages:
            @pl.when(step == at)
            def _():
                stage()

        @pl.when((step % 2 == 0) & (step + 2 < ITEMS))
        def _():
            start_group(step // 2 + 1, (step // 2 + 1) % 2, 1)
            start_group(step // 2 + 1, (step // 2 + 1) % 2, 0)

    for third in range(3):
        pair_whole(third).wait_send()
        for hop in range(3):
            hop_copy(third, 0, hop, True).wait_send()
        out_copy(third, 0, True).wait()

    @pl.when(reached[3])
    def _():
        long_out().wait()

    for n, ref in enumerate((m_ref, v_ref, w_ref)):
        pltpu.make_async_remote_copy(
            src_ref=ref.at[pl.ds(0, EDGE)], dst_ref=edge_ref.at[pl.ds(n * EDGE, EDGE)],
            send_sem=edge_send.at[n], recv_sem=edge_recv.at[n],
            device_id=(before // 8, before // 4 % 2, before % 4), device_id_type=MESH).wait()


def scatter(grads, m, v, w):
    any_spec = pl.BlockSpec(memory_space=pl.ANY)
    dma = pltpu.SemaphoreType.DMA
    return pl.pallas_call(
        scatter_kernel,
        out_shape=(jax.ShapeDtypeStruct((WINDOW, LANES), jnp.float32), jax.ShapeDtypeStruct((3 * EDGE,), jnp.float32)),
        in_specs=[any_spec] * 8,
        out_specs=(any_spec, any_spec),
        scratch_shapes=[
            pltpu.VMEM((2, 2, 2, COMMON, LANES), jnp.float32),
            pltpu.VMEM((2, 2, COMMON, LANES), jnp.float32),
            pltpu.VMEM((2, COMMON, LANES), jnp.float32),
            pltpu.VMEM((COMMON, LANES), jnp.float32),
            pltpu.VMEM((2, 3, 2, 4, GROUP, LANES), jnp.float32),
            dma((3,)), dma((2, 3, ITEMS // 2)), dma((2, 3, 2)),
            dma((3, 3)), dma((3, 3, ITEMS)), dma((3,)), dma((3,)), dma((3,)),
            pltpu.VMEM((GROUP, LANES), jnp.float32), pltpu.VMEM((GROUP, LANES), jnp.float32),
            pltpu.VMEM((3, GROUP, LANES), jnp.float32), dma((10,)),
            pltpu.VMEM((1, VEC_WIDTH), jnp.float32), pltpu.VMEM((VEC_BLOCK_ROWS, LANES), jnp.float32), dma(()),
        ],
        compiler_params=pltpu.CompilerParams(has_side_effects=True, collective_id=0, vmem_limit_bytes=67043328),
    )(*grads, m, v, w)


def gather_kernel(w_ref, full_ref, pair_send, pair_recv, send, arrive):
    z, y, x, core = position()
    here = (z, y, x)

    def rows_of(third, item, whole=False):
        if whole:
            return pl.ds(third * OWN_THIRD, OWN_THIRD)
        return pl.ds(pl.multiple_of(third * OWN_THIRD + item * OWN_CHUNK, OWN_CHUNK), OWN_CHUNK)

    def copy(third, item, hop, whole=False):
        rows = rows_of(third, item, whole)
        order = ORDERS[third]
        if hop == 0:
            source = w_ref.at[rows, :]
            target = full_ref.at[z, y, x, core, rows, :]
        else:
            index = tuple(slice(None) if n in order[:hop] else here[n] for n in range(3))
            source = target = full_ref.at[index + (core, rows, slice(None))]
        return pltpu.make_async_remote_copy(
            src_ref=source, dst_ref=target, send_sem=send.at[third, hop], recv_sem=arrive.at[third, item, hop],
            device_id=neighbour(order[hop]), device_id_type=MESH)

    def arrival(third, item, hop):
        order = ORDERS[third]
        index = tuple(slice(None) if n in order[:hop] else (1 - here[n] if n == order[hop] else here[n]) for n in range(3))
        block = full_ref.at[index + (core, rows_of(third, item), slice(None))]
        return pltpu.make_async_remote_copy(
            src_ref=block, dst_ref=block, send_sem=send.at[third, hop], recv_sem=arrive.at[third, item, hop],
            device_id=neighbour(order[hop]), device_id_type=MESH)

    def pair(third, item, side, whole=False):
        block = full_ref.at[:, :, :, side, rows_of(third, item, whole), :]
        return pltpu.make_async_remote_copy(
            src_ref=block, dst_ref=block, send_sem=pair_send.at[third], recv_sem=pair_recv.at[third, item],
            device_id=neighbour(3), device_id_type=MESH)

    meet([neighbour(axis) for axis in range(4)])
    for item in range(OWN_LAG):
        for third in range(3):
            copy(third, item, 0).start()

    @pl.loop(0, OWN // OWN_CHUNK)
    def _(n):
        rows = pl.ds(pl.multiple_of(n * OWN_CHUNK, OWN_CHUNK), OWN_CHUNK)
        full_ref[z, y, x, core, rows, :] = w_ref[rows, :]

    @pl.loop(0, OWN_ITEMS + 2 * OWN_LAG)
    def _(step):
        @pl.when(step + OWN_LAG < OWN_ITEMS)
        def _():
            for third in range(3):
                copy(third, step + OWN_LAG, 0).start()

        for hop in range(1, 4):
            delay = (hop - 1) * OWN_LAG

            @pl.when((step >= delay) & (step < OWN_ITEMS + delay))
            def _():
                item = step - delay
                for third in range(3):
                    arrival(third, item, hop - 1).wait_recv()
                    if hop < 3:
                        copy(third, item, hop).start()
                    else:
                        pair(third, item, core).start()

    @pl.loop(0, OWN_ITEMS)
    def _(item):
        for third in range(3):
            pair(third, item, 1 - core).wait_recv()
    for third in range(3):
        pair(third, 0, core, True).wait_send()
        for hop in range(3):
            copy(third, 0, hop, True).wait_send()


def gather(w_own):
    dma = pltpu.SemaphoreType.DMA
    return pl.pallas_call(
        gather_kernel,
        out_shape=jax.ShapeDtypeStruct((2, 2, 2, 2, OWN, LANES), jnp.bfloat16),
        in_specs=[pl.BlockSpec(memory_space=pltpu.VMEM)],
        out_specs=pl.BlockSpec(memory_space=pltpu.VMEM),
        scratch_shapes=[
            dma((3,)), dma((3, OWN_ITEMS)), dma((3, 3)), dma((3, OWN_ITEMS, 3)),
        ],
        compiler_params=pltpu.CompilerParams(has_side_effects=True, collective_id=1, vmem_limit_bytes=GATHER_LIMIT),
    )(w_own)


def device_index():
    outer, middle, inner = (lax.axis_index(name) for name in MESH_AXES)
    return (outer * 2 + middle) * 4 + inner


def for_blocks(start, length, action, tensors=TENSORS):
    for base, end, tiles in tensors:
        block = 8 * tiles
        low = (jnp.maximum(start, base) - base + block - 1) // block
        high = jnp.maximum(jnp.minimum(start + length, end) - base, 0) // block

        count = jnp.maximum(high - low, 0)
        together = 4 if tiles <= 8 else 1

        @pl.loop(0, count // together)
        def _(n):
            for k in range(together):
                action(pl.multiple_of(base + (low + n * together + k) * block - start, 8), tiles)

        if together > 1:
            @pl.loop(count // together * together, count)
            def _(n):
                action(pl.multiple_of(base + (low + n) * block - start, 8), tiles)


PAD = 8
FLAT_ROWS = WINDOW + 272
SHARD_VREGS = SLICE // 1024
TAIL_ROWS = SLICE % 1024 // LANES
TAIL_LANES = SLICE % LANES
EDGE_ROWS = EDGE // LANES
OWN_FLAT_ROWS = OWN + 512


def lane_index(rows=8):
    return lax.broadcasted_iota(jnp.int32, (rows, LANES), 1)


BATCH = 256
BATCHES = SHARD_VREGS * 8 // BATCH
CHUNK_BATCHES = 3
CHUNKS = BATCHES // CHUNK_BATCHES
CHUNK = CHUNK_BATCHES * BATCH * LANES


def mid_kernel(tile_ref, m_ref, v_ref, w_ref, edge_ref, m_out, v_out, w_out, own_ref,
               m_buf, v_buf, w_buf, flat, shifted, edged, aligned, in_sem, out_sem):
    device = device_index()
    start = window_start(device)
    arrays = ((m_ref, m_buf, m_out), (v_ref, v_buf, v_out), (w_ref, w_buf, w_out))

    def span(chunk):
        return pl.ds(chunk * CHUNK, CHUNK if chunk < CHUNKS - 1 else SLICE - chunk * CHUNK)

    def loads(chunk):
        return [pltpu.make_async_copy(ref.at[span(chunk)], buf.at[span(chunk)], in_sem.at[n, chunk])
                for n, (ref, buf, _) in enumerate(arrays)]

    def stores(chunk):
        return [pltpu.make_async_copy(buf.at[span(chunk)], out.at[span(chunk)], out_sem.at[n, chunk])
                for n, (_, buf, out) in enumerate(arrays)]

    for chunk in range(CHUNKS):
        for copy in loads(chunk):
            copy.start()

    def to_flat(row, tiles):
        for t in range(tiles):
            flat[pl.ds(row + t, 8, stride=tiles), :] = tile_ref[pl.ds(row + 8 * t, 8), :]
    for_blocks(start, WINDOW, to_flat)

    first_row = device * (SLICE // 16) // 8
    next_row = (device + 1) * (SLICE // 16) // 8
    shift = device * SLICE - first_row * LANES
    next_shift = (device + 1) * SLICE - next_row * LANES

    def mean_rows(row, amount, rows):
        here = flat[pl.ds(row, rows), :]
        below = flat[pl.ds(row + 1, rows), :]
        back = (LANES - amount) % LANES
        return jnp.where(lane_index(rows) < LANES - amount, pltpu.roll(here, back, 1), pltpu.roll(below, back, 1))

    for chunk in range(CHUNKS):
        for copy in loads(chunk):
            copy.wait()

        @pl.loop(chunk * CHUNK_BATCHES, (chunk + 1) * CHUNK_BATCHES)
        def _(n):
            at = pl.ds(pl.multiple_of(n * BATCH * LANES, BATCH * LANES), BATCH * LANES)
            mean = mean_rows(first_row - start + n * BATCH, shift, BATCH)
            new = adam_update(mean, *(buf[at].reshape(BATCH, LANES) for _, buf, _ in arrays))
            for (_, buf, _), value in zip(arrays, new):
                buf[at] = value.reshape(BATCH * LANES)
            shifted[pl.ds(pl.multiple_of(PAD + n * BATCH, 8), BATCH), :] = pltpu.roll(new[2], shift, 1)

        if chunk > 0:
            for copy in stores(chunk - 1):
                copy.start()

    mean = mean_rows(first_row - start + SHARD_VREGS * 8, shift, 8)
    for r in range(TAIL_ROWS + 1):
        size = LANES if r < TAIL_ROWS else TAIL_LANES
        at = pl.ds(SHARD_VREGS * 1024 + r * LANES, size)
        new = adam_update(mean[r:r + 1, :size], *(buf[at].reshape(1, size) for _, buf, _ in arrays))
        for (_, buf, _), value in zip(arrays, new):
            buf[at] = value.reshape(size)
        flat[pl.ds(FLAT_ROWS - 8 + r, 1), pl.ds(0, size)] = new[2]
    shifted[pl.ds(PAD + SHARD_VREGS * 8, 8), :] = pltpu.roll(flat[pl.ds(FLAT_ROWS - 8, 8), :], shift, 1)

    @pl.loop(0, EDGE_ROWS // 64)
    def _(n):
        mean = mean_rows(next_row - start + n * 64, next_shift, 64)
        old = (edge_ref[pl.ds(pl.multiple_of(k * EDGE + n * 8192, 1024), 8192)].reshape(64, LANES) for k in range(3))
        edged[pl.ds(pl.multiple_of(PAD + n * 64, 8), 64), :] = pltpu.roll(adam_update(mean, *old)[2], next_shift, 1)

    for copy in stores(CHUNKS - 1):
        copy.start()

    own = own_start(device)
    skip = own - first_row

    @pl.loop(0, BATCHES + 1)
    def _(n):
        row = PAD + skip + n * BATCH
        aligned[pl.ds(pl.multiple_of(n * BATCH, 8), BATCH), :] = jnp.where(
            lane_index(BATCH) >= shift, shifted[pl.ds(row, BATCH), :], shifted[pl.ds(row - 1, BATCH), :])
    edged[pl.ds(PAD - 1, 1), :] = aligned[pl.ds(next_row - own, 1), :]

    @pl.loop(0, EDGE_ROWS // 64)
    def _(n):
        row = PAD + n * 64
        aligned[pl.ds(next_row - own + n * 64, 64), :] = jnp.where(
            lane_index(64) >= next_shift, edged[pl.ds(row, 64), :], edged[pl.ds(row - 1, 64), :])

    def to_tile(row, tiles):
        for t in range(0, tiles, 2):
            both = [aligned[pl.ds(row + t + k, 8, stride=tiles), :] for k in range(2)]
            own_ref[pl.ds(pl.multiple_of(row + 8 * t, 16), 16), :] = jnp.concatenate(both, axis=0).astype(jnp.bfloat16)

    def plain(row, _):
        own_ref[pl.ds(pl.multiple_of(row, 16), 16), :] = aligned[pl.ds(row, 16), :].astype(jnp.bfloat16)
    for_blocks(own, OWN, to_tile, TENSORS[:4])
    for_blocks(own, OWN, plain, ((*TENSORS[4][:2], 2),))

    for chunk in range(CHUNKS):
        for copy in stores(chunk):
            copy.wait()


def mid(mean_tiles, m, v, w, edges):
    vmem = pl.BlockSpec(memory_space=pltpu.VMEM)
    any_spec = pl.BlockSpec(memory_space=pl.ANY)
    shard = jax.ShapeDtypeStruct((SLICE,), jnp.float32)
    return pl.pallas_call(
        mid_kernel,
        out_shape=(shard, shard, shard, jax.ShapeDtypeStruct((OWN, LANES), jnp.bfloat16)),
        in_specs=[vmem, any_spec, any_spec, any_spec, vmem], out_specs=(any_spec, any_spec, any_spec, vmem),
        scratch_shapes=[
            pltpu.VMEM((SLICE,), jnp.float32), pltpu.VMEM((SLICE,), jnp.float32), pltpu.VMEM((SLICE,), jnp.float32),
            pltpu.VMEM((FLAT_ROWS, LANES), jnp.float32),
            pltpu.VMEM((PAD + SHARD_VREGS * 8 + 8 + 512, LANES), jnp.float32),
            pltpu.VMEM((PAD + EDGE_ROWS, LANES), jnp.float32),
            pltpu.VMEM((OWN_FLAT_ROWS, LANES), jnp.float32),
            pltpu.SemaphoreType.DMA((3, CHUNKS)), pltpu.SemaphoreType.DMA((3, CHUNKS)),
        ],
        compiler_params=pltpu.CompilerParams(vmem_limit_bytes=MID_LIMIT),
    )(mean_tiles, m, v, w, edges)


def pieces_of(tensor):
    base, end, _ = TENSORS[tensor]
    for d in range(SIXTEEN):
        low, high = max(OWN_STARTS[d], base), min(OWN_STARTS[d + 1], end)
        if low < high:
            yield d, low - OWN_STARTS[d], low - base, high - low


PIECES = [(tensor,) + piece for tensor in range(4) for piece in pieces_of(tensor)]
VEC_WIDTH = 12032
VEC_ROWS = VEC_WIDTH // LANES
VEC_BLOCK = VEC_WIDTH // 8
CHIP_COUNTS = tuple((end - base) // 8 for base, end, _ in TENSORS[:4])
CHIP_ROWS = sum(CHIP_COUNTS)
CHIP_SIZE = CHIP_ROWS * LANES + VEC_BLOCK
CHIP_PARTS = 6
CHIP_PART = CHIP_SIZE // 16384 // CHIP_PARTS * 16384


def final_kernel(full_ref, e_out, a_out, f_out, h_out, vec_out, chip_ref, chip_out, flat, vec, out_sem, chip_sem):
    outs = (e_out, a_out, f_out, h_out)
    chip = device_index() // 2
    copies = []
    for n, (tensor, d, source, target, rows) in enumerate(PIECES):
        copies.append(pltpu.make_async_copy(
            full_ref.at[d, pl.ds(source, rows), :], outs[tensor].at[pl.ds(target, rows), :], out_sem.at[n]))
        copies[-1].start()

    slot, source, _, _ = next(pieces_of(4))
    vec[pl.ds(0, 96), :] = full_ref[slot, pl.ds(source, 96), :].astype(jnp.float32)
    for n in range(VEC_ROWS // 8):
        vec_out[:, n * 1024:(n + 1) * 1024] = vec[n * 8:n * 8 + 8, :].reshape(1, 1024).astype(jnp.bfloat16)
    rest = VEC_ROWS % 8
    vec_out[:, VEC_ROWS // 8 * 1024:] = vec[pl.ds(VEC_ROWS - rest, rest), :].reshape(1, rest * LANES).astype(jnp.bfloat16)

    offset = 0
    for tensor, rows in enumerate(CHIP_COUNTS):
        base, _, tiles = TENSORS[tensor]
        step = 16 * tiles

        begin = base + chip * rows
        slot, low, bound = jnp.int32(0), jnp.int32(0), jnp.int32(OWN_STARTS[1])
        for d in range(1, SIXTEEN):
            inside = begin >= OWN_STARTS[d]
            slot = jnp.where(inside, d, slot)
            low = jnp.where(inside, OWN_STARTS[d], low)
            bound = jnp.where(inside, OWN_STARTS[d + 1], bound)

        @pl.loop(0, rows // step)
        def _(n):
            for half in range(2):
                row = begin + n * step + half * 8 * tiles
                following = row >= bound
                at_slot = jnp.where(following, slot + 1, slot)
                at_row = row - jnp.where(following, bound, low)
                for t in range(0, tiles, 2):
                    value = full_ref[at_slot, pl.ds(pl.multiple_of(at_row + 8 * t, 16), 16), :].astype(jnp.float32)
                    for k in range(2):
                        to = offset + n * step + half * 8 * tiles + t + k
                        flat[pl.ds(to, 8, stride=tiles), :] = value[8 * k:8 * k + 8]
        offset += rows

    vec_row = chip * (VEC_BLOCK // 32) // 4
    amount = chip * VEC_BLOCK - vec_row * LANES
    back = (LANES - amount) % LANES
    lane = lane_index()
    for n in range(2):
        here, below = vec[pl.ds(vec_row + n * 8, 8), :], vec[pl.ds(vec_row + n * 8 + 1, 8), :]
        flat[pl.ds(CHIP_ROWS + n * 8, 8), :] = jnp.where(
            lane < LANES - amount, pltpu.roll(here, back, 1), pltpu.roll(below, back, 1))

    def part_copy(part):
        span = pl.ds(part * CHIP_PART, CHIP_PART if part < CHIP_PARTS - 1 else CHIP_SIZE - part * CHIP_PART)
        return pltpu.make_async_copy(chip_out.at[:, span], chip_ref.at[:, span], chip_sem.at[part])

    for part in range(CHIP_PARTS):
        @pl.loop(part * CHIP_PART // 16384, (part + 1) * CHIP_PART // 16384)
        def _(n):
            chip_out[:, pl.ds(pl.multiple_of(n * 16384, 16384), 16384)] = flat[
                pl.ds(pl.multiple_of(n * 128, 128), 128), :].reshape(1, 16384).astype(jnp.bfloat16)
        if part > 0:
            part_copy(part - 1).start()
    done = CHIP_SIZE // 1024 * 1024
    rows = (CHIP_SIZE - done) // LANES
    last = CHIP_SIZE - done - rows * LANES
    first = done // LANES
    chip_out[:, CHIP_PARTS * CHIP_PART:done] = flat[CHIP_PARTS * CHIP_PART // LANES:first, :].reshape(
        1, done - CHIP_PARTS * CHIP_PART).astype(jnp.bfloat16)
    chip_out[:, done:done + rows * LANES] = flat[first:first + rows, :].reshape(1, rows * LANES).astype(jnp.bfloat16)
    chip_out[:, CHIP_SIZE - last:] = flat[first + rows:first + rows + 1, :last].astype(jnp.bfloat16)
    part_copy(CHIP_PARTS - 1).start()
    for part in range(CHIP_PARTS):
        part_copy(part).wait()
    for copy in copies:
        copy.wait()


def finish(full):
    vmem = pl.BlockSpec(memory_space=pltpu.VMEM)
    any_spec = pl.BlockSpec(memory_space=pl.ANY)
    shape = lambda rows: jax.ShapeDtypeStruct((rows, LANES), jnp.bfloat16)
    return pl.pallas_call(
        final_kernel,
        out_shape=tuple(shape(end - base) for base, end, _ in TENSORS[:4]) + (
            jax.ShapeDtypeStruct((1, VEC_WIDTH), jnp.bfloat16), jax.ShapeDtypeStruct((1, CHIP_SIZE), jnp.bfloat16)),
        in_specs=[vmem], out_specs=(any_spec,) * 4 + (vmem, any_spec),
        scratch_shapes=[
            pltpu.VMEM((1, CHIP_SIZE), jnp.bfloat16),
            pltpu.VMEM((CHIP_ROWS + 16, LANES), jnp.float32),
            pltpu.VMEM((120, LANES), jnp.float32),
            pltpu.SemaphoreType.DMA((len(PIECES),)), pltpu.SemaphoreType.DMA((CHIP_PARTS,)),
        ],
        compiler_params=pltpu.CompilerParams(vmem_limit_bytes=FINAL_LIMIT),
    )(full)


def solution(mesh):
    def local_step(g_embed, g_attn, g_ffn_in, g_ffn_out, g_vec, m_shard, v_shard, w_shard):
        matrices = (g_embed, g_attn, g_ffn_in, g_ffn_out)
        grads = [to_tiles(g[0] if g.ndim == 3 else g[0, 0]) for g in matrices]
        grads.append(g_vec.reshape(1, -1))
        mean_tiles, edges = scatter(grads, m_shard, v_shard, w_shard)
        m_new, v_new, w_new, w_own = mid(mean_tiles, m_shard, v_shard, w_shard, edges)
        full = gather(w_own).reshape(SIXTEEN, OWN, LANES)
        *tiles, vec, w_chip = finish(full)
        tensors = [from_tiles(t, g.shape[-1]).reshape(g.shape[1:]) for t, g in zip(tiles, matrices)]
        return (m_new, v_new, w_new) + tuple(tensors) + (vec, w_chip)

    return jax.shard_map(local_step, mesh=mesh, in_specs=(P(MESH_AXES),) * 8, out_specs=(P(MESH_AXES),) * 3 + (P(),) * 5 + (P(MESH_AXES),), check_vma=False)
```

```python
import functools
import math
import jax
import jax.numpy as jnp
from jax import lax
from jax.experimental import pallas as pl
from jax.experimental.pallas import tpu as pltpu
from jax.sharding import PartitionSpec as P

MESH_AXES = ('outer', 'middle', 'inner')
MESH = pl.DeviceIdType.MESH
ADAM_BETA1 = 0.9
ADAM_BETA2 = 0.98
ADAM_EPS = 1e-9
LEARN_RATE = 0.05
ADAM_STEP = 3

LANES = 128
SLICE = 885488
TENSORS = ((0, 32768, 8), (32768, 65536, 32), (65536, 88064, 22), (88064, 110592, 8), (110592, 110720, 1))
ROWS = 110720
VEC_BLOCK_ROWS = 128
UNIT = 64
GROUP = 128
COMMON = 7168
WINDOW = COMMON + GROUP
LONG_SLICE = 10
COUNTS = (38, 38, 36)
FIRSTS = (0, 38, 76)
ITEMS = max(COUNTS)
LAG = 2
EDGE = 32768
OWN = 7104
OWN_THIRD = OWN // 3
OWN_CHUNK = 64
OWN_ITEMS = OWN_THIRD // OWN_CHUNK
OWN_LAG = 2
SIXTEEN = 16
FINAL_LIMIT = 20000000
GATHER_LIMIT = 6000000
MID_LIMIT = 52000000


def floor_block(row):
    result = row
    for base, end, tiles in TENSORS:
        block = 8 * tiles if tiles > 1 else VEC_BLOCK_ROWS
        floored = base + (row - base) // block * block
        result = jnp.where((row >= base) & (row < end), floored, result)
    return result


def window_start(index):
    row = floor_block(index * (SLICE // 16) // 8)
    return jnp.minimum(row // GROUP * GROUP, ROWS - COMMON)


def own_start_static(index):
    row = -(-index * SLICE // LANES)
    for base, end, tiles in TENSORS:
        if base <= row < end:
            block = 8 * tiles if tiles > 1 else VEC_BLOCK_ROWS
            return base + -(-(row - base) // block) * block
    return ROWS


OWN_STARTS = [own_start_static(d) for d in range(SIXTEEN)] + [ROWS]


def own_start(index):
    result = jnp.int32(0)
    for d in range(SIXTEEN):
        result = jnp.where(index == d, OWN_STARTS[d], result)
    return result


def adam_update(grad_mean, m_old, v_old, w_old):
    m_new = ADAM_BETA1 * m_old + (1.0 - ADAM_BETA1) * grad_mean
    v_new = ADAM_BETA2 * v_old + (1.0 - ADAM_BETA2) * (grad_mean * grad_mean)
    scale = LEARN_RATE / (1.0 - ADAM_BETA1 ** ADAM_STEP)
    w_new = w_old - scale * m_new / (jnp.sqrt(v_new * (1.0 / (1.0 - ADAM_BETA2 ** ADAM_STEP))) + ADAM_EPS)
    return m_new, v_new, w_new


def to_tiles(tensor):
    rows, width = tensor.shape
    return tensor.reshape(rows // 8, 8, width // LANES, LANES).transpose(0, 2, 1, 3).reshape(-1, LANES)


def from_tiles(tiles, width):
    return tiles.reshape(-1, width // LANES, 8, LANES).transpose(0, 2, 1, 3).reshape(-1, width)


ORDERS = ((0, 1, 2), (1, 2, 0), (2, 0, 1))


def position():
    outer, middle, inner = (lax.axis_index(name) for name in MESH_AXES)
    return outer, middle, inner // 2, inner % 2


def neighbour(axis):
    outer, middle, x, core = position()
    z, y = outer, middle
    if axis == 0:
        z = 1 - z
    elif axis == 1:
        y = 1 - y
    elif axis == 2:
        x = 1 - x
    else:
        core = 1 - core
    return (z, y, 2 * x + core)


def meet(devices):
    barrier = pltpu.get_barrier_semaphore()
    for device in devices:
        pl.semaphore_signal(barrier, inc=1, device_id=device, device_id_type=MESH)
    pl.semaphore_wait(barrier, len(devices))


def scatter_kernel(e_ref, a_ref, f_ref, h_ref, b_ref, m_ref, v_ref, w_ref, out_ref, edge_ref,
                   part, recv0, recv1, recv2, mine, pair_send, pair_recv, mine_sem,
                   send, arrive, out_sem, edge_send, edge_recv, long_mine, long_part, long_recv, long_sem, vec_raw, vec_rows, vec_sem):
    z, y, x, core = position()
    chip = (z * 2 + y) * 2 + x
    device = chip * 2 + core
    sources = (e_ref, a_ref, f_ref, h_ref, vec_rows)
    vec_load = pltpu.make_async_copy(b_ref, vec_raw, vec_sem)
    vec_load.start()

    before = (device + SIXTEEN - 1) % SIXTEEN
    after = (device + 1) % SIXTEEN
    meet([neighbour(axis) for axis in range(4)] + [(d // 8, d // 4 % 2, d % 4) for d in (before, after)])
    for n, ref in enumerate((m_ref, v_ref, w_ref)):
        pltpu.make_async_remote_copy(
            src_ref=ref.at[pl.ds(0, EDGE)], dst_ref=edge_ref.at[pl.ds(n * EDGE, EDGE)],
            send_sem=edge_send.at[n], recv_sem=edge_recv.at[n],
            device_id=(before // 8, before // 4 % 2, before % 4), device_id_type=MESH).start()

    def from_source(row, action):
        def choose(low, high):
            if high - low == 1:
                action(sources[low].at[pl.ds(pl.multiple_of(row - TENSORS[low][0], GROUP), GROUP), :])
                return
            middle = (low + high) // 2
            lax.cond(row < TENSORS[middle][0], lambda: choose(low, middle), lambda: choose(middle, high))
        choose(0, len(sources))

    def item_row(third, item):
        return pl.multiple_of((FIRSTS[third] + item) * UNIT, UNIT)

    def each_third(index, counts, action):
        for third in range(3):
            if counts[third] == max(counts):
                action(third)
            else:
                @pl.when(index < counts[third])
                def _():
                    action(third)

    def group_row(third, group):
        return pl.multiple_of(FIRSTS[third] * UNIT + group * GROUP, GROUP)

    def start_group(group, slot):
        @pl.loop(0, 8)
        def _(j):
            jz, jy, jx = j // 4, j // 2 % 2, j % 2
            other = ((z + jz) % 2 * 2 + (y + jy) % 2) * 2 + (x + jx) % 2
            theirs = window_start(other * 2 + 1 - core)
            ours = window_start(other * 2 + core)

            def action(third):
                row = group_row(third, group)
                from_source(theirs + row, lambda src: pltpu.make_async_remote_copy(
                    src_ref=src, dst_ref=part.at[jz, jy, jx, pl.ds(row, GROUP), :],
                    send_sem=pair_send.at[third], recv_sem=pair_recv.at[third, group],
                    device_id=neighbour(3), device_id_type=MESH).start())
                from_source(ours + row, lambda src: pltpu.make_async_copy(
                    src, mine.at[slot, third, jz, jy, jx], mine_sem.at[slot, third]).start())
            each_third(group, [count // 2 for count in COUNTS], action)

    def hop_copy(third, item, hop, whole=False):
        rows = pl.ds(item_row(third, 0), COUNTS[third] * UNIT) if whole else pl.ds(item_row(third, item), UNIT)
        first, second, last = ORDERS[third]
        if hop == 0:
            index = tuple(1 if n == first else slice(None) for n in range(3))
            target = recv0.at[:, :, rows, :]
        elif hop == 1:
            index = tuple(0 if n == first else 1 if n == second else slice(None) for n in range(3))
            target = recv1.at[:, rows, :]
        else:
            index = tuple(1 if n == last else 0 for n in range(3))
            target = recv2.at[rows, :]
        return pltpu.make_async_remote_copy(
            src_ref=part.at[index + (rows, slice(None))], dst_ref=target,
            send_sem=send.at[third, hop], recv_sem=arrive.at[third, hop, item],
            device_id=neighbour(ORDERS[third][hop]), device_id_type=MESH)

    def pair_all(third, group, whole=False):
        rows = pl.ds(FIRSTS[third] * UNIT, COUNTS[third] * UNIT) if whole else pl.ds(group_row(third, group), GROUP)
        block = part.at[:, :, :, rows, :]
        return pltpu.make_async_remote_copy(
            src_ref=block, dst_ref=block, send_sem=pair_send.at[third], recv_sem=pair_recv.at[third, group],
            device_id=neighbour(3), device_id_type=MESH)

    def out_copy(third, item, whole=False):
        rows = pl.ds(item_row(third, 0), COUNTS[third] * UNIT) if whole else pl.ds(item_row(third, item), UNIT)
        return pltpu.make_async_copy(part.at[0, 0, 0, rows, :], out_ref.at[rows, :], out_sem.at[third])

    start_group(0, 0)

    def stage0(item, third):
        rows = pl.ds(item_row(third, item), UNIT)
        group = item // 2
        slot = group % 2

        @pl.when(item % 2 == 0)
        def _():
            pltpu.make_async_copy(mine.at[slot, third], mine.at[slot, third], mine_sem.at[slot, third]).wait()
            pair_all(third, group).wait_recv()
        within = pl.ds(pl.multiple_of(item % 2 * UNIT, UNIT), UNIT)
        for j in range(8):
            index = (j // 4, j // 2 % 2, j % 2)
            part[index + (rows, slice(None))] += mine[(slot, third) + index + (within, slice(None))]
        hop_copy(third, item, 0).start()

    def stage1(item, third):
        rows = pl.ds(item_row(third, item), UNIT)
        hop_copy(third, item, 0).wait_recv()
        first = ORDERS[third][0]
        for j in range(4):
            pair = [j // 2, j % 2]
            index = tuple(pair[:first] + [0] + pair[first:])
            part[index + (rows, slice(None))] += recv0[j // 2, j % 2, rows, :]
        hop_copy(third, item, 1).start()

    def stage2(item, third):
        rows = pl.ds(item_row(third, item), UNIT)
        hop_copy(third, item, 1).wait_recv()
        last = ORDERS[third][2]
        for j in range(2):
            index = tuple(j if n == last else 0 for n in range(3))
            part[index + (rows, slice(None))] += recv1[j, rows, :]
        hop_copy(third, item, 2).start()

    def stage3(item, third):
        rows = pl.ds(item_row(third, item), UNIT)
        hop_copy(third, item, 2).wait_recv()
        part[0, 0, 0, rows, :] = (part[0, 0, 0, rows, :] + recv2[rows, :]) / SIXTEEN

    long_chip, long_core = LONG_SLICE // 2, LONG_SLICE % 2
    lz, ly, lx = (z + long_chip // 4) % 2, (y + long_chip // 2 % 2) % 2, (x + long_chip % 2) % 2
    long_row = window_start(LONG_SLICE) + COMMON
    holder = core == long_core

    def long_pair():
        return pltpu.make_async_remote_copy(
            src_ref=long_mine, dst_ref=long_part, send_sem=long_sem.at[0], recv_sem=long_sem.at[1],
            device_id=neighbour(3), device_id_type=MESH)

    def long_load():
        return pltpu.make_async_copy(
            sources[2].at[pl.ds(pl.multiple_of(long_row - TENSORS[2][0], GROUP), GROUP), :], long_mine, long_sem.at[2])

    def long_hop(hop):
        return pltpu.make_async_remote_copy(
            src_ref=long_part, dst_ref=long_recv.at[hop], send_sem=long_sem.at[3 + hop], recv_sem=long_sem.at[6 + hop],
            device_id=neighbour((2, 0, 1)[hop]), device_id_type=MESH)

    def long_out():
        return pltpu.make_async_copy(long_part, out_ref.at[pl.ds(COMMON, GROUP), :], long_sem.at[9])

    reached = (holder, holder & (lx == 0), holder & (lx == 0) & (lz == 0), holder & (lx == 0) & (lz == 0) & (ly == 0))
    far = (lx == 1, lz == 1, ly == 1)

    def long_start():
        long_load().start()

    def long_exchange():
        long_load().wait()

        @pl.when(core != long_core)
        def _():
            long_pair().start()

    def long_sum():
        @pl.when(holder)
        def _():
            long_pair().wait_recv()
            long_part[...] += long_mine[...]

        @pl.when(core != long_core)
        def _():
            long_pair().wait_send()

    def long_send(hop):
        @pl.when(reached[hop] & far[hop])
        def _():
            long_hop(hop).start()

    def long_add(hop):
        @pl.when(reached[hop] & far[hop])
        def _():
            long_hop(hop).wait_send()

        @pl.when(reached[hop + 1])
        def _():
            long_hop(hop).wait_recv()
            if hop < 2:
                long_part[...] += long_recv[hop]
            else:
                long_part[...] = (long_part[...] + long_recv[hop]) / SIXTEEN

    def long_store():
        @pl.when(reached[3])
        def _():
            long_out().start()

    long_stages = ((4, long_start), (6, long_exchange), (8, long_sum)) + tuple(
        (9 + 3 * hop + k, functools.partial((long_send, long_add)[k // 2], hop)) for hop in range(3) for k in (0, 2)
    ) + ((19, long_store),)

    stages = ((0, stage0), (LAG, stage1), (2 * LAG, stage2), (3 * LAG, stage3),
              (3 * LAG + 1, lambda item, third: out_copy(third, item).start()))

    vec_load.wait()
    vec_rows[pl.ds(VEC_ROWS // 8 * 8, VEC_BLOCK_ROWS - VEC_ROWS // 8 * 8), :] = jnp.zeros(
        (VEC_BLOCK_ROWS - VEC_ROWS // 8 * 8, LANES), jnp.float32)
    for n in range(-(-VEC_ROWS // 8)):
        rows = min(8, VEC_ROWS - n * 8)
        vec_rows[n * 8:n * 8 + rows, :] = vec_raw[:, n * 1024:n * 1024 + rows * LANES].reshape(rows, LANES)

    @pl.loop(0, ITEMS + stages[-1][0])
    def _(step):
        for delay, stage in stages:
            @pl.when((step >= delay) & (step < ITEMS + delay))
            def _():
                each_third(step - delay, COUNTS, functools.partial(stage, step - delay))

        for at, stage in long_stages:
            @pl.when(step == at)
            def _():
                stage()

        @pl.when((step % 2 == 0) & (step + 2 < ITEMS))
        def _():
            start_group(step // 2 + 1, (step // 2 + 1) % 2)

    for third in range(3):
        pair_all(third, 0, True).wait_send()
        for hop in range(3):
            hop_copy(third, 0, hop, True).wait_send()
        out_copy(third, 0, True).wait()

    @pl.when(reached[3])
    def _():
        long_out().wait()

    for n, ref in enumerate((m_ref, v_ref, w_ref)):
        pltpu.make_async_remote_copy(
            src_ref=ref.at[pl.ds(0, EDGE)], dst_ref=edge_ref.at[pl.ds(n * EDGE, EDGE)],
            send_sem=edge_send.at[n], recv_sem=edge_recv.at[n],
            device_id=(before // 8, before // 4 % 2, before % 4), device_id_type=MESH).wait()


def scatter(grads, m, v, w):
    any_spec = pl.BlockSpec(memory_space=pl.ANY)
    dma = pltpu.SemaphoreType.DMA
    return pl.pallas_call(
        scatter_kernel,
        out_shape=(jax.ShapeDtypeStruct((WINDOW, LANES), jnp.float32), jax.ShapeDtypeStruct((3 * EDGE,), jnp.float32)),
        in_specs=[any_spec] * 8,
        out_specs=(any_spec, any_spec),
        scratch_shapes=[
            pltpu.VMEM((2, 2, 2, COMMON, LANES), jnp.float32),
            pltpu.VMEM((2, 2, COMMON, LANES), jnp.float32),
            pltpu.VMEM((2, COMMON, LANES), jnp.float32),
            pltpu.VMEM((COMMON, LANES), jnp.float32),
            pltpu.VMEM((2, 3, 2, 2, 2, GROUP, LANES), jnp.float32),
            dma((3,)), dma((3, ITEMS // 2)), dma((2, 3)),
            dma((3, 3)), dma((3, 3, ITEMS)), dma((3,)), dma((3,)), dma((3,)),
            pltpu.VMEM((GROUP, LANES), jnp.float32), pltpu.VMEM((GROUP, LANES), jnp.float32),
            pltpu.VMEM((3, GROUP, LANES), jnp.float32), dma((10,)),
            pltpu.VMEM((1, VEC_WIDTH), jnp.float32), pltpu.VMEM((VEC_BLOCK_ROWS, LANES), jnp.float32), dma(()),
        ],
        compiler_params=pltpu.CompilerParams(has_side_effects=True, collective_id=0, vmem_limit_bytes=67043328),
    )(*grads, m, v, w)


def gather_kernel(w_ref, full_ref, pair_send, pair_recv, send, arrive):
    z, y, x, core = position()
    here = (z, y, x)

    def rows_of(third, item, whole=False):
        if whole:
            return pl.ds(0, whole * OWN_CHUNK)
        main = OWN_ITEMS - 1
        row = jnp.where(item < main, third * main + item, 3 * main + third) * OWN_CHUNK
        return pl.ds(pl.multiple_of(row, OWN_CHUNK), OWN_CHUNK)

    def sent(item, side):
        return (item < OWN_ITEMS - 1) | (side == 0)

    def copy(third, item, hop, whole=False):
        rows = rows_of(third, item, whole)
        order = ORDERS[third]
        if hop == 0:
            source = w_ref.at[rows, :]
            target = full_ref.at[z, y, x, core, rows, :]
        else:
            index = tuple(slice(None) if n in order[:hop] else here[n] for n in range(3))
            source = target = full_ref.at[index + (core, rows, slice(None))]
        return pltpu.make_async_remote_copy(
            src_ref=source, dst_ref=target, send_sem=send.at[third, hop], recv_sem=arrive.at[third, item, hop],
            device_id=neighbour(order[hop]), device_id_type=MESH)

    def arrival(third, item, hop):
        order = ORDERS[third]
        index = tuple(slice(None) if n in order[:hop] else (1 - here[n] if n == order[hop] else here[n]) for n in range(3))
        block = full_ref.at[index + (core, rows_of(third, item), slice(None))]
        return pltpu.make_async_remote_copy(
            src_ref=block, dst_ref=block, send_sem=send.at[third, hop], recv_sem=arrive.at[third, item, hop],
            device_id=neighbour(order[hop]), device_id_type=MESH)

    def pair(third, item, side, whole=False):
        block = full_ref.at[:, :, :, side, rows_of(third, item, whole), :]
        return pltpu.make_async_remote_copy(
            src_ref=block, dst_ref=block, send_sem=pair_send.at[third], recv_sem=pair_recv.at[third, item],
            device_id=neighbour(3), device_id_type=MESH)

    meet([neighbour(axis) for axis in range(4)])
    for item in range(OWN_LAG):
        for third in range(3):
            copy(third, item, 0).start()

    @pl.loop(0, OWN // OWN_CHUNK)
    def _(n):
        rows = pl.ds(pl.multiple_of(n * OWN_CHUNK, OWN_CHUNK), OWN_CHUNK)
        full_ref[z, y, x, core, rows, :] = w_ref[rows, :]

    @pl.loop(0, OWN_ITEMS + 2 * OWN_LAG)
    def _(step):
        @pl.when((step + OWN_LAG < OWN_ITEMS) & sent(step + OWN_LAG, core))
        def _():
            for third in range(3):
                copy(third, step + OWN_LAG, 0).start()

        for hop in range(1, 4):
            delay = (hop - 1) * OWN_LAG

            @pl.when((step >= delay) & (step < OWN_ITEMS + delay) & sent(step - delay, core))
            def _():
                item = step - delay
                for third in range(3):
                    arrival(third, item, hop - 1).wait_recv()
                    if hop < 3:
                        copy(third, item, hop).start()
                    else:
                        pair(third, item, core).start()

    @pl.loop(0, OWN_ITEMS)
    def _(item):
        @pl.when(sent(item, 1 - core))
        def _():
            for third in range(3):
                pair(third, item, 1 - core).wait_recv()

    def drain(count):
        for third in range(3):
            pair(third, 0, core, count).wait_send()
            for hop in range(3):
                copy(third, 0, hop, count).wait_send()

    @pl.when(core == 0)
    def _():
        drain(OWN_ITEMS)

    @pl.when(core != 0)
    def _():
        drain(OWN_ITEMS - 1)


def gather(w_own):
    dma = pltpu.SemaphoreType.DMA
    return pl.pallas_call(
        gather_kernel,
        out_shape=jax.ShapeDtypeStruct((2, 2, 2, 2, OWN, LANES), jnp.bfloat16),
        in_specs=[pl.BlockSpec(memory_space=pltpu.VMEM)],
        out_specs=pl.BlockSpec(memory_space=pltpu.VMEM),
        scratch_shapes=[
            dma((3,)), dma((3, OWN_ITEMS)), dma((3, 3)), dma((3, OWN_ITEMS, 3)),
        ],
        compiler_params=pltpu.CompilerParams(has_side_effects=True, collective_id=1, vmem_limit_bytes=GATHER_LIMIT),
    )(w_own)


def device_index():
    outer, middle, inner = (lax.axis_index(name) for name in MESH_AXES)
    return (outer * 2 + middle) * 4 + inner


def for_blocks(start, length, action, tensors=TENSORS):
    for base, end, tiles in tensors:
        block = 8 * tiles
        low = (jnp.maximum(start, base) - base + block - 1) // block
        high = jnp.maximum(jnp.minimum(start + length, end) - base, 0) // block

        count = jnp.maximum(high - low, 0)
        together = 4 if tiles <= 8 else 1

        @pl.loop(0, count // together)
        def _(n):
            for k in range(together):
                action(pl.multiple_of(base + (low + n * together + k) * block - start, 8), tiles)

        if together > 1:
            @pl.loop(count // together * together, count)
            def _(n):
                action(pl.multiple_of(base + (low + n) * block - start, 8), tiles)


PAD = 8
FLAT_ROWS = WINDOW + 272
SHARD_VREGS = SLICE // 1024
TAIL_ROWS = SLICE % 1024 // LANES
TAIL_LANES = SLICE % LANES
EDGE_ROWS = EDGE // LANES
OWN_FLAT_ROWS = OWN + 512


def lane_index(rows=8):
    return lax.broadcasted_iota(jnp.int32, (rows, LANES), 1)


BATCH = 256
BATCHES = SHARD_VREGS * 8 // BATCH
CHUNK_BATCHES = 3
CHUNKS = BATCHES // CHUNK_BATCHES
CHUNK = CHUNK_BATCHES * BATCH * LANES


def mid_kernel(tile_ref, m_ref, v_ref, w_ref, edge_ref, m_out, v_out, w_out, own_ref,
               m_buf, v_buf, w_buf, flat, shifted, edged, aligned, in_sem, out_sem):
    device = device_index()
    start = window_start(device)
    arrays = ((m_ref, m_buf, m_out), (v_ref, v_buf, v_out), (w_ref, w_buf, w_out))

    def span(chunk):
        return pl.ds(chunk * CHUNK, CHUNK if chunk < CHUNKS - 1 else SLICE - chunk * CHUNK)

    def loads(chunk):
        return [pltpu.make_async_copy(ref.at[span(chunk)], buf.at[span(chunk)], in_sem.at[n, chunk])
                for n, (ref, buf, _) in enumerate(arrays)]

    def stores(chunk):
        return [pltpu.make_async_copy(buf.at[span(chunk)], out.at[span(chunk)], out_sem.at[n, chunk])
                for n, (_, buf, out) in enumerate(arrays)]

    for chunk in range(CHUNKS):
        for copy in loads(chunk):
            copy.start()

    def to_flat(row, tiles):
        for t in range(tiles):
            flat[pl.ds(row + t, 8, stride=tiles), :] = tile_ref[pl.ds(row + 8 * t, 8), :]
    for_blocks(start, WINDOW, to_flat)

    first_row = device * (SLICE // 16) // 8
    next_row = (device + 1) * (SLICE // 16) // 8
    shift = device * SLICE - first_row * LANES
    next_shift = (device + 1) * SLICE - next_row * LANES

    def mean_rows(row, amount, rows):
        here = flat[pl.ds(row, rows), :]
        below = flat[pl.ds(row + 1, rows), :]
        back = (LANES - amount) % LANES
        return jnp.where(lane_index(rows) < LANES - amount, pltpu.roll(here, back, 1), pltpu.roll(below, back, 1))

    for chunk in range(CHUNKS):
        for copy in loads(chunk):
            copy.wait()

        @pl.loop(chunk * CHUNK_BATCHES, (chunk + 1) * CHUNK_BATCHES)
        def _(n):
            at = pl.ds(pl.multiple_of(n * BATCH * LANES, BATCH * LANES), BATCH * LANES)
            mean = mean_rows(first_row - start + n * BATCH, shift, BATCH)
            new = adam_update(mean, *(buf[at].reshape(BATCH, LANES) for _, buf, _ in arrays))
            for (_, buf, _), value in zip(arrays, new):
                buf[at] = value.reshape(BATCH * LANES)
            shifted[pl.ds(pl.multiple_of(PAD + n * BATCH, 8), BATCH), :] = pltpu.roll(new[2], shift, 1)

        if chunk > 0:
            for copy in stores(chunk - 1):
                copy.start()

    mean = mean_rows(first_row - start + SHARD_VREGS * 8, shift, 8)
    for r in range(TAIL_ROWS + 1):
        size = LANES if r < TAIL_ROWS else TAIL_LANES
        at = pl.ds(SHARD_VREGS * 1024 + r * LANES, size)
        new = adam_update(mean[r:r + 1, :size], *(buf[at].reshape(1, size) for _, buf, _ in arrays))
        for (_, buf, _), value in zip(arrays, new):
            buf[at] = value.reshape(size)
        flat[pl.ds(FLAT_ROWS - 8 + r, 1), pl.ds(0, size)] = new[2]
    shifted[pl.ds(PAD + SHARD_VREGS * 8, 8), :] = pltpu.roll(flat[pl.ds(FLAT_ROWS - 8, 8), :], shift, 1)

    @pl.loop(0, EDGE_ROWS // 64)
    def _(n):
        mean = mean_rows(next_row - start + n * 64, next_shift, 64)
        old = (edge_ref[pl.ds(pl.multiple_of(k * EDGE + n * 8192, 1024), 8192)].reshape(64, LANES) for k in range(3))
        edged[pl.ds(pl.multiple_of(PAD + n * 64, 8), 64), :] = pltpu.roll(adam_update(mean, *old)[2], next_shift, 1)

    for copy in stores(CHUNKS - 1):
        copy.start()

    own = own_start(device)
    skip = own - first_row

    @pl.loop(0, BATCHES + 1)
    def _(n):
        row = PAD + skip + n * BATCH
        aligned[pl.ds(pl.multiple_of(n * BATCH, 8), BATCH), :] = jnp.where(
            lane_index(BATCH) >= shift, shifted[pl.ds(row, BATCH), :], shifted[pl.ds(row - 1, BATCH), :])
    edged[pl.ds(PAD - 1, 1), :] = aligned[pl.ds(next_row - own, 1), :]

    @pl.loop(0, EDGE_ROWS // 64)
    def _(n):
        row = PAD + n * 64
        aligned[pl.ds(next_row - own + n * 64, 64), :] = jnp.where(
            lane_index(64) >= next_shift, edged[pl.ds(row, 64), :], edged[pl.ds(row - 1, 64), :])

    def to_tile(row, tiles):
        for t in range(0, tiles, 2):
            both = [aligned[pl.ds(row + t + k, 8, stride=tiles), :] for k in range(2)]
            own_ref[pl.ds(pl.multiple_of(row + 8 * t, 16), 16), :] = jnp.concatenate(both, axis=0).astype(jnp.bfloat16)

    def plain(row, _):
        own_ref[pl.ds(pl.multiple_of(row, 16), 16), :] = aligned[pl.ds(row, 16), :].astype(jnp.bfloat16)
    for_blocks(own, OWN, to_tile, TENSORS[:4])
    for_blocks(own, OWN, plain, ((*TENSORS[4][:2], 2),))

    for chunk in range(CHUNKS):
        for copy in stores(chunk):
            copy.wait()


def mid(mean_tiles, m, v, w, edges):
    vmem = pl.BlockSpec(memory_space=pltpu.VMEM)
    any_spec = pl.BlockSpec(memory_space=pl.ANY)
    shard = jax.ShapeDtypeStruct((SLICE,), jnp.float32)
    return pl.pallas_call(
        mid_kernel,
        out_shape=(shard, shard, shard, jax.ShapeDtypeStruct((OWN, LANES), jnp.bfloat16)),
        in_specs=[vmem, any_spec, any_spec, any_spec, vmem], out_specs=(any_spec, any_spec, any_spec, vmem),
        scratch_shapes=[
            pltpu.VMEM((SLICE,), jnp.float32), pltpu.VMEM((SLICE,), jnp.float32), pltpu.VMEM((SLICE,), jnp.float32),
            pltpu.VMEM((FLAT_ROWS, LANES), jnp.float32),
            pltpu.VMEM((PAD + SHARD_VREGS * 8 + 8 + 512, LANES), jnp.float32),
            pltpu.VMEM((PAD + EDGE_ROWS, LANES), jnp.float32),
            pltpu.VMEM((OWN_FLAT_ROWS, LANES), jnp.float32),
            pltpu.SemaphoreType.DMA((3, CHUNKS)), pltpu.SemaphoreType.DMA((3, CHUNKS)),
        ],
        compiler_params=pltpu.CompilerParams(vmem_limit_bytes=MID_LIMIT),
    )(mean_tiles, m, v, w, edges)


def pieces_of(tensor):
    base, end, _ = TENSORS[tensor]
    for d in range(SIXTEEN):
        low, high = max(OWN_STARTS[d], base), min(OWN_STARTS[d + 1], end)
        if low < high:
            yield d, low - OWN_STARTS[d], low - base, high - low


PIECES = [(tensor,) + piece for tensor in range(4) for piece in pieces_of(tensor)]
VEC_WIDTH = 12032
VEC_ROWS = VEC_WIDTH // LANES
VEC_BLOCK = VEC_WIDTH // 8
CHIP_COUNTS = tuple((end - base) // 8 for base, end, _ in TENSORS[:4])
CHIP_ROWS = sum(CHIP_COUNTS)
CHIP_SIZE = CHIP_ROWS * LANES + VEC_BLOCK
CHIP_PARTS = 6
CHIP_PART = CHIP_SIZE // 16384 // CHIP_PARTS * 16384


def final_kernel(full_ref, e_out, a_out, f_out, h_out, vec_out, chip_ref, chip_out, flat, vec, out_sem, chip_sem):
    outs = (e_out, a_out, f_out, h_out)
    chip = device_index() // 2
    copies = []
    for n, (tensor, d, source, target, rows) in enumerate(PIECES):
        copies.append(pltpu.make_async_copy(
            full_ref.at[d, pl.ds(source, rows), :], outs[tensor].at[pl.ds(target, rows), :], out_sem.at[n]))
        copies[-1].start()

    slot, source, _, _ = next(pieces_of(4))
    vec[pl.ds(0, 96), :] = full_ref[slot, pl.ds(source, 96), :].astype(jnp.float32)
    for n in range(VEC_ROWS // 8):
        vec_out[:, n * 1024:(n + 1) * 1024] = vec[n * 8:n * 8 + 8, :].reshape(1, 1024).astype(jnp.bfloat16)
    rest = VEC_ROWS % 8
    vec_out[:, VEC_ROWS // 8 * 1024:] = vec[pl.ds(VEC_ROWS - rest, rest), :].reshape(1, rest * LANES).astype(jnp.bfloat16)

    offset = 0
    for tensor, rows in enumerate(CHIP_COUNTS):
        base, _, tiles = TENSORS[tensor]
        step = 16 * tiles

        begin = base + chip * rows
        slot, low, bound = jnp.int32(0), jnp.int32(0), jnp.int32(OWN_STARTS[1])
        for d in range(1, SIXTEEN):
            inside = begin >= OWN_STARTS[d]
            slot = jnp.where(inside, d, slot)
            low = jnp.where(inside, OWN_STARTS[d], low)
            bound = jnp.where(inside, OWN_STARTS[d + 1], bound)

        @pl.loop(0, rows // step)
        def _(n):
            for half in range(2):
                row = begin + n * step + half * 8 * tiles
                following = row >= bound
                at_slot = jnp.where(following, slot + 1, slot)
                at_row = row - jnp.where(following, bound, low)
                for t in range(0, tiles, 2):
                    value = full_ref[at_slot, pl.ds(pl.multiple_of(at_row + 8 * t, 16), 16), :].astype(jnp.float32)
                    for k in range(2):
                        to = offset + n * step + half * 8 * tiles + t + k
                        flat[pl.ds(to, 8, stride=tiles), :] = value[8 * k:8 * k + 8]
        offset += rows

    vec_row = chip * (VEC_BLOCK // 32) // 4
    amount = chip * VEC_BLOCK - vec_row * LANES
    back = (LANES - amount) % LANES
    lane = lane_index()
    for n in range(2):
        here, below = vec[pl.ds(vec_row + n * 8, 8), :], vec[pl.ds(vec_row + n * 8 + 1, 8), :]
        flat[pl.ds(CHIP_ROWS + n * 8, 8), :] = jnp.where(
            lane < LANES - amount, pltpu.roll(here, back, 1), pltpu.roll(below, back, 1))

    def part_copy(part):
        span = pl.ds(part * CHIP_PART, CHIP_PART if part < CHIP_PARTS - 1 else CHIP_SIZE - part * CHIP_PART)
        return pltpu.make_async_copy(chip_out.at[:, span], chip_ref.at[:, span], chip_sem.at[part])

    for part in range(CHIP_PARTS):
        @pl.loop(part * CHIP_PART // 16384, (part + 1) * CHIP_PART // 16384)
        def _(n):
            chip_out[:, pl.ds(pl.multiple_of(n * 16384, 16384), 16384)] = flat[
                pl.ds(pl.multiple_of(n * 128, 128), 128), :].reshape(1, 16384).astype(jnp.bfloat16)
        if part > 0:
            part_copy(part - 1).start()
    done = CHIP_SIZE // 1024 * 1024
    rows = (CHIP_SIZE - done) // LANES
    last = CHIP_SIZE - done - rows * LANES
    first = done // LANES
    chip_out[:, CHIP_PARTS * CHIP_PART:done] = flat[CHIP_PARTS * CHIP_PART // LANES:first, :].reshape(
        1, done - CHIP_PARTS * CHIP_PART).astype(jnp.bfloat16)
    chip_out[:, done:done + rows * LANES] = flat[first:first + rows, :].reshape(1, rows * LANES).astype(jnp.bfloat16)
    chip_out[:, CHIP_SIZE - last:] = flat[first + rows:first + rows + 1, :last].astype(jnp.bfloat16)
    part_copy(CHIP_PARTS - 1).start()
    for part in range(CHIP_PARTS):
        part_copy(part).wait()
    for copy in copies:
        copy.wait()


def finish(full):
    vmem = pl.BlockSpec(memory_space=pltpu.VMEM)
    any_spec = pl.BlockSpec(memory_space=pl.ANY)
    shape = lambda rows: jax.ShapeDtypeStruct((rows, LANES), jnp.bfloat16)
    return pl.pallas_call(
        final_kernel,
        out_shape=tuple(shape(end - base) for base, end, _ in TENSORS[:4]) + (
            jax.ShapeDtypeStruct((1, VEC_WIDTH), jnp.bfloat16), jax.ShapeDtypeStruct((1, CHIP_SIZE), jnp.bfloat16)),
        in_specs=[vmem], out_specs=(any_spec,) * 4 + (vmem, any_spec),
        scratch_shapes=[
            pltpu.VMEM((1, CHIP_SIZE), jnp.bfloat16),
            pltpu.VMEM((CHIP_ROWS + 16, LANES), jnp.float32),
            pltpu.VMEM((120, LANES), jnp.float32),
            pltpu.SemaphoreType.DMA((len(PIECES),)), pltpu.SemaphoreType.DMA((CHIP_PARTS,)),
        ],
        compiler_params=pltpu.CompilerParams(vmem_limit_bytes=FINAL_LIMIT),
    )(full)


def solution(mesh):
    def local_step(g_embed, g_attn, g_ffn_in, g_ffn_out, g_vec, m_shard, v_shard, w_shard):
        matrices = (g_embed, g_attn, g_ffn_in, g_ffn_out)
        grads = [to_tiles(g[0] if g.ndim == 3 else g[0, 0]) for g in matrices]
        grads.append(g_vec.reshape(1, -1))
        mean_tiles, edges = scatter(grads, m_shard, v_shard, w_shard)
        m_new, v_new, w_new, w_own = mid(mean_tiles, m_shard, v_shard, w_shard, edges)
        full = gather(w_own).reshape(SIXTEEN, OWN, LANES)
        *tiles, vec, w_chip = finish(full)
        tensors = [from_tiles(t, g.shape[-1]).reshape(g.shape[1:]) for t, g in zip(tiles, matrices)]
        return (m_new, v_new, w_new) + tuple(tensors) + (vec, w_chip)

    return jax.shard_map(local_step, mesh=mesh, in_specs=(P(MESH_AXES),) * 8, out_specs=(P(MESH_AXES),) * 3 + (P(),) * 5 + (P(MESH_AXES),), check_vma=False)
```

```python
import functools
import math
import jax
import jax.numpy as jnp
from jax import lax
from jax.experimental import pallas as pl
from jax.experimental.pallas import tpu as pltpu
from jax.sharding import PartitionSpec as P

MESH_AXES = ('outer', 'middle', 'inner')
MESH = pl.DeviceIdType.MESH
ADAM_BETA1 = 0.9
ADAM_BETA2 = 0.98
ADAM_EPS = 1e-9
LEARN_RATE = 0.05
ADAM_STEP = 3

LANES = 128
SLICE = 885488
TENSORS = ((0, 32768, 8), (32768, 65536, 32), (65536, 88064, 22), (88064, 110592, 8), (110592, 110720, 1))
ROWS = 110720
VEC_BLOCK_ROWS = 128
UNIT = 64
GROUP = 128
COMMON = 7168
WINDOW = COMMON + GROUP
LONG_SLICE = 10
COUNTS = (38, 38, 36)
FIRSTS = (0, 38, 76)
ITEMS = max(COUNTS)
LAG = 2
EDGE = 32768
OWN = 7104
OWN_THIRD = OWN // 3
OWN_CHUNK = 64
OWN_ITEMS = OWN_THIRD // OWN_CHUNK
OWN_LAG = 2
SIXTEEN = 16
FINAL_LIMIT = 20000000
GATHER_LIMIT = 6000000
MID_LIMIT = 52000000


def floor_block(row):
    result = row
    for base, end, tiles in TENSORS:
        block = 8 * tiles if tiles > 1 else VEC_BLOCK_ROWS
        floored = base + (row - base) // block * block
        result = jnp.where((row >= base) & (row < end), floored, result)
    return result


def window_start(index):
    row = floor_block(index * (SLICE // 16) // 8)
    return jnp.minimum(row // GROUP * GROUP, ROWS - COMMON)


def own_start_static(index):
    row = -(-index * SLICE // LANES)
    for base, end, tiles in TENSORS:
        if base <= row < end:
            block = 8 * tiles if tiles > 1 else VEC_BLOCK_ROWS
            return base + -(-(row - base) // block) * block
    return ROWS


OWN_STARTS = [own_start_static(d) for d in range(SIXTEEN)] + [ROWS]


def own_start(index):
    result = jnp.int32(0)
    for d in range(SIXTEEN):
        result = jnp.where(index == d, OWN_STARTS[d], result)
    return result


def adam_update(grad_mean, m_old, v_old, w_old):
    m_new = ADAM_BETA1 * m_old + (1.0 - ADAM_BETA1) * grad_mean
    v_new = ADAM_BETA2 * v_old + (1.0 - ADAM_BETA2) * (grad_mean * grad_mean)
    scale = LEARN_RATE / (1.0 - ADAM_BETA1 ** ADAM_STEP)
    w_new = w_old - scale * m_new / (jnp.sqrt(v_new * (1.0 / (1.0 - ADAM_BETA2 ** ADAM_STEP))) + ADAM_EPS)
    return m_new, v_new, w_new


def to_tiles(tensor):
    rows, width = tensor.shape
    return tensor.reshape(rows // 8, 8, width // LANES, LANES).transpose(0, 2, 1, 3).reshape(-1, LANES)


def from_tiles(tiles, width):
    return tiles.reshape(-1, width // LANES, 8, LANES).transpose(0, 2, 1, 3).reshape(-1, width)


ORDERS = ((0, 1, 2), (1, 2, 0), (2, 0, 1))


def position():
    outer, middle, inner = (lax.axis_index(name) for name in MESH_AXES)
    return outer, middle, inner // 2, inner % 2


def neighbour(axis):
    outer, middle, x, core = position()
    z, y = outer, middle
    if axis == 0:
        z = 1 - z
    elif axis == 1:
        y = 1 - y
    elif axis == 2:
        x = 1 - x
    else:
        core = 1 - core
    return (z, y, 2 * x + core)


def meet(devices):
    barrier = pltpu.get_barrier_semaphore()
    for device in devices:
        pl.semaphore_signal(barrier, inc=1, device_id=device, device_id_type=MESH)
    pl.semaphore_wait(barrier, len(devices))


def scatter_kernel(e_ref, a_ref, f_ref, h_ref, b_ref, m_ref, v_ref, w_ref, out_ref, edge_ref,
                   part, recv0, recv1, recv2, mine, pair_send, pair_recv, mine_sem,
                   send, arrive, out_sem, edge_send, edge_recv, long_mine, long_part, long_recv, long_sem, vec_raw, vec_rows, vec_sem):
    z, y, x, core = position()
    chip = (z * 2 + y) * 2 + x
    device = chip * 2 + core
    sources = (e_ref, a_ref, f_ref, h_ref, vec_rows)
    vec_load = pltpu.make_async_copy(b_ref, vec_raw, vec_sem)
    vec_load.start()

    before = (device + SIXTEEN - 1) % SIXTEEN
    after = (device + 1) % SIXTEEN
    meet([neighbour(axis) for axis in range(4)] + [(d // 8, d // 4 % 2, d % 4) for d in (before, after)])
    for n, ref in enumerate((m_ref, v_ref, w_ref)):
        pltpu.make_async_remote_copy(
            src_ref=ref.at[pl.ds(0, EDGE)], dst_ref=edge_ref.at[pl.ds(n * EDGE, EDGE)],
            send_sem=edge_send.at[n], recv_sem=edge_recv.at[n],
            device_id=(before // 8, before // 4 % 2, before % 4), device_id_type=MESH).start()

    def from_source(row, action):
        def choose(low, high):
            if high - low == 1:
                action(sources[low].at[pl.ds(pl.multiple_of(row - TENSORS[low][0], GROUP), GROUP), :])
                return
            middle = (low + high) // 2
            lax.cond(row < TENSORS[middle][0], lambda: choose(low, middle), lambda: choose(middle, high))
        choose(0, len(sources))

    def item_row(third, item):
        return pl.multiple_of((FIRSTS[third] + item) * UNIT, UNIT)

    def each_third(index, counts, action):
        for third in range(3):
            if counts[third] == max(counts):
                action(third)
            else:
                @pl.when(index < counts[third])
                def _():
                    action(third)

    def group_row(third, group):
        return pl.multiple_of(FIRSTS[third] * UNIT + group * GROUP, GROUP)

    def start_group(group, slot):
        @pl.loop(0, 8)
        def _(j):
            jz, jy, jx = j // 4, j // 2 % 2, j % 2
            other = ((z + jz) % 2 * 2 + (y + jy) % 2) * 2 + (x + jx) % 2
            theirs = window_start(other * 2 + 1 - core)
            ours = window_start(other * 2 + core)

            def action(third):
                row = group_row(third, group)
                from_source(theirs + row, lambda src: pltpu.make_async_remote_copy(
                    src_ref=src, dst_ref=part.at[jz, jy, jx, pl.ds(row, GROUP), :],
                    send_sem=pair_send.at[third], recv_sem=pair_recv.at[third, group],
                    device_id=neighbour(3), device_id_type=MESH).start())
                from_source(ours + row, lambda src: pltpu.make_async_copy(
                    src, mine.at[slot, third, jz, jy, jx], mine_sem.at[slot, third]).start())
            each_third(group, [count // 2 for count in COUNTS], action)

    def hop_copy(third, item, hop, whole=False):
        rows = pl.ds(item_row(third, 0), COUNTS[third] * UNIT) if whole else pl.ds(item_row(third, item), UNIT)
        first, second, last = ORDERS[third]
        if hop == 0:
            index = tuple(1 if n == first else slice(None) for n in range(3))
            target = recv0.at[:, :, rows, :]
        elif hop == 1:
            index = tuple(0 if n == first else 1 if n == second else slice(None) for n in range(3))
            target = recv1.at[:, rows, :]
        else:
            index = tuple(1 if n == last else 0 for n in range(3))
            target = recv2.at[rows, :]
        return pltpu.make_async_remote_copy(
            src_ref=part.at[index + (rows, slice(None))], dst_ref=target,
            send_sem=send.at[third, hop], recv_sem=arrive.at[third, hop, item],
            device_id=neighbour(ORDERS[third][hop]), device_id_type=MESH)

    def pair_all(third, group, whole=False):
        rows = pl.ds(FIRSTS[third] * UNIT, COUNTS[third] * UNIT) if whole else pl.ds(group_row(third, group), GROUP)
        block = part.at[:, :, :, rows, :]
        return pltpu.make_async_remote_copy(
            src_ref=block, dst_ref=block, send_sem=pair_send.at[third], recv_sem=pair_recv.at[third, group],
            device_id=neighbour(3), device_id_type=MESH)

    def out_copy(third, item, whole=False):
        rows = pl.ds(item_row(third, 0), COUNTS[third] * UNIT) if whole else pl.ds(item_row(third, item), UNIT)
        return pltpu.make_async_copy(part.at[0, 0, 0, rows, :], out_ref.at[rows, :], out_sem.at[third])

    start_group(0, 0)

    def stage0(item, third):
        rows = pl.ds(item_row(third, item), UNIT)
        group = item // 2
        slot = group % 2

        @pl.when(item % 2 == 0)
        def _():
            pltpu.make_async_copy(mine.at[slot, third], mine.at[slot, third], mine_sem.at[slot, third]).wait()
            pair_all(third, group).wait_recv()
        within = pl.ds(pl.multiple_of(item % 2 * UNIT, UNIT), UNIT)
        for j in range(8):
            index = (j // 4, j // 2 % 2, j % 2)
            part[index + (rows, slice(None))] += mine[(slot, third) + index + (within, slice(None))]
        hop_copy(third, item, 0).start()

    def stage1(item, third):
        rows = pl.ds(item_row(third, item), UNIT)
        hop_copy(third, item, 0).wait_recv()
        first = ORDERS[third][0]
        for j in range(4):
            pair = [j // 2, j % 2]
            index = tuple(pair[:first] + [0] + pair[first:])
            part[index + (rows, slice(None))] += recv0[j // 2, j % 2, rows, :]
        hop_copy(third, item, 1).start()

    def stage2(item, third):
        rows = pl.ds(item_row(third, item), UNIT)
        hop_copy(third, item, 1).wait_recv()
        last = ORDERS[third][2]
        for j in range(2):
            index = tuple(j if n == last else 0 for n in range(3))
            part[index + (rows, slice(None))] += recv1[j, rows, :]
        hop_copy(third, item, 2).start()

    def stage3(item, third):
        rows = pl.ds(item_row(third, item), UNIT)
        hop_copy(third, item, 2).wait_recv()
        part[0, 0, 0, rows, :] = (part[0, 0, 0, rows, :] + recv2[rows, :]) / SIXTEEN

    long_chip, long_core = LONG_SLICE // 2, LONG_SLICE % 2
    lz, ly, lx = (z + long_chip // 4) % 2, (y + long_chip // 2 % 2) % 2, (x + long_chip % 2) % 2
    long_row = window_start(LONG_SLICE) + COMMON
    holder = core == long_core

    def long_pair():
        return pltpu.make_async_remote_copy(
            src_ref=long_mine, dst_ref=long_part, send_sem=long_sem.at[0], recv_sem=long_sem.at[1],
            device_id=neighbour(3), device_id_type=MESH)

    def long_load():
        return pltpu.make_async_copy(
            sources[2].at[pl.ds(pl.multiple_of(long_row - TENSORS[2][0], GROUP), GROUP), :], long_mine, long_sem.at[2])

    def long_hop(hop):
        return pltpu.make_async_remote_copy(
            src_ref=long_part, dst_ref=long_recv.at[hop], send_sem=long_sem.at[3 + hop], recv_sem=long_sem.at[6 + hop],
            device_id=neighbour((2, 0, 1)[hop]), device_id_type=MESH)

    def long_out():
        return pltpu.make_async_copy(long_part, out_ref.at[pl.ds(COMMON, GROUP), :], long_sem.at[9])

    reached = (holder, holder & (lx == 0), holder & (lx == 0) & (lz == 0), holder & (lx == 0) & (lz == 0) & (ly == 0))
    far = (lx == 1, lz == 1, ly == 1)

    def long_start():
        long_load().start()

    def long_exchange():
        long_load().wait()

        @pl.when(core != long_core)
        def _():
            long_pair().start()

    def long_sum():
        @pl.when(holder)
        def _():
            long_pair().wait_recv()
            long_part[...] += long_mine[...]

        @pl.when(core != long_core)
        def _():
            long_pair().wait_send()

    def long_send(hop):
        @pl.when(reached[hop] & far[hop])
        def _():
            long_hop(hop).start()

    def long_add(hop):
        @pl.when(reached[hop] & far[hop])
        def _():
            long_hop(hop).wait_send()

        @pl.when(reached[hop + 1])
        def _():
            long_hop(hop).wait_recv()
            if hop < 2:
                long_part[...] += long_recv[hop]
            else:
                long_part[...] = (long_part[...] + long_recv[hop]) / SIXTEEN

    def long_store():
        @pl.when(reached[3])
        def _():
            long_out().start()

    long_stages = ((4, long_start), (6, long_exchange), (8, long_sum)) + tuple(
        (9 + 3 * hop + k, functools.partial((long_send, long_add)[k // 2], hop)) for hop in range(3) for k in (0, 2)
    ) + ((19, long_store),)

    stages = ((0, stage0), (LAG, stage1), (2 * LAG, stage2), (3 * LAG, stage3),
              (3 * LAG + 1, lambda item, third: out_copy(third, item).start()))

    vec_load.wait()
    vec_rows[pl.ds(VEC_ROWS // 8 * 8, VEC_BLOCK_ROWS - VEC_ROWS // 8 * 8), :] = jnp.zeros(
        (VEC_BLOCK_ROWS - VEC_ROWS // 8 * 8, LANES), jnp.float32)
    for n in range(-(-VEC_ROWS // 8)):
        rows = min(8, VEC_ROWS - n * 8)
        vec_rows[n * 8:n * 8 + rows, :] = vec_raw[:, n * 1024:n * 1024 + rows * LANES].reshape(rows, LANES)

    @pl.loop(0, ITEMS + stages[-1][0])
    def _(step):
        for delay, stage in stages:
            @pl.when((step >= delay) & (step < ITEMS + delay))
            def _():
                each_third(step - delay, COUNTS, functools.partial(stage, step - delay))

        for at, stage in long_stages:
            @pl.when(step == at)
            def _():
                stage()

        @pl.when((step % 2 == 0) & (step + 2 < ITEMS))
        def _():
            start_group(step // 2 + 1, (step // 2 + 1) % 2)

    for third in range(3):
        pair_all(third, 0, True).wait_send()
        for hop in range(3):
            hop_copy(third, 0, hop, True).wait_send()
        out_copy(third, 0, True).wait()

    @pl.when(reached[3])
    def _():
        long_out().wait()

    for n, ref in enumerate((m_ref, v_ref, w_ref)):
        pltpu.make_async_remote_copy(
            src_ref=ref.at[pl.ds(0, EDGE)], dst_ref=edge_ref.at[pl.ds(n * EDGE, EDGE)],
            send_sem=edge_send.at[n], recv_sem=edge_recv.at[n],
            device_id=(before // 8, before // 4 % 2, before % 4), device_id_type=MESH).wait()


def scatter(grads, m, v, w):
    any_spec = pl.BlockSpec(memory_space=pl.ANY)
    dma = pltpu.SemaphoreType.DMA
    return pl.pallas_call(
        scatter_kernel,
        out_shape=(jax.ShapeDtypeStruct((WINDOW, LANES), jnp.float32), jax.ShapeDtypeStruct((3 * EDGE,), jnp.float32)),
        in_specs=[any_spec] * 8,
        out_specs=(any_spec, any_spec),
        scratch_shapes=[
            pltpu.VMEM((2, 2, 2, COMMON, LANES), jnp.float32),
            pltpu.VMEM((2, 2, COMMON, LANES), jnp.float32),
            pltpu.VMEM((2, COMMON, LANES), jnp.float32),
            pltpu.VMEM((COMMON, LANES), jnp.float32),
            pltpu.VMEM((2, 3, 2, 2, 2, GROUP, LANES), jnp.float32),
            dma((3,)), dma((3, ITEMS // 2)), dma((2, 3)),
            dma((3, 3)), dma((3, 3, ITEMS)), dma((3,)), dma((3,)), dma((3,)),
            pltpu.VMEM((GROUP, LANES), jnp.float32), pltpu.VMEM((GROUP, LANES), jnp.float32),
            pltpu.VMEM((3, GROUP, LANES), jnp.float32), dma((10,)),
            pltpu.VMEM((1, VEC_WIDTH), jnp.float32), pltpu.VMEM((VEC_BLOCK_ROWS, LANES), jnp.float32), dma(()),
        ],
        compiler_params=pltpu.CompilerParams(has_side_effects=True, collective_id=0, vmem_limit_bytes=67043328),
    )(*grads, m, v, w)


def gather_kernel(w_ref, full_ref, pair_send, pair_recv, send, arrive):
    z, y, x, core = position()
    here = (z, y, x)

    def rows_of(third, item, whole=False):
        if whole:
            return pl.ds(0, whole * OWN_CHUNK)
        main = OWN_ITEMS - 1
        row = jnp.where(item < main, third * main + item, 3 * main + third) * OWN_CHUNK
        return pl.ds(pl.multiple_of(row, OWN_CHUNK), OWN_CHUNK)

    def sent(item, side):
        return (item < OWN_ITEMS - 1) | (side == 0)

    def copy(third, item, hop, whole=False):
        rows = rows_of(third, item, whole)
        order = ORDERS[third]
        if hop == 0:
            source = w_ref.at[rows, :]
            target = full_ref.at[z, y, x, core, rows, :]
        else:
            index = tuple(slice(None) if n in order[:hop] else here[n] for n in range(3))
            source = target = full_ref.at[index + (core, rows, slice(None))]
        return pltpu.make_async_remote_copy(
            src_ref=source, dst_ref=target, send_sem=send.at[third, hop], recv_sem=arrive.at[third, item, hop],
            device_id=neighbour(order[hop]), device_id_type=MESH)

    def arrival(third, item, hop):
        order = ORDERS[third]
        index = tuple(slice(None) if n in order[:hop] else (1 - here[n] if n == order[hop] else here[n]) for n in range(3))
        block = full_ref.at[index + (core, rows_of(third, item), slice(None))]
        return pltpu.make_async_remote_copy(
            src_ref=block, dst_ref=block, send_sem=send.at[third, hop], recv_sem=arrive.at[third, item, hop],
            device_id=neighbour(order[hop]), device_id_type=MESH)

    def pair(third, item, side, whole=False):
        block = full_ref.at[:, :, :, side, rows_of(third, item, whole), :]
        return pltpu.make_async_remote_copy(
            src_ref=block, dst_ref=block, send_sem=pair_send.at[third], recv_sem=pair_recv.at[third, item],
            device_id=neighbour(3), device_id_type=MESH)

    meet([neighbour(axis) for axis in range(4)])
    for item in range(OWN_LAG):
        for third in range(3):
            copy(third, item, 0).start()

    @pl.loop(0, OWN // OWN_CHUNK)
    def _(n):
        rows = pl.ds(pl.multiple_of(n * OWN_CHUNK, OWN_CHUNK), OWN_CHUNK)
        full_ref[z, y, x, core, rows, :] = w_ref[rows, :]

    @pl.loop(0, OWN_ITEMS + 2 * OWN_LAG)
    def _(step):
        @pl.when((step + OWN_LAG < OWN_ITEMS) & sent(step + OWN_LAG, core))
        def _():
            for third in range(3):
                copy(third, step + OWN_LAG, 0).start()

        for hop in range(1, 4):
            delay = (hop - 1) * OWN_LAG

            @pl.when((step >= delay) & (step < OWN_ITEMS + delay) & sent(step - delay, core))
            def _():
                item = step - delay
                for third in range(3):
                    arrival(third, item, hop - 1).wait_recv()
                    if hop < 3:
                        copy(third, item, hop).start()
                    else:
                        pair(third, item, core).start()

    @pl.loop(0, OWN_ITEMS)
    def _(item):
        @pl.when(sent(item, 1 - core))
        def _():
            for third in range(3):
                pair(third, item, 1 - core).wait_recv()

    def drain(count):
        for third in range(3):
            pair(third, 0, core, count).wait_send()
            for hop in range(3):
                copy(third, 0, hop, count).wait_send()

    @pl.when(core == 0)
    def _():
        drain(OWN_ITEMS)

    @pl.when(core != 0)
    def _():
        drain(OWN_ITEMS - 1)


def gather(w_own):
    dma = pltpu.SemaphoreType.DMA
    return pl.pallas_call(
        gather_kernel,
        out_shape=jax.ShapeDtypeStruct((2, 2, 2, 2, OWN, LANES), jnp.bfloat16),
        in_specs=[pl.BlockSpec(memory_space=pltpu.VMEM)],
        out_specs=pl.BlockSpec(memory_space=pltpu.VMEM),
        scratch_shapes=[
            dma((3,)), dma((3, OWN_ITEMS)), dma((3, 3)), dma((3, OWN_ITEMS, 3)),
        ],
        compiler_params=pltpu.CompilerParams(has_side_effects=True, collective_id=1, vmem_limit_bytes=GATHER_LIMIT),
    )(w_own)


def device_index():
    outer, middle, inner = (lax.axis_index(name) for name in MESH_AXES)
    return (outer * 2 + middle) * 4 + inner


def for_blocks(start, length, action, tensors=TENSORS):
    for base, end, tiles in tensors:
        block = 8 * tiles
        low = (jnp.maximum(start, base) - base + block - 1) // block
        high = jnp.maximum(jnp.minimum(start + length, end) - base, 0) // block

        count = jnp.maximum(high - low, 0)
        together = 4 if tiles <= 8 else 1

        @pl.loop(0, count // together)
        def _(n):
            for k in range(together):
                action(pl.multiple_of(base + (low + n * together + k) * block - start, 8), tiles)

        if together > 1:
            @pl.loop(count // together * together, count)
            def _(n):
                action(pl.multiple_of(base + (low + n) * block - start, 8), tiles)


PAD = 8
FLAT_ROWS = WINDOW + 272
SHARD_VREGS = SLICE // 1024
TAIL_ROWS = SLICE % 1024 // LANES
TAIL_LANES = SLICE % LANES
EDGE_ROWS = EDGE // LANES
OWN_FLAT_ROWS = OWN + 512


def lane_index(rows=8):
    return lax.broadcasted_iota(jnp.int32, (rows, LANES), 1)


BATCH = 384
BATCHES = SHARD_VREGS * 8 // BATCH
CHUNK_BATCHES = 2
CHUNKS = BATCHES // CHUNK_BATCHES
CHUNK = CHUNK_BATCHES * BATCH * LANES


def mid_kernel(tile_ref, m_ref, v_ref, w_ref, edge_ref, m_out, v_out, w_out, own_ref,
               m_buf, v_buf, w_buf, flat, shifted, edged, aligned, in_sem, out_sem):
    device = device_index()
    start = window_start(device)
    arrays = ((m_ref, m_buf, m_out), (v_ref, v_buf, v_out), (w_ref, w_buf, w_out))

    def span(chunk):
        return pl.ds(chunk * CHUNK, CHUNK if chunk < CHUNKS - 1 else SLICE - chunk * CHUNK)

    def loads(chunk):
        return [pltpu.make_async_copy(ref.at[span(chunk)], buf.at[span(chunk)], in_sem.at[n, chunk])
                for n, (ref, buf, _) in enumerate(arrays)]

    def stores(chunk):
        return [pltpu.make_async_copy(buf.at[span(chunk)], out.at[span(chunk)], out_sem.at[n, chunk])
                for n, (_, buf, out) in enumerate(arrays)]

    for chunk in range(CHUNKS):
        for copy in loads(chunk):
            copy.start()

    def to_flat(row, tiles):
        for t in range(tiles):
            flat[pl.ds(row + t, 8, stride=tiles), :] = tile_ref[pl.ds(row + 8 * t, 8), :]
    for_blocks(start, WINDOW, to_flat)

    first_row = device * (SLICE // 16) // 8
    next_row = (device + 1) * (SLICE // 16) // 8
    shift = device * SLICE - first_row * LANES
    next_shift = (device + 1) * SLICE - next_row * LANES

    def mean_rows(row, amount, rows):
        here = flat[pl.ds(row, rows), :]
        below = flat[pl.ds(row + 1, rows), :]
        back = (LANES - amount) % LANES
        return jnp.where(lane_index(rows) < LANES - amount, pltpu.roll(here, back, 1), pltpu.roll(below, back, 1))

    for chunk in range(CHUNKS):
        for copy in loads(chunk):
            copy.wait()

        @pl.loop(chunk * CHUNK_BATCHES, (chunk + 1) * CHUNK_BATCHES)
        def _(n):
            at = pl.ds(pl.multiple_of(n * BATCH * LANES, BATCH * LANES), BATCH * LANES)
            mean = mean_rows(first_row - start + n * BATCH, shift, BATCH)
            new = adam_update(mean, *(buf[at].reshape(BATCH, LANES) for _, buf, _ in arrays))
            for (_, buf, _), value in zip(arrays, new):
                buf[at] = value.reshape(BATCH * LANES)
            shifted[pl.ds(pl.multiple_of(PAD + n * BATCH, 8), BATCH), :] = pltpu.roll(new[2], shift, 1)

        if chunk > 0:
            for copy in stores(chunk - 1):
                copy.start()

    mean = mean_rows(first_row - start + SHARD_VREGS * 8, shift, 8)
    for r in range(TAIL_ROWS + 1):
        size = LANES if r < TAIL_ROWS else TAIL_LANES
        at = pl.ds(SHARD_VREGS * 1024 + r * LANES, size)
        new = adam_update(mean[r:r + 1, :size], *(buf[at].reshape(1, size) for _, buf, _ in arrays))
        for (_, buf, _), value in zip(arrays, new):
            buf[at] = value.reshape(size)
        flat[pl.ds(FLAT_ROWS - 8 + r, 1), pl.ds(0, size)] = new[2]
    shifted[pl.ds(PAD + SHARD_VREGS * 8, 8), :] = pltpu.roll(flat[pl.ds(FLAT_ROWS - 8, 8), :], shift, 1)

    @pl.loop(0, EDGE_ROWS // 64)
    def _(n):
        mean = mean_rows(next_row - start + n * 64, next_shift, 64)
        old = (edge_ref[pl.ds(pl.multiple_of(k * EDGE + n * 8192, 1024), 8192)].reshape(64, LANES) for k in range(3))
        edged[pl.ds(pl.multiple_of(PAD + n * 64, 8), 64), :] = pltpu.roll(adam_update(mean, *old)[2], next_shift, 1)

    for copy in stores(CHUNKS - 1):
        copy.start()

    own = own_start(device)
    skip = own - first_row

    @pl.loop(0, BATCHES + 1)
    def _(n):
        row = PAD + skip + n * BATCH
        aligned[pl.ds(pl.multiple_of(n * BATCH, 8), BATCH), :] = jnp.where(
            lane_index(BATCH) >= shift, shifted[pl.ds(row, BATCH), :], shifted[pl.ds(row - 1, BATCH), :])
    edged[pl.ds(PAD - 1, 1), :] = aligned[pl.ds(next_row - own, 1), :]

    @pl.loop(0, EDGE_ROWS // 64)
    def _(n):
        row = PAD + n * 64
        aligned[pl.ds(next_row - own + n * 64, 64), :] = jnp.where(
            lane_index(64) >= next_shift, edged[pl.ds(row, 64), :], edged[pl.ds(row - 1, 64), :])

    def to_tile(row, tiles):
        for t in range(0, tiles, 2):
            both = [aligned[pl.ds(row + t + k, 8, stride=tiles), :] for k in range(2)]
            own_ref[pl.ds(pl.multiple_of(row + 8 * t, 16), 16), :] = jnp.concatenate(both, axis=0).astype(jnp.bfloat16)

    def plain(row, _):
        own_ref[pl.ds(pl.multiple_of(row, 16), 16), :] = aligned[pl.ds(row, 16), :].astype(jnp.bfloat16)
    for_blocks(own, OWN, to_tile, TENSORS[:4])
    for_blocks(own, OWN, plain, ((*TENSORS[4][:2], 2),))

    for chunk in range(CHUNKS):
        for copy in stores(chunk):
            copy.wait()


def mid(mean_tiles, m, v, w, edges):
    vmem = pl.BlockSpec(memory_space=pltpu.VMEM)
    any_spec = pl.BlockSpec(memory_space=pl.ANY)
    shard = jax.ShapeDtypeStruct((SLICE,), jnp.float32)
    return pl.pallas_call(
        mid_kernel,
        out_shape=(shard, shard, shard, jax.ShapeDtypeStruct((OWN, LANES), jnp.bfloat16)),
        in_specs=[vmem, any_spec, any_spec, any_spec, vmem], out_specs=(any_spec, any_spec, any_spec, vmem),
        scratch_shapes=[
            pltpu.VMEM((SLICE,), jnp.float32), pltpu.VMEM((SLICE,), jnp.float32), pltpu.VMEM((SLICE,), jnp.float32),
            pltpu.VMEM((FLAT_ROWS, LANES), jnp.float32),
            pltpu.VMEM((PAD + SHARD_VREGS * 8 + 8 + 640, LANES), jnp.float32),
            pltpu.VMEM((PAD + EDGE_ROWS, LANES), jnp.float32),
            pltpu.VMEM((OWN_FLAT_ROWS, LANES), jnp.float32),
            pltpu.SemaphoreType.DMA((3, CHUNKS)), pltpu.SemaphoreType.DMA((3, CHUNKS)),
        ],
        compiler_params=pltpu.CompilerParams(vmem_limit_bytes=MID_LIMIT),
    )(mean_tiles, m, v, w, edges)


def pieces_of(tensor):
    base, end, _ = TENSORS[tensor]
    for d in range(SIXTEEN):
        low, high = max(OWN_STARTS[d], base), min(OWN_STARTS[d + 1], end)
        if low < high:
            yield d, low - OWN_STARTS[d], low - base, high - low


PIECES = [(tensor,) + piece for tensor in range(4) for piece in pieces_of(tensor)]
VEC_WIDTH = 12032
VEC_ROWS = VEC_WIDTH // LANES
VEC_BLOCK = VEC_WIDTH // 8
CHIP_COUNTS = tuple((end - base) // 8 for base, end, _ in TENSORS[:4])
CHIP_ROWS = sum(CHIP_COUNTS)
CHIP_SIZE = CHIP_ROWS * LANES + VEC_BLOCK
CHIP_PARTS = 6
CHIP_PART = CHIP_SIZE // 16384 // CHIP_PARTS * 16384


def final_kernel(full_ref, e_out, a_out, f_out, h_out, vec_out, chip_ref, chip_out, flat, vec, out_sem, chip_sem):
    outs = (e_out, a_out, f_out, h_out)
    chip = device_index() // 2
    copies = []
    for n, (tensor, d, source, target, rows) in enumerate(PIECES):
        copies.append(pltpu.make_async_copy(
            full_ref.at[d, pl.ds(source, rows), :], outs[tensor].at[pl.ds(target, rows), :], out_sem.at[n]))
        copies[-1].start()

    slot, source, _, _ = next(pieces_of(4))
    vec[pl.ds(0, 96), :] = full_ref[slot, pl.ds(source, 96), :].astype(jnp.float32)
    for n in range(VEC_ROWS // 8):
        vec_out[:, n * 1024:(n + 1) * 1024] = vec[n * 8:n * 8 + 8, :].reshape(1, 1024).astype(jnp.bfloat16)
    rest = VEC_ROWS % 8
    vec_out[:, VEC_ROWS // 8 * 1024:] = vec[pl.ds(VEC_ROWS - rest, rest), :].reshape(1, rest * LANES).astype(jnp.bfloat16)

    offset = 0
    for tensor, rows in enumerate(CHIP_COUNTS):
        base, _, tiles = TENSORS[tensor]
        step = 16 * tiles

        begin = base + chip * rows
        slot, low, bound = jnp.int32(0), jnp.int32(0), jnp.int32(OWN_STARTS[1])
        for d in range(1, SIXTEEN):
            inside = begin >= OWN_STARTS[d]
            slot = jnp.where(inside, d, slot)
            low = jnp.where(inside, OWN_STARTS[d], low)
            bound = jnp.where(inside, OWN_STARTS[d + 1], bound)

        @pl.loop(0, rows // step)
        def _(n):
            for half in range(2):
                row = begin + n * step + half * 8 * tiles
                following = row >= bound
                at_slot = jnp.where(following, slot + 1, slot)
                at_row = row - jnp.where(following, bound, low)
                for t in range(0, tiles, 2):
                    value = full_ref[at_slot, pl.ds(pl.multiple_of(at_row + 8 * t, 16), 16), :].astype(jnp.float32)
                    for k in range(2):
                        to = offset + n * step + half * 8 * tiles + t + k
                        flat[pl.ds(to, 8, stride=tiles), :] = value[8 * k:8 * k + 8]
        offset += rows

    vec_row = chip * (VEC_BLOCK // 32) // 4
    amount = chip * VEC_BLOCK - vec_row * LANES
    back = (LANES - amount) % LANES
    lane = lane_index()
    for n in range(2):
        here, below = vec[pl.ds(vec_row + n * 8, 8), :], vec[pl.ds(vec_row + n * 8 + 1, 8), :]
        flat[pl.ds(CHIP_ROWS + n * 8, 8), :] = jnp.where(
            lane < LANES - amount, pltpu.roll(here, back, 1), pltpu.roll(below, back, 1))

    def part_copy(part):
        span = pl.ds(part * CHIP_PART, CHIP_PART if part < CHIP_PARTS - 1 else CHIP_SIZE - part * CHIP_PART)
        return pltpu.make_async_copy(chip_out.at[:, span], chip_ref.at[:, span], chip_sem.at[part])

    for part in range(CHIP_PARTS):
        @pl.loop(part * CHIP_PART // 16384, (part + 1) * CHIP_PART // 16384)
        def _(n):
            chip_out[:, pl.ds(pl.multiple_of(n * 16384, 16384), 16384)] = flat[
                pl.ds(pl.multiple_of(n * 128, 128), 128), :].reshape(1, 16384).astype(jnp.bfloat16)
        if part > 0:
            part_copy(part - 1).start()
    done = CHIP_SIZE // 1024 * 1024
    rows = (CHIP_SIZE - done) // LANES
    last = CHIP_SIZE - done - rows * LANES
    first = done // LANES
    chip_out[:, CHIP_PARTS * CHIP_PART:done] = flat[CHIP_PARTS * CHIP_PART // LANES:first, :].reshape(
        1, done - CHIP_PARTS * CHIP_PART).astype(jnp.bfloat16)
    chip_out[:, done:done + rows * LANES] = flat[first:first + rows, :].reshape(1, rows * LANES).astype(jnp.bfloat16)
    chip_out[:, CHIP_SIZE - last:] = flat[first + rows:first + rows + 1, :last].astype(jnp.bfloat16)
    part_copy(CHIP_PARTS - 1).start()
    for part in range(CHIP_PARTS):
        part_copy(part).wait()
    for copy in copies:
        copy.wait()


def finish(full):
    vmem = pl.BlockSpec(memory_space=pltpu.VMEM)
    any_spec = pl.BlockSpec(memory_space=pl.ANY)
    shape = lambda rows: jax.ShapeDtypeStruct((rows, LANES), jnp.bfloat16)
    return pl.pallas_call(
        final_kernel,
        out_shape=tuple(shape(end - base) for base, end, _ in TENSORS[:4]) + (
            jax.ShapeDtypeStruct((1, VEC_WIDTH), jnp.bfloat16), jax.ShapeDtypeStruct((1, CHIP_SIZE), jnp.bfloat16)),
        in_specs=[vmem], out_specs=(any_spec,) * 4 + (vmem, any_spec),
        scratch_shapes=[
            pltpu.VMEM((1, CHIP_SIZE), jnp.bfloat16),
            pltpu.VMEM((CHIP_ROWS + 16, LANES), jnp.float32),
            pltpu.VMEM((120, LANES), jnp.float32),
            pltpu.SemaphoreType.DMA((len(PIECES),)), pltpu.SemaphoreType.DMA((CHIP_PARTS,)),
        ],
        compiler_params=pltpu.CompilerParams(vmem_limit_bytes=FINAL_LIMIT),
    )(full)


def solution(mesh):
    def local_step(g_embed, g_attn, g_ffn_in, g_ffn_out, g_vec, m_shard, v_shard, w_shard):
        matrices = (g_embed, g_attn, g_ffn_in, g_ffn_out)
        grads = [to_tiles(g[0] if g.ndim == 3 else g[0, 0]) for g in matrices]
        grads.append(g_vec.reshape(1, -1))
        mean_tiles, edges = scatter(grads, m_shard, v_shard, w_shard)
        m_new, v_new, w_new, w_own = mid(mean_tiles, m_shard, v_shard, w_shard, edges)
        full = gather(w_own).reshape(SIXTEEN, OWN, LANES)
        *tiles, vec, w_chip = finish(full)
        tensors = [from_tiles(t, g.shape[-1]).reshape(g.shape[1:]) for t, g in zip(tiles, matrices)]
        return (m_new, v_new, w_new) + tuple(tensors) + (vec, w_chip)

    return jax.shard_map(local_step, mesh=mesh, in_specs=(P(MESH_AXES),) * 8, out_specs=(P(MESH_AXES),) * 3 + (P(),) * 5 + (P(MESH_AXES),), check_vma=False)
```
